1024 devices in a mesh: morton: 64 (over x, y), group: 16 (over z, core).
Axes of the slice: x: 8, y: 8, z: 8, core: 2. Of those that a mesh axis runs over, the one named last changes fastest.
Arguments:
- state: float32 [16, 512, 5, 512], P('group', 'morton'), may hold values from -12 to 110, as said below
- patch_count: int32 [64], P('morton'), may hold values from 1 to 8, as said below
- neighbour_table: int32 [64, 8, 4], P('morton'), may hold values from -1 to 511, as said below
- send_table: int32 [64, 64, 5], P('morton'), may hold values from -1 to 31, as said below
- ghost_table: int32 [64, 8, 4], P('morton'), may hold values from -1 to 319, as said below
Outputs:
- updated: float32 [16, 512, 5, 512], P('group', 'morton')
The draws below stay inside these ranges and needn't reach their ends.
Inputs may be any that keep to these rules, and one draw needn't show every extreme that they name: `state`: density lies in [0.5, 2] and the pressure implied by the five variables in [0.1, 0.4] in every live cell. `patch_count`: range i holds slab-order positions starting[i] to starting[i+1] - 1, where starting[i] = i * 4 + j[i] with |j[i]| <= 2 and j[0] = j[64] = 0; some range holds 8. `neighbour_table`: global slot = range * 8 + local slot; slab positions form rows of 4; faces 0 and 1 meet positions -4 and +4, faces 2 and 3 the neighbours in the row; empty slots and domain walls give -1. `send_table`: entry [i, j, t] is -1 or local slot * 4 + face of a patch of range i whose face goes to slot t of the message from i to j; messages of some pair use all 5 slots. `ghost_table`: -1 for faces whose neighbour is held by the same range or absent; else i * 5 + t for the face sent by range i in slot t, and i lies within 2 of the receiving range.
All inputs are finite; a program needn't handle non-finite values.
Results may differ from the reference program's by a relative error of at most 0.00002.
Values sent between devices are 32-bit elements; how exact they have to be, the bound alone decides.
A program may use at most 32 MiB of HBM per device.

```python
import jax
import jax.numpy as jnp
from jax import lax

EDGE = 8
VARS = 5
PATCH_DEV = 4
RANGES = 64
SLABS = 16
SLOTS = 8
MSG_SLOTS = 5
CELLS = 512


def layout(key):
    half = PATCH_DEV // 2
    jitter = jax.random.randint(jax.random.fold_in(key, 11), (RANGES + 1,), -half + 1, half)
    chosen = jax.random.randint(jax.random.fold_in(key, 12), (), 1, RANGES - 2)
    marks = jnp.arange(RANGES + 1, dtype=jnp.int32)
    jitter = jnp.where(marks == chosen, -half, jitter)
    jitter = jnp.where((marks == chosen + 1) | (marks == chosen + 2), half, jitter)
    jitter = jnp.where((marks == 0) | (marks == RANGES), 0, jitter)
    starts = (marks * PATCH_DEV + jitter).astype(jnp.int32)
    counts = (starts[1:] - starts[:-1]).astype(jnp.int32)
    total = RANGES * PATCH_DEV
    slot_ids = jnp.arange(SLOTS, dtype=jnp.int32)
    places = starts[:-1, None] + slot_ids[None, :]
    filled = slot_ids[None, :] < counts[:, None]
    offsets = jnp.array([-PATCH_DEV, PATCH_DEV, -1, 1], dtype=jnp.int32)
    target = places[:, :, None] + offsets
    column = places % PATCH_DEV
    always = jnp.ones_like(filled)
    inside = (target >= 0) & (target < total)
    inside = inside & jnp.stack([always, always, column > 0, column < PATCH_DEV - 1], axis=-1)
    inside = inside & filled[:, :, None]
    clipped = jnp.clip(target, 0, total - 1)
    owners = jnp.sum((clipped[..., None] >= starts[1:RANGES]).astype(jnp.int32), axis=-1).astype(jnp.int32)
    local = (clipped - starts[owners]).astype(jnp.int32)
    neighbour = jnp.where(inside, owners * SLOTS + local, -1).astype(jnp.int32)
    home = jnp.arange(RANGES, dtype=jnp.int32)[:, None, None]
    remote = inside & (owners != home)
    flat_remote = remote.reshape(RANGES, SLOTS * 4)
    flat_owner = owners.reshape(RANGES, SLOTS * 4)
    onehot = (flat_remote[:, :, None] & (flat_owner[:, :, None] == jnp.arange(RANGES, dtype=jnp.int32))).astype(jnp.int32)
    running = jnp.cumsum(onehot, axis=1) - 1
    message_slot = jnp.sum(onehot * running, axis=-1).reshape(RANGES, SLOTS, 4).astype(jnp.int32)
    ghost = jnp.where(remote, owners * MSG_SLOTS + message_slot, -1).astype(jnp.int32)
    directions = jnp.arange(4, dtype=jnp.int32)
    opposite = directions + 1 - 2 * (directions % 2)
    face_id = (local * 4 + opposite).astype(jnp.int32)
    sender = jnp.where(remote, owners, RANGES)
    receiver = jnp.broadcast_to(home, sender.shape)
    table = jnp.full((RANGES, RANGES, MSG_SLOTS), -1, dtype=jnp.int32)
    table = table.at[sender, receiver, message_slot].set(face_id, mode='drop')
    return (counts, neighbour, table, ghost)


def draw_patch_count(key, part):
    return layout(key)[0]


def draw_neighbour_table(key, part):
    return layout(key)[1]


def draw_send_table(key, part):
    return layout(key)[2]


def draw_ghost_table(key, part):
    return layout(key)[3]


def draw_state(key, part):
    count_all = RANGES * SLOTS
    shape = (SLABS, count_all, 1, CELLS)
    slab = jnp.arange(SLABS, dtype=jnp.int32)[:, None, None, None]
    slot = jnp.arange(count_all, dtype=jnp.int32)[None, :, None, None]
    rise = (slot // SLOTS * SLABS + slab).astype(jnp.float32) / (RANGES * SLABS - 1)
    density = jnp.exp(jax.random.uniform(jax.random.fold_in(key, 1), shape, jnp.float32, jnp.log(0.5), jnp.log(2.0)))
    pressure = jnp.exp(jax.random.uniform(jax.random.fold_in(key, 2), shape, jnp.float32, jnp.log(0.1), jnp.log(0.4)))
    vshape = (SLABS, count_all, 3, CELLS)
    velocity = 0.5 * (1.0 + 3.0 * rise) * jnp.clip(jax.random.normal(jax.random.fold_in(key, 3), vshape, jnp.float32), -3.0, 3.0)
    momenta = density * velocity
    energy = pressure / 0.4 + 0.5 * density * jnp.sum(velocity * velocity, axis=2, keepdims=True)
    return jnp.concatenate([density, momenta, energy], axis=2).astype(jnp.float32)


def setup_inputs(seed: int = 0) -> dict:
    seeds = jax.random.split(jax.random.key(seed), 6)
    return {
        "state": draw_state(jax.random.fold_in(seeds[5], 71), 0),
        "patch_count": draw_patch_count(jax.random.fold_in(seeds[5], 71), 0),
        "neighbour_table": draw_neighbour_table(jax.random.fold_in(seeds[5], 71), 0),
        "send_table": draw_send_table(jax.random.fold_in(seeds[5], 71), 0),
        "ghost_table": draw_ghost_table(jax.random.fold_in(seeds[5], 71), 0),
    }


GAMMA = 1.4
COURANT = 0.8

def face_layer(blocks, direction):
    if direction == 0:
        return blocks[..., 0, :, :]
    if direction == 1:
        return blocks[..., -1, :, :]
    if direction == 2:
        return blocks[..., :, 0, :]
    if direction == 3:
        return blocks[..., :, -1, :]
    if direction == 4:
        return blocks[..., :, :, 0]
    return blocks[..., :, :, -1]

def primitives(blocks):
    density = blocks[..., 0, :, :, :]
    momenta = blocks[..., 1:4, :, :, :]
    energy = blocks[..., 4, :, :, :]
    velocity = momenta / density[..., None, :, :, :]
    pressure = (GAMMA - 1.0) * (energy - 0.5 * lax.optimization_barrier(jnp.sum(momenta * velocity, axis=-4)))
    sound = jnp.sqrt(GAMMA * pressure / density)
    return (density, momenta, energy, velocity, pressure, sound)

def wave_bound(blocks):
    density, momenta, energy, velocity, pressure, sound = primitives(blocks)
    return lax.optimization_barrier(jnp.sum(jnp.abs(velocity), axis=-4)) + 3.0 * sound

def euler_flux(blocks, normal_axis):
    density, momenta, energy, velocity, pressure, sound = primitives(blocks)
    normal = velocity[..., normal_axis, :, :, :]
    parts = [momenta[..., normal_axis, :, :, :]]
    for compon in range(3):
        term = momenta[..., compon, :, :, :] * normal
        if compon == normal_axis:
            term = term + pressure
        parts.append(term)
    parts.append((energy + pressure) * normal)
    return (jnp.stack(parts, axis=-4), jnp.abs(normal) + sound)

def rusanov(left, right, normal_axis):
    flux_left, speed_left = euler_flux(left, normal_axis)
    flux_right, speed_right = euler_flux(right, normal_axis)
    speed = jnp.maximum(speed_left, speed_right)
    return 0.5 * (flux_left + flux_right) - 0.5 * speed[..., None, :, :, :] * (right - left)

def divergence(blocks, ghosts):
    extended = jnp.concatenate([ghosts[0][..., None, :, :], blocks, ghosts[1][..., None, :, :]], axis=-3)
    flux = rusanov(extended[..., :-1, :, :], extended[..., 1:, :, :], 0)
    total = flux[..., 1:, :, :] - flux[..., :-1, :, :]
    extended = jnp.concatenate([ghosts[2][..., :, None, :], blocks, ghosts[3][..., :, None, :]], axis=-2)
    flux = rusanov(extended[..., :, :-1, :], extended[..., :, 1:, :], 1)
    total = total + (flux[..., :, 1:, :] - flux[..., :, :-1, :])
    extended = jnp.concatenate([ghosts[4][..., :, :, None], blocks, ghosts[5][..., :, :, None]], axis=-1)
    flux = rusanov(extended[..., :, :, :-1], extended[..., :, :, 1:], 2)
    total = total + (flux[..., :, :, 1:] - flux[..., :, :, :-1])
    return total

def reference(state, patch_count, neighbour_table, send_table, ghost_table):
    slots_total = RANGES * SLOTS
    blocks_all = state.reshape(SLABS, slots_total, VARS, EDGE, EDGE, EDGE)
    slot_ids = jnp.arange(slots_total, dtype=jnp.int32)
    valid = slot_ids % SLOTS < patch_count[slot_ids // SLOTS]
    speeds = wave_bound(blocks_all)
    top_speed = jnp.max(jnp.where(valid[None, :, None, None, None], speeds, jnp.float32(0.0)))
    step_size = COURANT / top_speed
    face_count = slots_total * 4
    positions = jnp.arange(face_count, dtype=jnp.int32)
    home = (positions // (SLOTS * 4)).astype(jnp.int32)
    directions = positions % 4
    opposite = directions + 1 - 2 * (directions % 2)
    neighbours = neighbour_table.reshape(face_count)
    is_local = (neighbours >= 0) & (neighbours // SLOTS == home)
    local_index = jnp.where(is_local, jnp.maximum(neighbours, 0) * 4 + opposite, positions).astype(jnp.int32)
    ghost_flat = ghost_table.reshape(face_count)
    is_remote = ghost_flat >= 0
    safe_ghost = jnp.maximum(ghost_flat, 0)
    sender = (safe_ghost // MSG_SLOTS).astype(jnp.int32)
    message_slot = (safe_ghost % MSG_SLOTS).astype(jnp.int32)
    entry = send_table[sender, home, message_slot]
    remote_index = (sender * (SLOTS * 4) + jnp.maximum(entry, 0)).astype(jnp.int32)
    lower_all = jnp.concatenate([face_layer(blocks_all[:1], 4), face_layer(blocks_all[:-1], 5)], axis=0)
    upper_all = jnp.concatenate([face_layer(blocks_all[1:], 4), face_layer(blocks_all[-1:], 5)], axis=0)

    def one_slab(inputs):
        blocks, lower, upper = inputs
        faces = jnp.stack([face_layer(blocks, direction) for direction in range(4)], axis=1)
        faces = faces.reshape(face_count, VARS, EDGE, EDGE)
        local_faces = jnp.take(faces, local_index, axis=0)
        remote_faces = jnp.take(faces, remote_index, axis=0)
        remote_faces = jnp.where((entry >= 0)[:, None, None, None], remote_faces, jnp.float32(0.0))
        chosen = jnp.where(is_remote[:, None, None, None], remote_faces, local_faces)
        lateral = chosen.reshape(slots_total, 4, VARS, EDGE, EDGE)
        ghosts = [lateral[:, direction] for direction in range(4)]
        ghosts.append(lower)
        ghosts.append(upper)
        change = divergence(blocks, ghosts)
        result = jnp.where(valid[:, None, None, None, None], blocks - step_size * change, jnp.float32(0.0))
        return result.reshape(slots_total, VARS, CELLS)
    return lax.map(one_slab, (blocks_all, lower_all, upper_all))
```

```python
import functools

import jax
import jax.numpy as jnp
from jax import lax
from jax.experimental import pallas as pl
from jax.experimental.pallas import tpu as pltpu
from jax.sharding import Mesh
from jax.sharding import PartitionSpec as P

EDGE = 8
VARS = 5
CELLS = EDGE * EDGE * EDGE
FACE = EDGE * EDGE
SLOTS = 8
MSG = 5
LANES = 128
WIDE = 384
GAMMA = 1.4
COURANT = 0.8
AXES = ("morton_0", "morton_1", "group_0", "group_1")
MORTON = ("morton_0", "morton_1")
GROUP = ("group_0", "group_1")
OFFSETS = (-2, -1, 1, 2)
HUB = 1


def primitives(cells):
    density, mx, my, mz, energy = cells
    inverse = 1.0 / density
    velocity = (mx * inverse, my * inverse, mz * inverse)
    kinetic = mx * velocity[0] + my * velocity[1] + mz * velocity[2]
    pressure = (GAMMA - 1.0) * (energy - 0.5 * kinetic)
    sound = jnp.sqrt(GAMMA * pressure * inverse)
    return velocity, pressure, sound


def axis_flux(cells, prims, axis):
    velocity, pressure, sound = prims
    normal = velocity[axis]
    parts = [cells[1 + axis]]
    for comp in range(3):
        term = cells[1 + comp] * normal
        parts.append(term + pressure if comp == axis else term)
    parts.append((cells[4] + pressure) * normal)
    return parts, jnp.abs(normal) + sound


def lane(shape):
    return lax.broadcasted_iota(jnp.int32, shape, 1)


def pick_lanes(tile, index):
    return jnp.take_along_axis(tile, index, axis=1, mode="promise_in_bounds")


def tiles_of(wide):
    return [wide[:, q * LANES:(q + 1) * LANES] for q in range(wide.shape[1] // LANES)]


def pack_face(cells, face):
    axis, far = face // 2, face % 2
    if axis == 0:
        parts = [v[:, CELLS - FACE:] if far else v[:, :FACE] for v in cells]
        parts.append(jnp.zeros((SLOTS, FACE), jnp.float32))
        return jnp.concatenate(parts, axis=1)
    at = lane((SLOTS, LANES))
    place = at & (FACE - 1)
    if axis == 1:
        source = ((place >> 3) & 1) * FACE + far * (FACE - EDGE) + (place & 7)
    else:
        source = (place & 15) * EDGE + far * (EDGE - 1)
    packed = []
    for v in cells:
        tiles = tiles_of(v)
        out = pick_lanes(tiles[0], source)
        for q in range(1, 4):
            out = jnp.where((place >> 4) == q, pick_lanes(tiles[q], source), out)
        packed.append(out)
    packed.append(jnp.zeros((SLOTS, LANES), jnp.float32))
    pairs = [jnp.where(at < FACE, packed[2 * j], packed[2 * j + 1]) for j in range(3)]
    return jnp.concatenate(pairs, axis=1)


def spread_face(packed, var, axis):
    tile = tiles_of(packed)[var // 2]
    base = (var % 2) * FACE
    at = lane((SLOTS, LANES))
    if axis == 0:
        one = pick_lanes(tile, base + (at & (FACE - 1)))
        return jnp.concatenate([one] * 4, axis=1)
    out = []
    for q in range(4):
        if axis == 1:
            index = base + q * 16 + (at >> 6) * EDGE + (at & 7)
        else:
            index = base + q * 16 + (at >> 3)
        out.append(pick_lanes(tile, index))
    return jnp.concatenate(out, axis=1)


def diagonal(row):
    shape = (SLOTS, SLOTS)
    keep = lax.broadcasted_iota(jnp.int32, shape, 0) == lane(shape)
    return jnp.sum(jnp.where(keep, jnp.broadcast_to(row, shape), 0.0), axis=1, keepdims=True)


def one_hot(column, width):
    places = lane((column.shape[0], width)).astype(jnp.float32)
    return (column == places).astype(jnp.float32)


def select_rows(hot, table):
    return jnp.dot(hot, table, precision=lax.Precision.HIGHEST, preferred_element_type=jnp.float32)


def kernel(
    sizes,
    state, count, neighbour, send, ghost,
    kept_out, change_out, top_out,
    cells_ref, count_ref, neighbour_ref, send_ref, ghost_ref,
    vertical_out, vertical_in, lateral_out, lateral_in,
    value, from_z, from_x, from_y,
    load_sem, count_sem, table_sem, up_sem, down_sem, vin_sem, lsend_sem, lin_sem, max_send, max_recv,
):
    nx, ny, nz, nc = sizes
    x, y, z, c = [lax.axis_index(a) for a in AXES]
    rank = x * ny + y
    ranks = nx * ny

    def device(px, py, pz, pc):
        return {"morton_0": px, "morton_1": py, "group_0": pz, "group_1": pc}

    def at_rank(offset):
        j = lax.rem(rank + (offset + ranks), ranks)
        return device(lax.div(j, ny), lax.rem(j, ny), z, c)

    other = 1 - c
    below = device(x, y, lax.rem(z + (nz - 1) + c, nz), other)
    above = device(x, y, lax.rem(z + c, nz), other)

    loads = [
        pltpu.make_async_copy(state.at[0], cells_ref, load_sem),
        pltpu.make_async_copy(count, count_ref, count_sem),
        pltpu.make_async_copy(neighbour.at[0], neighbour_ref, table_sem.at[0]),
        pltpu.make_async_copy(send, send_ref, table_sem.at[1]),
        pltpu.make_async_copy(ghost.at[0], ghost_ref, table_sem.at[2]),
    ]
    for load in loads:
        load.start()

    barrier = pltpu.get_barrier_semaphore()

    def greet(target):
        pl.semaphore_signal(barrier, inc=1, device_id=target, device_id_type=pl.DeviceIdType.MESH)

    def on(axis_size, here, step):
        return lax.rem(here + step, axis_size)

    hub_partners = (nz - 1) + (nx - 1) + (ny - 1) * 2 + 1
    for target in [below, above] + [at_rank(o) for o in OFFSETS]:
        greet(target)

    @pl.when(c == HUB)
    def _():
        for step in range(1, nz):
            greet(device(x, y, on(nz, z, step), HUB))
        for step in range(nz):
            greet(device(x, y, on(nz, z, step), 1 - HUB))
        for step in range(1, nx):
            greet(device(on(nx, x, step), y, z, HUB))
        for step in range(1, ny):
            greet(device(x, on(ny, y, step), z, HUB))

    @pl.when(c != HUB)
    def _():
        for step in range(ny):
            greet(device(x, on(ny, y, step), z, HUB))

    loads[1].wait()
    loads[0].wait()
    live = lax.broadcasted_iota(jnp.int32, (SLOTS, CELLS), 0) < count_ref[0]
    cells = [cells_ref[v] for v in range(VARS)]
    prims = primitives(cells)
    velocity, pressure, sound = prims
    speed = jnp.abs(velocity[0]) + jnp.abs(velocity[1]) + jnp.abs(velocity[2]) + 3.0 * sound
    speed = jnp.where(live, speed, 0.0)
    top = jnp.max(functools.reduce(jnp.maximum, tiles_of(speed)), axis=0, keepdims=True)
    value[0] = top

    @pl.when(c == HUB)
    def _():
        from_z[z * 2 + HUB] = top
        pl.semaphore_wait(barrier, hub_partners + 2 * 3)

    @pl.when(c != HUB)
    def _():
        pl.semaphore_wait(barrier, nz + 2 * 3)

    def push(source, target_ref, target, phase):
        copy = pltpu.make_async_remote_copy(
            src_ref=source, dst_ref=target_ref, send_sem=max_send.at[phase], recv_sem=max_recv.at[phase],
            device_id=target, device_id_type=pl.DeviceIdType.MESH)
        copy.start()

    def settle(ref, number, sem):
        pltpu.make_async_copy(ref.at[pl.ds(0, number)], ref.at[pl.ds(0, number)], sem).wait()

    def highest(ref, number):
        return functools.reduce(jnp.maximum, [ref[i] for i in range(number)])

    for step in range(1, nz):
        push(value.at[0], from_z.at[z * 2 + c], device(x, y, on(nz, z, step), HUB), 0)

    @pl.when(c != HUB)
    def _():
        push(value.at[0], from_z.at[z * 2 + c], device(x, y, z, HUB), 0)

    vertical_out[0] = pack_face(cells, 4)
    vertical_out[1] = pack_face(cells, 5)
    go_down = pltpu.make_async_remote_copy(
        src_ref=vertical_out.at[0], dst_ref=vertical_in.at[1], send_sem=down_sem, recv_sem=vin_sem.at[1],
        device_id=below, device_id_type=pl.DeviceIdType.MESH)
    go_up = pltpu.make_async_remote_copy(
        src_ref=vertical_out.at[1], dst_ref=vertical_in.at[0], send_sem=up_sem, recv_sem=vin_sem.at[0],
        device_id=above, device_id_type=pl.DeviceIdType.MESH)
    go_down.start()
    go_up.start()

    own = [pack_face(cells, face) for face in range(4)]
    own_rows = jnp.concatenate(own, axis=0)
    loads[3].wait()
    rows = jnp.concatenate([send_ref[t] for t in range(MSG)] + [jnp.full((SLOTS - MSG, ranks), -1, jnp.int32)], axis=0)
    columns = []
    for offset in OFFSETS:
        j = lax.rem(rank + (offset + ranks), ranks)
        picked = jnp.where(lane((SLOTS, ranks)) == j, rows, 0).astype(jnp.float32)
        entry = jnp.sum(picked, axis=1, keepdims=True)
        entry_int = entry.astype(jnp.int32)
        row = jnp.where(entry_int >= 0, (entry_int & 3) * SLOTS + (entry_int >> 2), -1)
        columns.append(row.astype(jnp.float32))
    hot = one_hot(jnp.concatenate(columns, axis=0), 4 * SLOTS)
    messages = select_rows(hot, own_rows)
    for d in range(4):
        lateral_out[d] = messages[d * SLOTS:(d + 1) * SLOTS]
    lateral = []
    for d, offset in enumerate(OFFSETS):
        copy = pltpu.make_async_remote_copy(
            src_ref=lateral_out.at[d], dst_ref=lateral_in.at[3 - d], send_sem=lsend_sem.at[d], recv_sem=lin_sem.at[3 - d],
            device_id=at_rank(offset), device_id_type=pl.DeviceIdType.MESH)
        copy.start()
        lateral.append(copy)

    @pl.when(c == HUB)
    def _():
        settle(from_z, 2 * nz - 1, max_recv.at[0])
        along_z = highest(from_z, 2 * nz)
        value[1] = along_z
        from_x[x] = along_z
        for step in range(1, nx):
            push(value.at[1], from_x.at[x], device(on(nx, x, step), y, z, HUB), 1)

    loads[2].wait()
    loads[4].wait()
    go_down.wait_recv()
    go_up.wait_recv()
    for d in range(4):
        pltpu.make_async_remote_copy(
            src_ref=lateral_out.at[d], dst_ref=lateral_in.at[d], send_sem=lsend_sem.at[d], recv_sem=lin_sem.at[d],
            device_id=at_rank(1), device_id_type=pl.DeviceIdType.MESH).wait_recv()
    faces = jnp.concatenate([own_rows] + [lateral_in[d] for d in range(4)], axis=0)
    near = neighbour_ref[...]
    far = ghost_ref[...]
    face_id = lax.broadcasted_iota(jnp.int32, (4, SLOTS), 0)
    slot_id = lane((4, SLOTS))
    local = (near >= 0) & ((near >> 3) == rank)
    place = jnp.where(local, (face_id ^ 1) * SLOTS + (near & 7), face_id * SLOTS + slot_id)
    relative = far - rank * MSG + 2 * MSG
    block = sum((relative >= MSG * k).astype(jnp.int32) for k in range(1, 5))
    remote = 4 * SLOTS + SLOTS * (block - (block > 2).astype(jnp.int32)) + relative - MSG * block
    place = jnp.where(far >= 0, jnp.where(block == 2, -1, remote), place).astype(jnp.float32)
    columns = [diagonal(place[k:k + 1, :]) for k in range(4)]
    hot = one_hot(jnp.concatenate(columns, axis=0), 8 * SLOTS)
    chosen = select_rows(hot, faces)
    ghosts = [chosen[k * SLOTS:(k + 1) * SLOTS] for k in range(4)]
    slab = z * nc + c
    ghosts.append(jnp.where(slab == 0, vertical_out[0], vertical_in[0]))
    ghosts.append(jnp.where(slab == nz * nc - 1, vertical_out[1], vertical_in[1]))

    total = [0.0] * VARS
    at = lane((SLOTS, CELLS))
    for axis in range(3):
        stride = EDGE ** (2 - axis)
        position = (at >> (3 * (2 - axis))) & 7
        low = [jnp.where(position == 0, spread_face(ghosts[2 * axis], v, axis), pltpu.roll(cells[v], stride, 1))
               for v in range(VARS)]
        high = [jnp.where(position == EDGE - 1, spread_face(ghosts[2 * axis + 1], v, axis),
                          pltpu.roll(cells[v], CELLS - stride, 1)) for v in range(VARS)]
        flux_low, speed_low = axis_flux(low, primitives(low), axis)
        flux_high, speed_high = axis_flux(high, primitives(high), axis)
        speed_here = jnp.abs(velocity[axis]) + sound
        lower = jnp.maximum(speed_low, speed_here)
        upper = jnp.maximum(speed_here, speed_high)
        for v in range(VARS):
            total[v] = total[v] + 0.5 * (
                (flux_high[v] - flux_low[v]) - (upper * (high[v] - cells[v]) - lower * (cells[v] - low[v])))
    for v in range(VARS):
        kept_out[v] = jnp.where(live, cells[v], 0.0)
        change_out[v] = jnp.where(live, total[v], 0.0)

    @pl.when(c == HUB)
    def _():
        settle(from_x, nx - 1, max_recv.at[1])
        plane = highest(from_x, nx)
        value[2] = plane
        from_y[y] = plane
        push(value.at[2], from_y.at[y], device(x, y, z, 1 - HUB), 2)
        for step in range(1, ny):
            push(value.at[2], from_y.at[y], device(x, on(ny, y, step), z, HUB), 2)
            push(value.at[2], from_y.at[y], device(x, on(ny, y, step), z, 1 - HUB), 2)
        settle(from_y, ny - 1, max_recv.at[2])

    @pl.when(c != HUB)
    def _():
        settle(from_y, ny, max_recv.at[2])

    over_all = jnp.max(highest(from_y, ny), axis=1, keepdims=True)
    top_out[...] = jnp.broadcast_to(COURANT / over_all, (1, LANES))

    go_down.wait_send()
    go_up.wait_send()
    for copy in lateral:
        copy.wait_send()

    @pl.when(c == HUB)
    def _():
        settle(from_z, nz - 1, max_send.at[0])
        settle(from_x, nx - 1, max_send.at[1])
        settle(from_z, 2 * ny - 1, max_send.at[2])

    @pl.when(c != HUB)
    def _():
        settle(from_z, nz, max_send.at[0])


def per_device(sizes, state, patch_count, neighbour_table, send_table, ghost_table):
    nx, ny, nz, nc = sizes
    any_space = pl.BlockSpec(memory_space=pl.ANY)
    vmem = pl.BlockSpec(memory_space=pltpu.VMEM)
    f32 = jnp.float32
    dma = pltpu.SemaphoreType.DMA
    kept, change, step = pl.pallas_call(
        functools.partial(kernel, sizes),
        out_shape=(
            jax.ShapeDtypeStruct((VARS, SLOTS, CELLS), f32),
            jax.ShapeDtypeStruct((VARS, SLOTS, CELLS), f32),
            jax.ShapeDtypeStruct((1, LANES), f32),
        ),
        in_specs=[any_space] * 5,
        out_specs=(vmem, vmem, vmem),
        scratch_shapes=[
            pltpu.VMEM((VARS, SLOTS, CELLS), f32),
            pltpu.SMEM((1,), jnp.int32),
            pltpu.VMEM((4, SLOTS), jnp.int32),
            pltpu.VMEM((MSG, 1, nx * ny), jnp.int32),
            pltpu.VMEM((4, SLOTS), jnp.int32),
            pltpu.VMEM((2, SLOTS, WIDE), f32),
            pltpu.VMEM((2, SLOTS, WIDE), f32),
            pltpu.VMEM((4, SLOTS, WIDE), f32),
            pltpu.VMEM((4, SLOTS, WIDE), f32),
            pltpu.VMEM((3, 1, LANES), f32),
            pltpu.VMEM((2 * max(nz, ny), 1, LANES), f32),
            pltpu.VMEM((nx, 1, LANES), f32),
            pltpu.VMEM((ny, 1, LANES), f32),
            dma, dma, dma((3,)), dma, dma, dma((2,)), dma((4,)), dma((4,)), dma((3,)), dma((3,)),
        ],
        compiler_params=pltpu.CompilerParams(collective_id=0, has_side_effects=True),
        name="step",
    )(
        jnp.transpose(state, (0, 2, 1, 3)),
        patch_count,
        jnp.transpose(neighbour_table, (0, 2, 1)),
        jnp.transpose(send_table, (2, 0, 1)),
        jnp.transpose(ghost_table, (0, 2, 1)),
    )
    updated = kept - step[0, 0] * change
    return jnp.transpose(updated[None], (0, 2, 1, 3))


def solution(mesh):
    nx = ny = round((mesh.shape["morton"]) ** 0.5)
    sizes = (nx, ny, mesh.shape["group"] // 2, 2)
    torus = Mesh(mesh.devices.reshape(sizes), AXES)
    return jax.shard_map(
        functools.partial(per_device, sizes),
        mesh=torus,
        in_specs=(
            P(GROUP, MORTON, None, None),
            P(MORTON),
            P(MORTON, None, None),
            P(MORTON, None, None),
            P(MORTON, None, None),
        ),
        out_specs=P(GROUP, MORTON, None, None),
        check_vma=False,
    )
```

```python
import functools

import jax
import jax.numpy as jnp
from jax import lax
from jax.experimental import pallas as pl
from jax.experimental.pallas import tpu as pltpu
from jax.sharding import Mesh
from jax.sharding import PartitionSpec as P

EDGE = 8
VARS = 5
CELLS = EDGE * EDGE * EDGE
FACE = EDGE * EDGE
SLOTS = 8
MSG = 5
LANES = 128
WIDE = 384
GAMMA = 1.4
COURANT = 0.8
AXES = ("morton_0", "morton_1", "group_0", "group_1")
MORTON = ("morton_0", "morton_1")
GROUP = ("group_0", "group_1")
OFFSETS = (-2, -1, 1, 2)
HUB = 1


def primitives(cells):
    density, mx, my, mz, energy = cells
    inverse = 1.0 / density
    velocity = (mx * inverse, my * inverse, mz * inverse)
    kinetic = mx * velocity[0] + my * velocity[1] + mz * velocity[2]
    pressure = (GAMMA - 1.0) * (energy - 0.5 * kinetic)
    sound = jnp.sqrt(GAMMA * pressure * inverse)
    return velocity, pressure, sound


def axis_flux(cells, prims, axis):
    velocity, pressure, sound = prims
    normal = velocity[axis]
    parts = [cells[1 + axis]]
    for comp in range(3):
        term = cells[1 + comp] * normal
        parts.append(term + pressure if comp == axis else term)
    parts.append((cells[4] + pressure) * normal)
    return parts, jnp.abs(normal) + sound


def lane(shape):
    return lax.broadcasted_iota(jnp.int32, shape, 1)


def pick_lanes(tile, index):
    return jnp.take_along_axis(tile, index, axis=1, mode="promise_in_bounds")


def tiles_of(wide):
    return [wide[:, q * LANES:(q + 1) * LANES] for q in range(wide.shape[1] // LANES)]


def pack_face(cells, face):
    axis, far = face // 2, face % 2
    if axis == 0:
        parts = [v[:, CELLS - FACE:] if far else v[:, :FACE] for v in cells]
        parts.append(jnp.zeros((SLOTS, FACE), jnp.float32))
        return jnp.concatenate(parts, axis=1)
    at = lane((SLOTS, LANES))
    place = at & (FACE - 1)
    if axis == 1:
        source = ((place >> 3) & 1) * FACE + far * (FACE - EDGE) + (place & 7)
    else:
        source = (place & 15) * EDGE + far * (EDGE - 1)
    packed = []
    for v in cells:
        tiles = tiles_of(v)
        out = pick_lanes(tiles[0], source)
        for q in range(1, 4):
            out = jnp.where((place >> 4) == q, pick_lanes(tiles[q], source), out)
        packed.append(out)
    packed.append(jnp.zeros((SLOTS, LANES), jnp.float32))
    pairs = [jnp.where(at < FACE, packed[2 * j], packed[2 * j + 1]) for j in range(3)]
    return jnp.concatenate(pairs, axis=1)


def spread_face(packed, var, axis):
    tile = tiles_of(packed)[var // 2]
    base = (var % 2) * FACE
    at = lane((SLOTS, LANES))
    if axis == 0:
        one = pick_lanes(tile, base + (at & (FACE - 1)))
        return jnp.concatenate([one] * 4, axis=1)
    out = []
    for q in range(4):
        if axis == 1:
            index = base + q * 16 + (at >> 6) * EDGE + (at & 7)
        else:
            index = base + q * 16 + (at >> 3)
        out.append(pick_lanes(tile, index))
    return jnp.concatenate(out, axis=1)


def diagonal(row):
    shape = (SLOTS, SLOTS)
    keep = lax.broadcasted_iota(jnp.int32, shape, 0) == lane(shape)
    return jnp.sum(jnp.where(keep, jnp.broadcast_to(row, shape), 0.0), axis=1, keepdims=True)


def one_hot(column, width):
    places = lane((column.shape[0], width)).astype(jnp.float32)
    return (column == places).astype(jnp.float32)


def select_rows(hot, table):
    return jnp.dot(hot, table, precision=lax.Precision.HIGHEST, preferred_element_type=jnp.float32)


def kernel(
    sizes,
    state, count, neighbour, send, ghost,
    updated_out,
    cells_ref, count_ref, neighbour_ref, send_ref, ghost_ref,
    vertical_out, vertical_in, lateral_out, lateral_in, change_ref,
    value, from_plane, from_hubs, result,
    load_sem, count_sem, table_sem, up_sem, down_sem, vin_sem, lsend_sem, lin_sem, max_send, max_recv,
):
    nx, ny, nz, nc = sizes
    x, y, z, c = [lax.axis_index(a) for a in AXES]
    rank = x * ny + y
    ranks = nx * ny
    in_plane = 2 * ny * nz
    first = 2 * nx * ny

    def device(px, py, pz, pc):
        return {"morton_0": px, "morton_1": py, "group_0": pz, "group_1": pc}

    def hub_of(px):
        return device(px, 0, 0, HUB)

    def at_rank(offset):
        j = lax.rem(rank + (offset + ranks), ranks)
        return device(lax.div(j, ny), lax.rem(j, ny), z, c)

    is_hub = (y == 0) & (z == 0) & (c == HUB)
    is_first = z == 0
    other = 1 - c
    below = device(x, y, lax.rem(z + (nz - 1) + c, nz), other)
    above = device(x, y, lax.rem(z + c, nz), other)

    loads = [
        pltpu.make_async_copy(state.at[0], cells_ref, load_sem),
        pltpu.make_async_copy(count, count_ref, count_sem),
        pltpu.make_async_copy(neighbour.at[0], neighbour_ref, table_sem.at[0]),
        pltpu.make_async_copy(send, send_ref, table_sem.at[1]),
        pltpu.make_async_copy(ghost.at[0], ghost_ref, table_sem.at[2]),
    ]
    for load in loads:
        load.start()

    barrier = pltpu.get_barrier_semaphore()

    def greet(target):
        pl.semaphore_signal(barrier, inc=1, device_id=target, device_id_type=pl.DeviceIdType.MESH)

    for target in [below, above] + [at_rank(o) for o in OFFSETS]:
        greet(target)

    @pl.when(is_hub)
    def _():
        for step in range(1, nx):
            greet(hub_of(lax.rem(x + step, nx)))
        greet(device(x, 0, 0, 1 - HUB))

        def plane(i, carry):
            greet(device(x, lax.rem(lax.div(i, 2), ny), lax.div(i, 2 * ny), lax.rem(i, 2)))
            return carry

        lax.fori_loop(2, in_plane, plane, 0)

    @pl.when(is_first & jnp.logical_not(is_hub))
    def _():
        for px in range(nx):
            greet(hub_of(px))

    loads[1].wait()
    loads[0].wait()
    live = lax.broadcasted_iota(jnp.int32, (SLOTS, CELLS), 0) < jnp.broadcast_to(count_ref[...], (SLOTS, CELLS))
    cells = [cells_ref[v] for v in range(VARS)]
    prims = primitives(cells)
    velocity, pressure, sound = prims
    speed = jnp.abs(velocity[0]) + jnp.abs(velocity[1]) + jnp.abs(velocity[2]) + 3.0 * sound
    speed = jnp.where(live, speed, 0.0)
    top = jnp.max(functools.reduce(jnp.maximum, tiles_of(speed)), axis=0, keepdims=True)
    value[0] = top

    def push(source, target_ref, target, phase, arrival):
        pltpu.make_async_remote_copy(
            src_ref=source, dst_ref=target_ref, send_sem=max_send.at[phase], recv_sem=max_recv.at[arrival],
            device_id=target, device_id_type=pl.DeviceIdType.MESH).start()

    def settle(ref, number, sem):
        pltpu.make_async_copy(ref.at[pl.ds(0, number)], ref.at[pl.ds(0, number)], sem).wait()

    mine = (z * ny + y) * 2 + c

    @pl.when(is_hub)
    def _():
        from_plane[mine] = top
        pl.semaphore_wait(barrier, first - 1 + 2 * 3)

    @pl.when(jnp.logical_not(is_hub))
    def _():
        pl.semaphore_wait(barrier, 1 + 2 * 3)
        push(value.at[0], from_plane.at[mine], hub_of(x), 0, 0)

    vertical_out[0] = pack_face(cells, 4)
    vertical_out[1] = pack_face(cells, 5)
    go_down = pltpu.make_async_remote_copy(
        src_ref=vertical_out.at[0], dst_ref=vertical_in.at[1], send_sem=down_sem, recv_sem=vin_sem.at[1],
        device_id=below, device_id_type=pl.DeviceIdType.MESH)
    go_up = pltpu.make_async_remote_copy(
        src_ref=vertical_out.at[1], dst_ref=vertical_in.at[0], send_sem=up_sem, recv_sem=vin_sem.at[0],
        device_id=above, device_id_type=pl.DeviceIdType.MESH)
    go_down.start()
    go_up.start()

    own = [pack_face(cells, face) for face in range(4)]
    own_rows = jnp.concatenate(own, axis=0)
    loads[3].wait()
    rows = jnp.concatenate([send_ref[t] for t in range(MSG)] + [jnp.full((SLOTS - MSG, ranks), -1, jnp.int32)], axis=0)
    columns = []
    for offset in OFFSETS:
        j = lax.rem(rank + (offset + ranks), ranks)
        picked = jnp.where(lane((SLOTS, ranks)) == j, rows, 0).astype(jnp.float32)
        entry = jnp.sum(picked, axis=1, keepdims=True)
        entry_int = entry.astype(jnp.int32)
        row = jnp.where(entry_int >= 0, (entry_int & 3) * SLOTS + (entry_int >> 2), -1)
        columns.append(row.astype(jnp.float32))
    hot = one_hot(jnp.concatenate(columns, axis=0), 4 * SLOTS)
    messages = select_rows(hot, own_rows)
    for d in range(4):
        lateral_out[d] = messages[d * SLOTS:(d + 1) * SLOTS]
    lateral = []
    for d, offset in enumerate(OFFSETS):
        copy = pltpu.make_async_remote_copy(
            src_ref=lateral_out.at[d], dst_ref=lateral_in.at[3 - d], send_sem=lsend_sem.at[d], recv_sem=lin_sem.at[3 - d],
            device_id=at_rank(offset), device_id_type=pl.DeviceIdType.MESH)
        copy.start()
        lateral.append(copy)

    loads[2].wait()
    loads[4].wait()
    go_down.wait_recv()
    go_up.wait_recv()
    for d in range(4):
        pltpu.make_async_remote_copy(
            src_ref=lateral_out.at[d], dst_ref=lateral_in.at[d], send_sem=lsend_sem.at[d], recv_sem=lin_sem.at[d],
            device_id=at_rank(1), device_id_type=pl.DeviceIdType.MESH).wait_recv()
    faces = jnp.concatenate([own_rows] + [lateral_in[d] for d in range(4)], axis=0)
    near = neighbour_ref[...]
    far = ghost_ref[...]
    face_id = lax.broadcasted_iota(jnp.int32, (4, SLOTS), 0)
    slot_id = lane((4, SLOTS))
    local = (near >= 0) & ((near >> 3) == rank)
    place = jnp.where(local, (face_id ^ 1) * SLOTS + (near & 7), face_id * SLOTS + slot_id)
    relative = far - rank * MSG + 2 * MSG
    block = sum((relative >= MSG * k).astype(jnp.int32) for k in range(1, 5))
    remote = 4 * SLOTS + SLOTS * (block - (block > 2).astype(jnp.int32)) + relative - MSG * block
    place = jnp.where(far >= 0, jnp.where(block == 2, -1, remote), place).astype(jnp.float32)
    columns = [diagonal(place[k:k + 1, :]) for k in range(4)]
    hot = one_hot(jnp.concatenate(columns, axis=0), 8 * SLOTS)
    chosen = select_rows(hot, faces)
    ghosts = [chosen[k * SLOTS:(k + 1) * SLOTS] for k in range(4)]
    slab = z * nc + c
    ghosts.append(jnp.where(slab == 0, vertical_out[0], vertical_in[0]))
    ghosts.append(jnp.where(slab == nz * nc - 1, vertical_out[1], vertical_in[1]))

    total = [0.0] * VARS
    at = lane((SLOTS, CELLS))
    for axis in range(3):
        stride = EDGE ** (2 - axis)
        position = (at >> (3 * (2 - axis))) & 7
        low = [jnp.where(position == 0, spread_face(ghosts[2 * axis], v, axis), pltpu.roll(cells[v], stride, 1))
               for v in range(VARS)]
        high = [jnp.where(position == EDGE - 1, spread_face(ghosts[2 * axis + 1], v, axis),
                          pltpu.roll(cells[v], CELLS - stride, 1)) for v in range(VARS)]
        flux_low, speed_low = axis_flux(low, primitives(low), axis)
        flux_high, speed_high = axis_flux(high, primitives(high), axis)
        speed_here = jnp.abs(velocity[axis]) + sound
        lower = jnp.maximum(speed_low, speed_here)
        upper = jnp.maximum(speed_here, speed_high)
        for v in range(VARS):
            total[v] = total[v] + 0.5 * (
                (flux_high[v] - flux_low[v]) - (upper * (high[v] - cells[v]) - lower * (cells[v] - low[v])))
    for v in range(VARS):
        change_ref[v] = total[v]

    go_down.wait_send()
    go_up.wait_send()
    for copy in lateral:
        copy.wait_send()

    def finish(highest):
        step = COURANT / jnp.max(highest, axis=1, keepdims=True)
        for v in range(VARS):
            updated_out[v] = jnp.where(live, cells_ref[v] - step * change_ref[v], 0.0)

    def of_hubs():
        return functools.reduce(jnp.maximum, [from_hubs[i] for i in range(nx)])

    @pl.when(is_hub)
    def _():
        settle(from_plane, in_plane - 1, max_recv.at[0])
        plane_top = jnp.max(from_plane[...], axis=0)
        value[1] = plane_top
        from_hubs[x] = plane_top

        def tell(i, carry):
            px, py, pc = lax.rem(lax.div(i, 2), nx), lax.div(i, 2 * nx), lax.rem(i + 1, 2)

            @pl.when((px != x) | (py != 0) | (pc != HUB))
            def _():
                push(value.at[1], from_hubs.at[x], device(px, py, 0, pc), 1, 1)

            return carry

        lax.fori_loop(0, first, tell, 0)
        settle(from_hubs, nx - 1, max_recv.at[1])
        finish(of_hubs())
        settle(from_plane, first - 1, max_send.at[1])

    @pl.when(is_first & (c == HUB) & jnp.logical_not(is_hub))
    def _():
        settle(from_hubs, nx, max_recv.at[1])
        finish(of_hubs())
        settle(from_plane, 1, max_send.at[0])

    @pl.when(is_first & (c != HUB))
    def _():
        settle(from_hubs, nx, max_recv.at[1])
        over_all = of_hubs()
        value[2] = over_all
        for pz in range(1, nz):
            for pc in (1, 0):
                push(value.at[2], result.at[0], device(x, y, pz, pc), 2, 2)
        finish(over_all)
        settle(from_plane, 1, max_send.at[0])
        settle(from_plane, 2 * (nz - 1), max_send.at[2])

    @pl.when(jnp.logical_not(is_first))
    def _():
        settle(result, 1, max_recv.at[2])
        finish(result[0])
        settle(from_plane, 1, max_send.at[0])


def per_device(sizes, state, patch_count, neighbour_table, send_table, ghost_table):
    nx, ny, nz, nc = sizes
    any_space = pl.BlockSpec(memory_space=pl.ANY)
    vmem = pl.BlockSpec(memory_space=pltpu.VMEM)
    f32 = jnp.float32
    dma = pltpu.SemaphoreType.DMA
    updated = pl.pallas_call(
        functools.partial(kernel, sizes),
        out_shape=pltpu.VMEM((VARS, SLOTS, CELLS), f32),
        in_specs=[any_space] * 5,
        out_specs=vmem,
        scratch_shapes=[
            pltpu.VMEM((VARS, SLOTS, CELLS), f32),
            pltpu.VMEM((1, 1), jnp.int32),
            pltpu.VMEM((4, SLOTS), jnp.int32),
            pltpu.VMEM((MSG, 1, nx * ny), jnp.int32),
            pltpu.VMEM((4, SLOTS), jnp.int32),
            pltpu.VMEM((2, SLOTS, WIDE), f32),
            pltpu.VMEM((2, SLOTS, WIDE), f32),
            pltpu.VMEM((4, SLOTS, WIDE), f32),
            pltpu.VMEM((4, SLOTS, WIDE), f32),
            pltpu.VMEM((VARS, SLOTS, CELLS), f32),
            pltpu.VMEM((3, 1, LANES), f32),
            pltpu.VMEM((2 * ny * max(nz, nx), 1, LANES), f32),
            pltpu.VMEM((nx, 1, LANES), f32),
            pltpu.VMEM((1, 1, LANES), f32),
            dma, dma, dma((3,)), dma, dma, dma((2,)), dma((4,)), dma((4,)), dma((3,)), dma((3,)),
        ],
        compiler_params=pltpu.CompilerParams(collective_id=0, has_side_effects=True),
        name="step",
    )(
        jnp.transpose(state, (0, 2, 1, 3)),
        patch_count.reshape(1, 1),
        jnp.transpose(neighbour_table, (0, 2, 1)),
        jnp.transpose(send_table, (2, 0, 1)),
        jnp.transpose(ghost_table, (0, 2, 1)),
    )
    return jnp.transpose(updated[None], (0, 2, 1, 3))


def solution(mesh):
    nx = ny = round((mesh.shape["morton"]) ** 0.5)
    sizes = (nx, ny, mesh.shape["group"] // 2, 2)
    torus = Mesh(mesh.devices.reshape(sizes), AXES)
    return jax.shard_map(
        functools.partial(per_device, sizes),
        mesh=torus,
        in_specs=(
            P(GROUP, MORTON, None, None),
            P(MORTON),
            P(MORTON, None, None),
            P(MORTON, None, None),
            P(MORTON, None, None),
        ),
        out_specs=P(GROUP, MORTON, None, None),
        check_vma=False,
    )
```

```python
import functools

import jax
import jax.numpy as jnp
from jax import lax
from jax.experimental import pallas as pl
from jax.experimental.pallas import tpu as pltpu
from jax.sharding import Mesh
from jax.sharding import PartitionSpec as P

EDGE = 8
VARS = 5
CELLS = EDGE * EDGE * EDGE
FACE = EDGE * EDGE
SLOTS = 8
MSG = 5
LANES = 128
WIDE = 384
GAMMA = 1.4
COURANT = 0.8
AXES = ("morton_0", "morton_1", "group_0", "group_1")
MORTON = ("morton_0", "morton_1")
GROUP = ("group_0", "group_1")
OFFSETS = (-2, -1, 1, 2)
HUB = 1


def primitives(cells):
    density, mx, my, mz, energy = cells
    inverse = 1.0 / density
    velocity = (mx * inverse, my * inverse, mz * inverse)
    kinetic = mx * velocity[0] + my * velocity[1] + mz * velocity[2]
    pressure = (GAMMA - 1.0) * (energy - 0.5 * kinetic)
    sound = jnp.sqrt(GAMMA * pressure * inverse)
    return velocity, pressure, sound


def axis_flux(cells, prims, axis):
    velocity, pressure, sound = prims
    normal = velocity[axis]
    parts = [cells[1 + axis]]
    for comp in range(3):
        term = cells[1 + comp] * normal
        parts.append(term + pressure if comp == axis else term)
    parts.append((cells[4] + pressure) * normal)
    return parts, jnp.abs(normal) + sound


def lane(shape):
    return lax.broadcasted_iota(jnp.int32, shape, 1)


def pick_lanes(tile, index):
    return jnp.take_along_axis(tile, index, axis=1, mode="promise_in_bounds")


def tiles_of(wide):
    return [wide[:, q * LANES:(q + 1) * LANES] for q in range(wide.shape[1] // LANES)]


def pack_face(cells, face):
    axis, far = face // 2, face % 2
    if axis == 0:
        parts = [v[:, CELLS - FACE:] if far else v[:, :FACE] for v in cells]
        parts.append(jnp.zeros((SLOTS, FACE), jnp.float32))
        return jnp.concatenate(parts, axis=1)
    at = lane((SLOTS, LANES))
    place = at & (FACE - 1)
    if axis == 1:
        source = ((place >> 3) & 1) * FACE + far * (FACE - EDGE) + (place & 7)
    else:
        source = (place & 15) * EDGE + far * (EDGE - 1)
    packed = []
    for v in cells:
        tiles = tiles_of(v)
        out = pick_lanes(tiles[0], source)
        for q in range(1, 4):
            out = jnp.where((place >> 4) == q, pick_lanes(tiles[q], source), out)
        packed.append(out)
    packed.append(jnp.zeros((SLOTS, LANES), jnp.float32))
    pairs = [jnp.where(at < FACE, packed[2 * j], packed[2 * j + 1]) for j in range(3)]
    return jnp.concatenate(pairs, axis=1)


def spread_face(packed, var, axis):
    tile = tiles_of(packed)[var // 2]
    base = (var % 2) * FACE
    at = lane((SLOTS, LANES))
    if axis == 0:
        one = pick_lanes(tile, base + (at & (FACE - 1)))
        return jnp.concatenate([one] * 4, axis=1)
    out = []
    for q in range(4):
        if axis == 1:
            index = base + q * 16 + (at >> 6) * EDGE + (at & 7)
        else:
            index = base + q * 16 + (at >> 3)
        out.append(pick_lanes(tile, index))
    return jnp.concatenate(out, axis=1)


def diagonal(row):
    shape = (SLOTS, SLOTS)
    keep = lax.broadcasted_iota(jnp.int32, shape, 0) == lane(shape)
    return jnp.sum(jnp.where(keep, jnp.broadcast_to(row, shape), 0.0), axis=1, keepdims=True)


def one_hot(column, width):
    places = lane((column.shape[0], width)).astype(jnp.float32)
    return (column == places).astype(jnp.float32)


def select_rows(hot, table):
    return jnp.dot(hot, table, precision=lax.Precision.HIGHEST, preferred_element_type=jnp.float32)


def kernel(
    sizes,
    state, neighbour, send, ghost,
    updated_out,
    cells_ref, neighbour_ref, send_ref, ghost_ref,
    vertical_out, vertical_in, lateral_out, lateral_in, change_ref,
    value, from_plane, from_hubs, result,
    load_sem, table_sem, up_sem, down_sem, vin_sem, lsend_sem, lin_sem, max_send, max_recv,
):
    nx, ny, nz, nc = sizes
    x, y, z, c = [lax.axis_index(a) for a in AXES]
    rank = x * ny + y
    ranks = nx * ny
    in_plane = 2 * ny * nz
    slab = z * nc + c
    has_below, has_above = slab > 0, slab < nz * nc - 1
    mid = ny // 2

    def group_of(py):
        return ((py * 4 >= ny) & (py * 4 <= 3 * ny)).astype(jnp.int32) if not isinstance(py, int) else int(ny <= py * 4 <= 3 * ny)

    members = [[py for py in range(ny) if group_of(py) == g] for g in (0, 1)]

    def device(px, py, pz, pc):
        return {"morton_0": px, "morton_1": py, "group_0": pz, "group_1": pc}

    def hub_of(px, group):
        return device(px, group * mid, 0, HUB)

    def at_rank(offset):
        j = lax.rem(rank + (offset + ranks), ranks)
        return device(lax.div(j, ny), lax.rem(j, ny), z, c)

    group = group_of(y)
    is_hub = ((y == 0) | (y == mid)) & (z == 0) & (c == HUB)
    is_listener = (z == 0) & jnp.logical_not(is_hub)
    is_teller = (z == 1) & (c != HUB)
    is_other = (z > 1) | ((z == 1) & (c == HUB))
    other = 1 - c
    below = device(x, y, lax.rem(z + (nz - 1) + c, nz), other)
    above = device(x, y, lax.rem(z + c, nz), other)

    loads = [
        pltpu.make_async_copy(state.at[0], cells_ref, load_sem),
        pltpu.make_async_copy(neighbour.at[0], neighbour_ref, table_sem.at[0]),
        pltpu.make_async_copy(send, send_ref, table_sem.at[1]),
        pltpu.make_async_copy(ghost.at[0], ghost_ref, table_sem.at[2]),
    ]
    for load in loads:
        load.start()

    barrier = pltpu.get_barrier_semaphore()

    def greet(target):
        pl.semaphore_signal(barrier, inc=1, device_id=target, device_id_type=pl.DeviceIdType.MESH)

    for target in [at_rank(o) for o in OFFSETS]:
        greet(target)

    @pl.when(has_below)
    def _():
        greet(below)

    @pl.when(has_above)
    def _():
        greet(above)

    @pl.when(is_hub)
    def _():
        def plane(i, carry):
            py, pz, pc = lax.rem(lax.div(i, 2), ny), lax.div(i, 2 * ny), lax.rem(i, 2)

            @pl.when((py != y) | (pz != 0) | (pc != HUB))
            def _():
                greet(device(x, py, pz, pc))

            return carry

        lax.fori_loop(0, in_plane, plane, 0)
        for step in range(1, nx):
            greet(hub_of(lax.rem(x + step, nx), group))

    @pl.when(is_listener | is_teller)
    def _():
        for px in range(nx):
            greet(hub_of(px, group))

    loads[1].wait()
    near = neighbour_ref[...]
    loads[0].wait()
    in_row = diagonal(jnp.maximum(near[2:3, :], near[3:4, :]).astype(jnp.float32))
    live = jnp.broadcast_to(in_row, (SLOTS, CELLS)) >= 0.0
    cells = [cells_ref[v] for v in range(VARS)]
    prims = primitives(cells)
    velocity, pressure, sound = prims
    speed = jnp.abs(velocity[0]) + jnp.abs(velocity[1]) + jnp.abs(velocity[2]) + 3.0 * sound
    speed = jnp.where(live, speed, 0.0)
    top = jnp.max(functools.reduce(jnp.maximum, tiles_of(speed)), axis=0, keepdims=True)
    value[0] = top

    def push(source, target_ref, target, phase, arrival):
        pltpu.make_async_remote_copy(
            src_ref=source, dst_ref=target_ref, send_sem=max_send.at[phase], recv_sem=max_recv.at[arrival],
            device_id=target, device_id_type=pl.DeviceIdType.MESH).start()

    def settle(ref, number, sem):
        pltpu.make_async_copy(ref.at[pl.ds(0, number)], ref.at[pl.ds(0, number)], sem).wait()

    mine = (z * ny + y) * 2 + c

    halo = 4 + has_below.astype(jnp.int32) + has_above.astype(jnp.int32)

    @pl.when(is_hub)
    def _():
        from_plane[mine] = top
        told = jnp.where(group == 0, len(members[0]), len(members[1])) * nx * 3
        pl.semaphore_wait(barrier, told + halo)
        push(value.at[0], from_plane.at[mine], hub_of(x, 1 - group), 0, 0)

    @pl.when(jnp.logical_not(is_hub))
    def _():
        pl.semaphore_wait(barrier, 2 + halo)
        push(value.at[0], from_plane.at[mine], hub_of(x, 0), 0, 0)
        push(value.at[0], from_plane.at[mine], hub_of(x, 1), 0, 0)

    vertical_out[0] = pack_face(cells, 4)
    vertical_out[1] = pack_face(cells, 5)
    go_down = pltpu.make_async_remote_copy(
        src_ref=vertical_out.at[0], dst_ref=vertical_in.at[1], send_sem=down_sem, recv_sem=vin_sem.at[1],
        device_id=below, device_id_type=pl.DeviceIdType.MESH)
    go_up = pltpu.make_async_remote_copy(
        src_ref=vertical_out.at[1], dst_ref=vertical_in.at[0], send_sem=up_sem, recv_sem=vin_sem.at[0],
        device_id=above, device_id_type=pl.DeviceIdType.MESH)

    @pl.when(has_below)
    def _():
        go_down.start()

    @pl.when(jnp.logical_not(has_below))
    def _():
        vertical_in[0] = vertical_out[0]

    @pl.when(has_above)
    def _():
        go_up.start()

    @pl.when(jnp.logical_not(has_above))
    def _():
        vertical_in[1] = vertical_out[1]


    own = [pack_face(cells, face) for face in range(4)]
    own_rows = jnp.concatenate(own, axis=0)
    loads[2].wait()
    rows = jnp.concatenate([send_ref[t] for t in range(MSG)] + [jnp.full((SLOTS - MSG, ranks), -1, jnp.int32)], axis=0)
    columns = []
    for offset in OFFSETS:
        j = lax.rem(rank + (offset + ranks), ranks)
        picked = jnp.where(lane((SLOTS, ranks)) == j, rows, 0).astype(jnp.float32)
        entry = jnp.sum(picked, axis=1, keepdims=True)
        entry_int = entry.astype(jnp.int32)
        row = jnp.where(entry_int >= 0, (entry_int & 3) * SLOTS + (entry_int >> 2), -1)
        columns.append(row.astype(jnp.float32))
    hot = one_hot(jnp.concatenate(columns, axis=0), 4 * SLOTS)
    messages = select_rows(hot, own_rows)
    for d in range(4):
        lateral_out[d] = messages[d * SLOTS:(d + 1) * SLOTS]
    lateral = []
    for d, offset in enumerate(OFFSETS):
        copy = pltpu.make_async_remote_copy(
            src_ref=lateral_out.at[d], dst_ref=lateral_in.at[3 - d], send_sem=lsend_sem.at[d], recv_sem=lin_sem.at[3 - d],
            device_id=at_rank(offset), device_id_type=pl.DeviceIdType.MESH)
        copy.start()
        lateral.append(copy)

    loads[3].wait()

    @pl.when(has_above)
    def _():
        go_down.wait_recv()

    @pl.when(has_below)
    def _():
        go_up.wait_recv()

    for d in range(4):
        pltpu.make_async_remote_copy(
            src_ref=lateral_out.at[d], dst_ref=lateral_in.at[d], send_sem=lsend_sem.at[d], recv_sem=lin_sem.at[d],
            device_id=at_rank(1), device_id_type=pl.DeviceIdType.MESH).wait_recv()
    faces = jnp.concatenate([own_rows] + [lateral_in[d] for d in range(4)], axis=0)
    far = ghost_ref[...]
    face_id = lax.broadcasted_iota(jnp.int32, (4, SLOTS), 0)
    slot_id = lane((4, SLOTS))
    local = (near >= 0) & ((near >> 3) == rank)
    place = jnp.where(local, (face_id ^ 1) * SLOTS + (near & 7), face_id * SLOTS + slot_id)
    relative = far - rank * MSG + 2 * MSG
    block = sum((relative >= MSG * k).astype(jnp.int32) for k in range(1, 5))
    remote = 4 * SLOTS + SLOTS * (block - (block > 2).astype(jnp.int32)) + relative - MSG * block
    place = jnp.where(far >= 0, jnp.where(block == 2, -1, remote), place).astype(jnp.float32)
    columns = [diagonal(place[k:k + 1, :]) for k in range(4)]
    hot = one_hot(jnp.concatenate(columns, axis=0), 8 * SLOTS)
    chosen = select_rows(hot, faces)
    ghosts = [chosen[k * SLOTS:(k + 1) * SLOTS] for k in range(4)]
    ghosts.append(vertical_in[0])
    ghosts.append(vertical_in[1])

    total = [0.0] * VARS
    at = lane((SLOTS, CELLS))
    for axis in range(3):
        stride = EDGE ** (2 - axis)
        position = (at >> (3 * (2 - axis))) & 7
        low = [jnp.where(position == 0, spread_face(ghosts[2 * axis], v, axis), pltpu.roll(cells[v], stride, 1))
               for v in range(VARS)]
        high = [jnp.where(position == EDGE - 1, spread_face(ghosts[2 * axis + 1], v, axis),
                          pltpu.roll(cells[v], CELLS - stride, 1)) for v in range(VARS)]
        flux_low, speed_low = axis_flux(low, primitives(low), axis)
        flux_high, speed_high = axis_flux(high, primitives(high), axis)
        speed_here = jnp.abs(velocity[axis]) + sound
        lower = jnp.maximum(speed_low, speed_here)
        upper = jnp.maximum(speed_here, speed_high)
        for v in range(VARS):
            total[v] = total[v] + 0.5 * (
                (flux_high[v] - flux_low[v]) - (upper * (high[v] - cells[v]) - lower * (cells[v] - low[v])))
    for v in range(VARS):
        change_ref[v] = total[v]

    @pl.when(has_below)
    def _():
        go_down.wait_send()

    @pl.when(has_above)
    def _():
        go_up.wait_send()

    for copy in lateral:
        copy.wait_send()

    def finish(highest):
        step = COURANT / jnp.max(highest, axis=1, keepdims=True)
        for v in range(VARS):
            updated_out[v] = jnp.where(live, cells_ref[v] - step * change_ref[v], 0.0)

    def of_hubs():
        return functools.reduce(jnp.maximum, [from_hubs[i] for i in range(nx)])

    for g in (0, 1):
        number = len(members[g]) * nx * 3 - 1

        @pl.when(is_hub & (group == g))
        def _(g=g, number=number):
            settle(from_plane, in_plane - 1, max_recv.at[0])
            plane_top = jnp.max(from_plane[pl.ds(0, in_plane)], axis=0)
            value[1] = plane_top
            from_hubs[x] = plane_top

            def tell(i, carry):
                py = i + members[1][0] if g else jnp.where(i < members[1][0], i, i + len(members[1]))
                for px in range(nx):
                    @pl.when((px != x) | (py != y))
                    def _(px=px):
                        push(value.at[1], from_hubs.at[x], device(px, py, 0, HUB), 1, 1)

                    push(value.at[1], from_hubs.at[x], device(px, py, 0, 1 - HUB), 1, 1)
                    push(value.at[1], from_hubs.at[x], device(px, py, 1, 1 - HUB), 1, 1)
                return carry

            lax.fori_loop(0, len(members[g]), tell, 0)
            settle(from_hubs, nx - 1, max_recv.at[1])
            finish(of_hubs())
            settle(from_plane, 1, max_send.at[0])
            settle(from_plane, number, max_send.at[1])

    @pl.when(is_listener)
    def _():
        settle(from_hubs, nx, max_recv.at[1])
        finish(of_hubs())
        settle(from_plane, 2, max_send.at[0])

    @pl.when(is_teller)
    def _():
        settle(from_hubs, nx, max_recv.at[1])
        over_all = of_hubs()
        value[2] = over_all
        push(value.at[2], result.at[0], device(x, y, 1, HUB), 2, 2)
        for pz in range(2, nz):
            for pc in (1, 0):
                push(value.at[2], result.at[0], device(x, y, pz, pc), 2, 2)
        finish(over_all)
        settle(from_plane, 2, max_send.at[0])
        settle(from_plane, 2 * nz - 3, max_send.at[2])

    @pl.when(is_other)
    def _():
        settle(result, 1, max_recv.at[2])
        finish(result[0])
        settle(from_plane, 2, max_send.at[0])


def per_device(sizes, state, patch_count, neighbour_table, send_table, ghost_table):
    nx, ny, nz, nc = sizes
    any_space = pl.BlockSpec(memory_space=pl.ANY)
    vmem = pl.BlockSpec(memory_space=pltpu.VMEM)
    f32 = jnp.float32
    dma = pltpu.SemaphoreType.DMA
    updated = pl.pallas_call(
        functools.partial(kernel, sizes),
        out_shape=pltpu.VMEM((VARS, SLOTS, CELLS), f32),
        in_specs=[any_space] * 4,
        out_specs=vmem,
        scratch_shapes=[
            pltpu.VMEM((VARS, SLOTS, CELLS), f32),
            pltpu.VMEM((4, SLOTS), jnp.int32),
            pltpu.VMEM((MSG, 1, nx * ny), jnp.int32),
            pltpu.VMEM((4, SLOTS), jnp.int32),
            pltpu.VMEM((2, SLOTS, WIDE), f32),
            pltpu.VMEM((2, SLOTS, WIDE), f32),
            pltpu.VMEM((4, SLOTS, WIDE), f32),
            pltpu.VMEM((4, SLOTS, WIDE), f32),
            pltpu.VMEM((VARS, SLOTS, CELLS), f32),
            pltpu.VMEM((3, 1, LANES), f32),
            pltpu.VMEM((max(2 * ny * nz, 3 * nx * ny), 1, LANES), f32),
            pltpu.VMEM((nx, 1, LANES), f32),
            pltpu.VMEM((1, 1, LANES), f32),
            dma, dma((3,)), dma, dma, dma((2,)), dma((4,)), dma((4,)), dma((3,)), dma((3,)),
        ],
        compiler_params=pltpu.CompilerParams(collective_id=0, has_side_effects=True),
        name="step",
    )(
        jnp.transpose(state, (0, 2, 1, 3)),
        jnp.transpose(neighbour_table, (0, 2, 1)),
        jnp.transpose(send_table, (2, 0, 1)),
        jnp.transpose(ghost_table, (0, 2, 1)),
    )
    return jnp.transpose(updated[None], (0, 2, 1, 3))


def solution(mesh):
    nx = ny = round((mesh.shape["morton"]) ** 0.5)
    sizes = (nx, ny, mesh.shape["group"] // 2, 2)
    torus = Mesh(mesh.devices.reshape(sizes), AXES)
    return jax.shard_map(
        functools.partial(per_device, sizes),
        mesh=torus,
        in_specs=(
            P(GROUP, MORTON, None, None),
            P(MORTON),
            P(MORTON, None, None),
            P(MORTON, None, None),
            P(MORTON, None, None),
        ),
        out_specs=P(GROUP, MORTON, None, None),
        check_vma=False,
    )
```

```python
import functools

import jax
import jax.numpy as jnp
from jax import lax
from jax.experimental import pallas as pl
from jax.experimental.pallas import tpu as pltpu
from jax.sharding import Mesh
from jax.sharding import PartitionSpec as P

EDGE = 8
VARS = 5
CELLS = EDGE * EDGE * EDGE
FACE = EDGE * EDGE
SLOTS = 8
MSG = 5
LANES = 128
WIDE = 384
GAMMA = 1.4
COURANT = 0.8
AXES = ("morton_0", "morton_1", "group_0", "group_1")
MORTON = ("morton_0", "morton_1")
GROUP = ("group_0", "group_1")
OFFSETS = (-2, -1, 1, 2)
HUB = 1


def primitives(cells):
    density, mx, my, mz, energy = cells
    inverse = 1.0 / density
    velocity = (mx * inverse, my * inverse, mz * inverse)
    kinetic = mx * velocity[0] + my * velocity[1] + mz * velocity[2]
    pressure = (GAMMA - 1.0) * (energy - 0.5 * kinetic)
    sound = jnp.sqrt(GAMMA * pressure * inverse)
    return velocity, pressure, sound


def axis_flux(cells, prims, axis):
    velocity, pressure, sound = prims
    normal = velocity[axis]
    parts = [cells[1 + axis]]
    for comp in range(3):
        term = cells[1 + comp] * normal
        parts.append(term + pressure if comp == axis else term)
    parts.append((cells[4] + pressure) * normal)
    return parts, jnp.abs(normal) + sound


def lane(shape):
    return lax.broadcasted_iota(jnp.int32, shape, 1)


def pick_lanes(tile, index):
    return jnp.take_along_axis(tile, index, axis=1, mode="promise_in_bounds")


def tiles_of(wide):
    return [wide[:, q * LANES:(q + 1) * LANES] for q in range(wide.shape[1] // LANES)]


def pack_face(cells, face):
    axis, far = face // 2, face % 2
    if axis == 0:
        parts = [v[:, CELLS - FACE:] if far else v[:, :FACE] for v in cells]
        parts.append(jnp.zeros((SLOTS, FACE), jnp.float32))
        return jnp.concatenate(parts, axis=1)
    at = lane((SLOTS, LANES))
    place = at & (FACE - 1)
    if axis == 1:
        source = ((place >> 3) & 1) * FACE + far * (FACE - EDGE) + (place & 7)
    else:
        source = (place & 15) * EDGE + far * (EDGE - 1)
    packed = []
    for v in cells:
        tiles = tiles_of(v)
        out = pick_lanes(tiles[0], source)
        for q in range(1, 4):
            out = jnp.where((place >> 4) == q, pick_lanes(tiles[q], source), out)
        packed.append(out)
    packed.append(jnp.zeros((SLOTS, LANES), jnp.float32))
    pairs = [jnp.where(at < FACE, packed[2 * j], packed[2 * j + 1]) for j in range(3)]
    return jnp.concatenate(pairs, axis=1)


def spread_face(packed, var, axis):
    tile = tiles_of(packed)[var // 2]
    base = (var % 2) * FACE
    at = lane((SLOTS, LANES))
    if axis == 0:
        one = pick_lanes(tile, base + (at & (FACE - 1)))
        return jnp.concatenate([one] * 4, axis=1)
    out = []
    for q in range(4):
        if axis == 1:
            index = base + q * 16 + (at >> 6) * EDGE + (at & 7)
        else:
            index = base + q * 16 + (at >> 3)
        out.append(pick_lanes(tile, index))
    return jnp.concatenate(out, axis=1)


def diagonal(row):
    shape = (SLOTS, SLOTS)
    keep = lax.broadcasted_iota(jnp.int32, shape, 0) == lane(shape)
    return jnp.sum(jnp.where(keep, jnp.broadcast_to(row, shape), 0.0), axis=1, keepdims=True)


def one_hot(column, width):
    places = lane((column.shape[0], width)).astype(jnp.float32)
    return (column == places).astype(jnp.float32)


def select_rows(hot, table):
    return jnp.dot(hot, table, precision=lax.Precision.HIGHEST, preferred_element_type=jnp.float32)


def late_sets(sizes):
    nx, ny, nz, nc = sizes
    late_x = [px for px in range(nx) if abs(px - nx // 2) <= nx // 8]
    late_y = [py for py in range(ny) if abs(py - ny // 2) <= ny // 4]
    return late_x, late_y, nz - nz // 2


def kernel(
    sizes,
    state, neighbour, send, ghost,
    updated_out,
    cells_ref, neighbour_ref, send_ref, ghost_ref,
    vertical_out, vertical_in, lateral_out, lateral_in, change_ref,
    value, from_plane, from_late, from_hubs, direct, result,
    load_sem, table_sem, up_sem, down_sem, vin_sem, lsend_sem, lin_sem, max_send, max_recv,
):
    nx, ny, nz, nc = sizes
    x, y, z, c = [lax.axis_index(a) for a in AXES]
    rank = x * ny + y
    ranks = nx * ny
    in_plane = 2 * ny * nz
    slab = z * nc + c
    has_below, has_above = slab > 0, slab < nz * nc - 1
    mid = ny // 2

    members = [[0], list(range(1, ny))]
    late_x, late_y, late_z = late_sets(sizes)
    n_late = len(late_y) * late_z * 2

    def device(px, py, pz, pc):
        return {"morton_0": px, "morton_1": py, "group_0": pz, "group_1": pc}

    def hub_of(px, group):
        return device(px, group * mid, 0, HUB)

    def at_rank(offset):
        j = lax.rem(rank + (offset + ranks), ranks)
        return device(lax.div(j, ny), lax.rem(j, ny), z, c)

    group = jnp.minimum(y, 1)

    def is_late(px, py, pz):
        return (px >= late_x[0]) & (px <= late_x[-1]) & (py >= late_y[0]) & (py <= late_y[-1]) & (pz >= nz - late_z)

    late = is_late(x, y, z)
    late_plane = (x >= late_x[0]) & (x <= late_x[-1])
    first_device = device(0, 0, 0, HUB)
    is_first_device = (x == 0) & (y == 0) & (z == 0) & (c == HUB)

    def key(px, py, pz, pc):
        hops = jnp.minimum(px, nx - px) + jnp.minimum(py, ny - py) + jnp.minimum(pz, nz - pz)
        far = lax.div(2 * px, nx) + lax.div(2 * py, ny) + lax.div(2 * pz, nz)
        number = ((pz * ny + py) * nx + px) * 2 + pc
        return (14 * number + 443 * hops + 620 * far - 420 * pc) * (2 * nx * ny * nz) + number

    my_key = key(x, y, z, c)

    def comes_later(p):
        return key(p["morton_0"], p["morton_1"], p["group_0"], p["group_1"]) > my_key

    is_hub = ((y == 0) | (y == mid)) & (z == 0) & (c == HUB)
    is_listener = (z == 0) & jnp.logical_not(is_hub)
    is_teller = (z == 1) & (c != HUB)
    is_other = (z > 1) | ((z == 1) & (c == HUB))
    other = 1 - c
    below = device(x, y, lax.rem(z + (nz - 1) + c, nz), other)
    above = device(x, y, lax.rem(z + c, nz), other)

    loads = [
        pltpu.make_async_copy(state.at[0, v], cells_ref.at[v], load_sem.at[v]) for v in range(VARS)
    ] + [
        pltpu.make_async_copy(neighbour.at[0], neighbour_ref, table_sem.at[0]),
        pltpu.make_async_copy(send, send_ref, table_sem.at[1]),
        pltpu.make_async_copy(ghost.at[0], ghost_ref, table_sem.at[2]),
    ]
    for load in loads:
        load.start()

    barrier = pltpu.get_barrier_semaphore()

    def greet(target):
        pl.semaphore_signal(barrier, inc=1, device_id=target, device_id_type=pl.DeviceIdType.MESH)

    beside = [at_rank(o) for o in OFFSETS]
    beside_later = [comes_later(p) for p in beside]
    below_later, above_later = has_below & comes_later(below), has_above & comes_later(above)
    below_earlier = has_below & jnp.logical_not(below_later)
    above_earlier = has_above & jnp.logical_not(above_later)
    partners = list(zip(beside + [below, above], beside_later + [below_later, above_later]))
    earlier = sum(jnp.logical_not(f).astype(jnp.int32) for f in beside_later)
    earlier = earlier + below_earlier.astype(jnp.int32) + above_earlier.astype(jnp.int32)

    for target, later in partners:
        @pl.when(later)
        def _(target=target):
            greet(target)

    @pl.when(is_hub)
    def _():
        def plane(i, carry):
            py, pz, pc = lax.rem(lax.div(i, 2), ny), lax.div(i, 2 * ny), lax.rem(i, 2)

            @pl.when((py != y) | (pz != 0) | (pc != HUB))
            def _():
                greet(device(x, py, pz, pc))

            return carry

        lax.fori_loop(0, in_plane, plane, 0)
        for step in range(1, nx):
            greet(hub_of(lax.rem(x + step, nx), group))

    @pl.when(is_first_device)
    def _():
        def late_one(i, carry):
            px = late_x[0] + lax.rem(lax.div(i, 2), len(late_x))
            rest = lax.div(i, 2 * len(late_x))
            greet(device(px, late_y[0] + lax.rem(rest, len(late_y)), nz - late_z + lax.div(rest, len(late_y)), lax.rem(i, 2)))
            return carry

        lax.fori_loop(0, len(late_x) * n_late, late_one, 0)

    @pl.when(is_listener | is_teller)
    def _():
        for px in range(nx):
            greet(hub_of(px, group))

    loads[VARS].wait()
    near = neighbour_ref[...]
    for v in range(VARS):
        loads[v].wait()
    in_row = diagonal(jnp.maximum(near[2:3, :], near[3:4, :]).astype(jnp.float32))
    live = jnp.broadcast_to(in_row, (SLOTS, CELLS)) >= 0.0
    cells = [cells_ref[v] for v in range(VARS)]
    prims = primitives(cells)
    velocity, pressure, sound = prims
    speed = jnp.abs(velocity[0]) + jnp.abs(velocity[1]) + jnp.abs(velocity[2]) + 3.0 * sound
    speed = jnp.where(live, speed, 0.0)
    top = jnp.max(functools.reduce(jnp.maximum, tiles_of(speed)), axis=0, keepdims=True)
    value[0] = top

    def push(source, target_ref, target, phase, arrival):
        pltpu.make_async_remote_copy(
            src_ref=source, dst_ref=target_ref, send_sem=max_send.at[phase], recv_sem=max_recv.at[arrival],
            device_id=target, device_id_type=pl.DeviceIdType.MESH).start()

    def settle(ref, number, sem):
        pltpu.make_async_copy(ref.at[pl.ds(0, number)], ref.at[pl.ds(0, number)], sem).wait()

    packed_z, others = z - (nz - late_z), ny - len(late_y)
    packed_y = jnp.where(y < late_y[0], y, y - len(late_y))
    mine = jnp.where(
        late_plane & (packed_z >= 0),
        ((nz - late_z) * ny + packed_z * others + packed_y) * 2 + c,
        (z * ny + y) * 2 + c,
    )


    @pl.when(is_hub)
    def _():
        from_plane[mine] = top
        told = jnp.where(group == 0, len(members[0]), len(members[1])) * nx * 3
        pl.semaphore_wait(barrier, told + earlier)
        push(value.at[0], from_plane.at[mine], hub_of(x, 1 - group), 0, 0)

    @pl.when(late)
    def _():
        place = ((z - (nz - late_z)) * len(late_y) + y - late_y[0]) * 2 + c
        pl.semaphore_wait(barrier, 3 + earlier)
        push(value.at[0], direct.at[(x - late_x[0]) * n_late + place], first_device, 0, 4)
        push(value.at[0], from_late.at[place], hub_of(x, 1), 0, 3)
        push(value.at[0], from_late.at[place], hub_of(x, 0), 0, 3)

    @pl.when(jnp.logical_not(is_hub | late))
    def _():
        pl.semaphore_wait(barrier, 2 + earlier)
        push(value.at[0], from_plane.at[mine], hub_of(x, 1), 0, 0)
        push(value.at[0], from_plane.at[mine], hub_of(x, 0), 0, 0)

    vertical_out[0] = pack_face(cells, 4)
    vertical_out[1] = pack_face(cells, 5)
    go_down = pltpu.make_async_remote_copy(
        src_ref=vertical_out.at[0], dst_ref=vertical_in.at[1], send_sem=down_sem, recv_sem=vin_sem.at[1],
        device_id=below, device_id_type=pl.DeviceIdType.MESH)
    go_up = pltpu.make_async_remote_copy(
        src_ref=vertical_out.at[1], dst_ref=vertical_in.at[0], send_sem=up_sem, recv_sem=vin_sem.at[0],
        device_id=above, device_id_type=pl.DeviceIdType.MESH)

    @pl.when(below_earlier)
    def _():
        go_down.start()

    @pl.when(above_earlier)
    def _():
        go_up.start()

    @pl.when(jnp.logical_not(has_below))
    def _():
        vertical_in[0] = vertical_out[0]

    @pl.when(jnp.logical_not(has_above))
    def _():
        vertical_in[1] = vertical_out[1]

    own = [pack_face(cells, face) for face in range(4)]
    own_rows = jnp.concatenate(own, axis=0)
    loads[VARS + 1].wait()
    rows = jnp.concatenate([send_ref[t] for t in range(MSG)] + [jnp.full((SLOTS - MSG, ranks), -1, jnp.int32)], axis=0)
    columns = []
    for offset in OFFSETS:
        j = lax.rem(rank + (offset + ranks), ranks)
        picked = jnp.where(lane((SLOTS, ranks)) == j, rows, 0).astype(jnp.float32)
        entry = jnp.sum(picked, axis=1, keepdims=True)
        entry_int = entry.astype(jnp.int32)
        row = jnp.where(entry_int >= 0, (entry_int & 3) * SLOTS + (entry_int >> 2), -1)
        columns.append(row.astype(jnp.float32))
    hot = one_hot(jnp.concatenate(columns, axis=0), 4 * SLOTS)
    messages = select_rows(hot, own_rows)
    for d in range(4):
        lateral_out[d] = messages[d * SLOTS:(d + 1) * SLOTS]
    lateral = [pltpu.make_async_remote_copy(
        src_ref=lateral_out.at[d], dst_ref=lateral_in.at[3 - d], send_sem=lsend_sem.at[d], recv_sem=lin_sem.at[3 - d],
        device_id=beside[d], device_id_type=pl.DeviceIdType.MESH) for d in range(4)]

    def arrived(d):
        return pltpu.make_async_remote_copy(
            src_ref=lateral_out.at[d], dst_ref=lateral_in.at[d], send_sem=lsend_sem.at[d], recv_sem=lin_sem.at[d],
            device_id=beside[d], device_id_type=pl.DeviceIdType.MESH)

    for d in range(4):
        @pl.when(jnp.logical_not(beside_later[d]))
        def _(d=d):
            lateral[d].start()

    for d in range(4):
        @pl.when(beside_later[d])
        def _(d=d):
            arrived(d).wait_recv()
            lateral[d].start()

    @pl.when(below_later)
    def _():
        go_up.wait_recv()
        go_down.start()

    @pl.when(above_later)
    def _():
        go_down.wait_recv()
        go_up.start()

    loads[VARS + 2].wait()

    for d in range(4):
        @pl.when(jnp.logical_not(beside_later[d]))
        def _(d=d):
            arrived(d).wait_recv()

    @pl.when(above_earlier)
    def _():
        go_down.wait_recv()

    @pl.when(below_earlier)
    def _():
        go_up.wait_recv()

    faces = jnp.concatenate([own_rows] + [lateral_in[d] for d in range(4)], axis=0)
    far = ghost_ref[...]
    face_id = lax.broadcasted_iota(jnp.int32, (4, SLOTS), 0)
    slot_id = lane((4, SLOTS))
    local = (near >= 0) & ((near >> 3) == rank)
    place = jnp.where(local, (face_id ^ 1) * SLOTS + (near & 7), face_id * SLOTS + slot_id)
    relative = far - rank * MSG + 2 * MSG
    block = sum((relative >= MSG * k).astype(jnp.int32) for k in range(1, 5))
    remote = 4 * SLOTS + SLOTS * (block - (block > 2).astype(jnp.int32)) + relative - MSG * block
    place = jnp.where(far >= 0, jnp.where(block == 2, -1, remote), place).astype(jnp.float32)
    columns = [diagonal(place[k:k + 1, :]) for k in range(4)]
    hot = one_hot(jnp.concatenate(columns, axis=0), 8 * SLOTS)
    chosen = select_rows(hot, faces)
    ghosts = [chosen[k * SLOTS:(k + 1) * SLOTS] for k in range(4)]
    ghosts.append(vertical_in[0])
    ghosts.append(vertical_in[1])

    total = [0.0] * VARS
    at = lane((SLOTS, CELLS))
    for axis in range(3):
        stride = EDGE ** (2 - axis)
        position = (at >> (3 * (2 - axis))) & 7
        low = [jnp.where(position == 0, spread_face(ghosts[2 * axis], v, axis), pltpu.roll(cells[v], stride, 1))
               for v in range(VARS)]
        high = [jnp.where(position == EDGE - 1, spread_face(ghosts[2 * axis + 1], v, axis),
                          pltpu.roll(cells[v], CELLS - stride, 1)) for v in range(VARS)]
        flux_low, speed_low = axis_flux(low, primitives(low), axis)
        flux_high, speed_high = axis_flux(high, primitives(high), axis)
        speed_here = jnp.abs(velocity[axis]) + sound
        lower = jnp.maximum(speed_low, speed_here)
        upper = jnp.maximum(speed_here, speed_high)
        for v in range(VARS):
            total[v] = total[v] + 0.5 * (
                (flux_high[v] - flux_low[v]) - (upper * (high[v] - cells[v]) - lower * (cells[v] - low[v])))
    for v in range(VARS):
        change_ref[v] = total[v]

    @pl.when(has_below)
    def _():
        go_down.wait_send()

    @pl.when(has_above)
    def _():
        go_up.wait_send()

    for copy in lateral:
        copy.wait_send()

    def finish(highest):
        step = COURANT / jnp.max(highest, axis=1, keepdims=True)
        for v in range(VARS):
            updated_out[v] = jnp.where(live, cells_ref[v] - step * change_ref[v], 0.0)

    def of_hubs():
        return functools.reduce(jnp.maximum, [from_hubs[i] for i in range(nx)])

    def plane_top_of(rows):
        return jnp.max(from_plane[pl.ds(0, rows)], axis=0)

    for g in (0, 1):
        number = len(members[g]) * nx * 3 - 1

        @pl.when(is_hub & (group == g))
        def _(g=g, number=number):
            @pl.when(jnp.logical_not(late_plane))
            def _():
                settle(from_plane, in_plane - 1, max_recv.at[0])
                value[1] = plane_top_of(in_plane)

            @pl.when(late_plane)
            def _():
                settle(from_plane, in_plane - n_late - 1, max_recv.at[0])
                value[2] = plane_top_of(in_plane - n_late)
                if g == 0:
                    push(value.at[2], from_hubs.at[x], first_device, 2, 1)
                settle(from_late, n_late, max_recv.at[3])
                value[1] = jnp.maximum(value[2], jnp.max(from_late[...], axis=0))

            from_hubs[x] = value[1]

            def tell(i, carry):
                py = i + members[g][0]
                for px in range(nx):
                    unless = (px != x) | (py != y)
                    if g == 0 and px == 0:
                        unless = unless & jnp.logical_not(late_plane)

                    @pl.when(unless)
                    def _(px=px):
                        push(value.at[1], from_hubs.at[x], device(px, py, 0, HUB), 1, 1)

                    push(value.at[1], from_hubs.at[x], device(px, py, 0, 1 - HUB), 1, 1)
                    push(value.at[1], from_hubs.at[x], device(px, py, 1, 1 - HUB), 1, 1)
                return carry

            lax.fori_loop(0, len(members[g]), tell, 0)
            settle(from_hubs, nx - 1, max_recv.at[1])
            if g == 0:
                @pl.when(is_first_device)
                def _():
                    settle(direct, len(late_x) * n_late, max_recv.at[4])
                    finish(jnp.maximum(of_hubs(), jnp.max(direct[...], axis=0)))

                @pl.when(jnp.logical_not(is_first_device))
                def _():
                    finish(of_hubs())

                @pl.when(late_plane)
                def _():
                    settle(from_plane, 1, max_send.at[2])
                    settle(from_plane, number - 1, max_send.at[1])

                @pl.when(jnp.logical_not(late_plane))
                def _():
                    settle(from_plane, number, max_send.at[1])
            else:
                finish(of_hubs())
                settle(from_plane, number, max_send.at[1])
            settle(from_plane, 1, max_send.at[0])

    @pl.when(is_listener)
    def _():
        settle(from_hubs, nx, max_recv.at[1])
        finish(of_hubs())

    @pl.when(is_teller)
    def _():
        settle(from_hubs, nx, max_recv.at[1])
        over_all = of_hubs()
        value[2] = over_all
        push(value.at[2], result.at[0], device(x, y, 1, HUB), 2, 2)
        for pz in range(2, nz):
            for pc in (1, 0):
                push(value.at[2], result.at[0], device(x, y, pz, pc), 2, 2)
        finish(over_all)
        settle(from_plane, 2 * nz - 3, max_send.at[2])

    @pl.when(is_other)
    def _():
        settle(result, 1, max_recv.at[2])
        finish(result[0])

    @pl.when(late)
    def _():
        settle(from_plane, 3, max_send.at[0])

    @pl.when(jnp.logical_not(is_hub | late))
    def _():
        settle(from_plane, 2, max_send.at[0])


def per_device(sizes, state, patch_count, neighbour_table, send_table, ghost_table):
    nx, ny, nz, nc = sizes
    late_x, late_y, late_z = late_sets(sizes)
    n_late = len(late_y) * late_z * 2
    any_space = pl.BlockSpec(memory_space=pl.ANY)
    vmem = pl.BlockSpec(memory_space=pltpu.VMEM)
    f32 = jnp.float32
    dma = pltpu.SemaphoreType.DMA
    updated = pl.pallas_call(
        functools.partial(kernel, sizes),
        out_shape=pltpu.VMEM((VARS, SLOTS, CELLS), f32),
        in_specs=[any_space] * 4,
        out_specs=vmem,
        scratch_shapes=[
            pltpu.VMEM((VARS, SLOTS, CELLS), f32),
            pltpu.VMEM((4, SLOTS), jnp.int32),
            pltpu.VMEM((MSG, 1, nx * ny), jnp.int32),
            pltpu.VMEM((4, SLOTS), jnp.int32),
            pltpu.VMEM((2, SLOTS, WIDE), f32),
            pltpu.VMEM((2, SLOTS, WIDE), f32),
            pltpu.VMEM((4, SLOTS, WIDE), f32),
            pltpu.VMEM((4, SLOTS, WIDE), f32),
            pltpu.VMEM((VARS, SLOTS, CELLS), f32),
            pltpu.VMEM((3, 1, LANES), f32),
            pltpu.VMEM((max(2 * ny * nz, 3 * nx * ny), 1, LANES), f32),
            pltpu.VMEM((n_late, 1, LANES), f32),
            pltpu.VMEM((nx, 1, LANES), f32),
            pltpu.VMEM((len(late_x) * n_late, 1, LANES), f32),
            pltpu.VMEM((1, 1, LANES), f32),
            dma((VARS,)), dma((3,)), dma, dma, dma((2,)), dma((4,)), dma((4,)), dma((3,)), dma((5,)),
        ],
        compiler_params=pltpu.CompilerParams(collective_id=0, has_side_effects=True),
        name="step",
    )(
        jnp.transpose(state, (0, 2, 1, 3)),
        jnp.transpose(neighbour_table, (0, 2, 1)),
        jnp.transpose(send_table, (2, 0, 1)),
        jnp.transpose(ghost_table, (0, 2, 1)),
    )
    return jnp.transpose(updated[None], (0, 2, 1, 3))


def solution(mesh):
    nx = ny = round((mesh.shape["morton"]) ** 0.5)
    sizes = (nx, ny, mesh.shape["group"] // 2, 2)
    torus = Mesh(mesh.devices.reshape(sizes), AXES)
    return jax.shard_map(
        functools.partial(per_device, sizes),
        mesh=torus,
        in_specs=(
            P(GROUP, MORTON, None, None),
            P(MORTON),
            P(MORTON, None, None),
            P(MORTON, None, None),
            P(MORTON, None, None),
        ),
        out_specs=P(GROUP, MORTON, None, None),
        check_vma=False,
    )
```

```python
import functools

import jax
import jax.numpy as jnp
from jax import lax
from jax.experimental import pallas as pl
from jax.experimental.pallas import tpu as pltpu
from jax.sharding import Mesh
from jax.sharding import PartitionSpec as P

EDGE = 8
VARS = 5
CELLS = EDGE * EDGE * EDGE
FACE = EDGE * EDGE
SLOTS = 8
MSG = 5
LANES = 128
WIDE = 384
GAMMA = 1.4
COURANT = 0.8
AXES = ("morton_0", "morton_1", "group_0", "group_1")
MORTON = ("morton_0", "morton_1")
GROUP = ("group_0", "group_1")
OFFSETS = (-2, -1, 1, 2)
HUB = 1


def primitives(cells):
    density, mx, my, mz, energy = cells
    inverse = 1.0 / density
    velocity = (mx * inverse, my * inverse, mz * inverse)
    kinetic = mx * velocity[0] + my * velocity[1] + mz * velocity[2]
    pressure = (GAMMA - 1.0) * (energy - 0.5 * kinetic)
    sound = jnp.sqrt(GAMMA * pressure * inverse)
    return velocity, pressure, sound


def axis_flux(cells, prims, axis):
    velocity, pressure, sound = prims
    normal = velocity[axis]
    parts = [cells[1 + axis]]
    for comp in range(3):
        term = cells[1 + comp] * normal
        parts.append(term + pressure if comp == axis else term)
    parts.append((cells[4] + pressure) * normal)
    return parts, jnp.abs(normal) + sound


def lane(shape):
    return lax.broadcasted_iota(jnp.int32, shape, 1)


def pick_lanes(tile, index):
    return jnp.take_along_axis(tile, index, axis=1, mode="promise_in_bounds")


def tiles_of(wide):
    return [wide[:, q * LANES:(q + 1) * LANES] for q in range(wide.shape[1] // LANES)]


def pack_face(cells, face):
    axis, far = face // 2, face % 2
    if axis == 0:
        parts = [v[:, CELLS - FACE:] if far else v[:, :FACE] for v in cells]
        parts.append(jnp.zeros((SLOTS, FACE), jnp.float32))
        return jnp.concatenate(parts, axis=1)
    at = lane((SLOTS, LANES))
    place = at & (FACE - 1)
    if axis == 1:
        source = ((place >> 3) & 1) * FACE + far * (FACE - EDGE) + (place & 7)
    else:
        source = (place & 15) * EDGE + far * (EDGE - 1)
    packed = []
    for v in cells:
        tiles = tiles_of(v)
        out = pick_lanes(tiles[0], source)
        for q in range(1, 4):
            out = jnp.where((place >> 4) == q, pick_lanes(tiles[q], source), out)
        packed.append(out)
    packed.append(jnp.zeros((SLOTS, LANES), jnp.float32))
    pairs = [jnp.where(at < FACE, packed[2 * j], packed[2 * j + 1]) for j in range(3)]
    return jnp.concatenate(pairs, axis=1)


def spread_face(packed, var, axis):
    tile = tiles_of(packed)[var // 2]
    base = (var % 2) * FACE
    at = lane((SLOTS, LANES))
    if axis == 0:
        one = pick_lanes(tile, base + (at & (FACE - 1)))
        return jnp.concatenate([one] * 4, axis=1)
    out = []
    for q in range(4):
        if axis == 1:
            index = base + q * 16 + (at >> 6) * EDGE + (at & 7)
        else:
            index = base + q * 16 + (at >> 3)
        out.append(pick_lanes(tile, index))
    return jnp.concatenate(out, axis=1)


def diagonal(row):
    shape = (SLOTS, SLOTS)
    keep = lax.broadcasted_iota(jnp.int32, shape, 0) == lane(shape)
    return jnp.sum(jnp.where(keep, jnp.broadcast_to(row, shape), 0.0), axis=1, keepdims=True)


def one_hot(column, width):
    places = lane((column.shape[0], width)).astype(jnp.float32)
    return (column == places).astype(jnp.float32)


def select_rows(hot, table):
    return jnp.dot(hot, table, precision=lax.Precision.HIGHEST, preferred_element_type=jnp.float32)


def early_and_late(sizes):
    nx, ny, nz, nc = sizes
    late_x = [px for px in range(nx) if abs(px - nx // 2) <= nx // 4]
    early = [(0, 0, HUB)] + [(px, py, pc) for px, py in ((1, 0), (0, 1)) for pc in (HUB, 1 - HUB) if px not in late_x]
    return early, late_x, nz - nz // 2


def kernel(
    sizes,
    state, neighbour, send, ghost,
    kept_out, change_out, top_out,
    cells_ref, neighbour_ref, send_ref, ghost_ref,
    vertical_out, vertical_in, lateral_out, lateral_in,
    value, from_plane, from_late, from_hubs, direct, result, overall,
    load_sem, table_sem, up_sem, down_sem, vin_sem, lsend_sem, lin_sem, max_send, max_recv,
):
    nx, ny, nz, nc = sizes
    x, y, z, c = [lax.axis_index(a) for a in AXES]
    rank = x * ny + y
    ranks = nx * ny
    in_plane = 2 * ny * nz
    slab = z * nc + c
    has_below, has_above = slab > 0, slab < nz * nc - 1
    mid = ny // 2

    members = [[0], list(range(1, ny))]
    early, late_x, late_z = early_and_late(sizes)
    n_late = ny * late_z * 2
    early_of = [[e for e in early if e[1] in members[g]] for g in (0, 1)]
    targets = 4 + (nz > 2)

    def device(px, py, pz, pc):
        return {"morton_0": px, "morton_1": py, "group_0": pz, "group_1": pc}

    def hub_of(px, group):
        return device(px, group * mid, 0, HUB)

    def at_rank(offset):
        j = lax.rem(rank + (offset + ranks), ranks)
        return device(lax.div(j, ny), lax.rem(j, ny), z, c)

    group = jnp.minimum(y, 1)

    late_plane = (x >= late_x[0]) & (x <= late_x[-1])
    late = late_plane & (z >= nz - late_z)
    is_early = functools.reduce(jnp.logical_or, [(x == px) & (y == py) & (c == pc) for px, py, pc in early]) & (z == 0)

    def key(px, py, pz, pc):
        hops = jnp.minimum(px, nx - px) + jnp.minimum(py, ny - py) + jnp.minimum(pz, nz - pz)
        far = lax.div(2 * px, nx) + lax.div(2 * py, ny) + lax.div(2 * pz, nz)
        number = ((pz * ny + py) * nx + px) * 2 + pc
        order = 14 * number + 443 * hops + 620 * far - 420 * pc
        return order * (2 * nx * ny * nz) + number

    my_key = key(x, y, z, c)

    def comes_later(p):
        return key(p["morton_0"], p["morton_1"], p["group_0"], p["group_1"]) > my_key

    is_hub = ((y == 0) | (y == mid)) & (z == 0) & (c == HUB)
    is_teller = (z == 2) & (c != HUB)
    is_listener = (z <= 1) & jnp.logical_not(is_hub)
    is_other = (z > 2) | ((z == 2) & (c == HUB))
    other = 1 - c
    below = device(x, y, lax.rem(z + (nz - 1) + c, nz), other)
    above = device(x, y, lax.rem(z + c, nz), other)

    loads = [
        pltpu.make_async_copy(state.at[0, v], cells_ref.at[v], load_sem.at[v]) for v in range(VARS)
    ] + [
        pltpu.make_async_copy(neighbour.at[0], neighbour_ref, table_sem.at[0]),
        pltpu.make_async_copy(send, send_ref, table_sem.at[1]),
        pltpu.make_async_copy(ghost.at[0], ghost_ref, table_sem.at[2]),
    ]
    for load in loads:
        load.start()

    barrier = pltpu.get_barrier_semaphore()

    def greet(target):
        pl.semaphore_signal(barrier, inc=1, device_id=target, device_id_type=pl.DeviceIdType.MESH)

    beside = [at_rank(o) for o in OFFSETS]
    beside_later = [comes_later(p) for p in beside]
    below_later, above_later = has_below & comes_later(below), has_above & comes_later(above)
    below_earlier = has_below & jnp.logical_not(below_later)
    above_earlier = has_above & jnp.logical_not(above_later)
    partners = list(zip(beside + [below, above], beside_later + [below_later, above_later]))
    earlier = sum(jnp.logical_not(f).astype(jnp.int32) for f in beside_later)
    earlier = earlier + below_earlier.astype(jnp.int32) + above_earlier.astype(jnp.int32)

    for target, later in partners:
        @pl.when(later)
        def _(target=target):
            greet(target)

    @pl.when(is_hub)
    def _():
        def plane(i, carry):
            py, pz, pc = lax.rem(lax.div(i, 2), ny), lax.div(i, 2 * ny), lax.rem(i, 2)

            @pl.when((py != y) | (pz != 0) | (pc != HUB))
            def _():
                greet(device(x, py, pz, pc))

            return carry

        lax.fori_loop(0, in_plane, plane, 0)
        for step in range(1, nx):
            greet(hub_of(lax.rem(x + step, nx), group))

    @pl.when(is_early)
    def _():
        def late_one(i, carry):
            px = late_x[0] + lax.rem(lax.div(i, 2), len(late_x))
            rest = lax.div(i, 2 * len(late_x))
            greet(device(px, lax.rem(rest, ny), nz - late_z + lax.div(rest, ny), lax.rem(i, 2)))
            return carry

        lax.fori_loop(0, len(late_x) * n_late, late_one, 0)

    @pl.when(is_listener | is_teller)
    def _():
        for px in range(nx):
            greet(hub_of(px, group))

    loads[VARS].wait()
    near = neighbour_ref[...]
    for v in range(VARS):
        loads[v].wait()
    in_row = diagonal(jnp.maximum(near[2:3, :], near[3:4, :]).astype(jnp.float32))
    live = jnp.broadcast_to(in_row, (SLOTS, CELLS)) >= 0.0
    cells = [cells_ref[v] for v in range(VARS)]
    prims = primitives(cells)
    velocity, pressure, sound = prims
    speed = jnp.abs(velocity[0]) + jnp.abs(velocity[1]) + jnp.abs(velocity[2]) + 3.0 * sound
    speed = jnp.where(live, speed, 0.0)
    top = jnp.max(functools.reduce(jnp.maximum, tiles_of(speed)), axis=0, keepdims=True)
    value[0] = top

    def push(source, target_ref, target, phase, arrival):
        pltpu.make_async_remote_copy(
            src_ref=source, dst_ref=target_ref, send_sem=max_send.at[phase], recv_sem=max_recv.at[arrival],
            device_id=target, device_id_type=pl.DeviceIdType.MESH).start()

    def settle(ref, number, sem):
        pltpu.make_async_copy(ref.at[pl.ds(0, number)], ref.at[pl.ds(0, number)], sem).wait()

    mine = (z * ny + y) * 2 + c

    @pl.when(is_hub)
    def _():
        from_plane[mine] = top
        told = jnp.where(group == 0, len(members[0]), len(members[1])) * nx * targets
        pl.semaphore_wait(barrier, told + earlier)
        push(value.at[0], from_plane.at[mine], hub_of(x, 1 - group), 0, 0)

    @pl.when(late)
    def _():
        place = mine - 2 * ny * (nz - late_z)
        to_early = ((z - (nz - late_z)) * len(late_x) + x - late_x[0]) * (2 * ny) + y * 2 + c
        pl.semaphore_wait(barrier, 2 + len(early) + earlier)
        for px, py, pc in early:
            push(value.at[0], direct.at[to_early], device(px, py, 0, pc), 0, 4 + (z == nz - 1).astype(jnp.int32))
        push(value.at[0], from_late.at[place], hub_of(x, 1), 0, 3)
        push(value.at[0], from_late.at[place], hub_of(x, 0), 0, 3)

    @pl.when(jnp.logical_not(is_hub | late))
    def _():
        pl.semaphore_wait(barrier, 2 + earlier)
        push(value.at[0], from_plane.at[mine], hub_of(x, 1), 0, 0)
        push(value.at[0], from_plane.at[mine], hub_of(x, 0), 0, 0)

    vertical_out[0] = pack_face(cells, 4)
    vertical_out[1] = pack_face(cells, 5)
    go_down = pltpu.make_async_remote_copy(
        src_ref=vertical_out.at[0], dst_ref=vertical_in.at[1], send_sem=down_sem, recv_sem=vin_sem.at[1],
        device_id=below, device_id_type=pl.DeviceIdType.MESH)
    go_up = pltpu.make_async_remote_copy(
        src_ref=vertical_out.at[1], dst_ref=vertical_in.at[0], send_sem=up_sem, recv_sem=vin_sem.at[0],
        device_id=above, device_id_type=pl.DeviceIdType.MESH)

    @pl.when(below_earlier)
    def _():
        go_down.start()

    @pl.when(above_earlier)
    def _():
        go_up.start()

    @pl.when(jnp.logical_not(has_below))
    def _():
        vertical_in[0] = vertical_out[0]

    @pl.when(jnp.logical_not(has_above))
    def _():
        vertical_in[1] = vertical_out[1]

    own = [pack_face(cells, face) for face in range(4)]
    own_rows = jnp.concatenate(own, axis=0)
    loads[VARS + 1].wait()
    rows = jnp.concatenate([send_ref[t] for t in range(MSG)] + [jnp.full((SLOTS - MSG, ranks), -1, jnp.int32)], axis=0)
    columns = []
    for offset in OFFSETS:
        j = lax.rem(rank + (offset + ranks), ranks)
        picked = jnp.where(lane((SLOTS, ranks)) == j, rows, 0).astype(jnp.float32)
        entry = jnp.sum(picked, axis=1, keepdims=True)
        entry_int = entry.astype(jnp.int32)
        row = jnp.where(entry_int >= 0, (entry_int & 3) * SLOTS + (entry_int >> 2), -1)
        columns.append(row.astype(jnp.float32))
    hot = one_hot(jnp.concatenate(columns, axis=0), 4 * SLOTS)
    messages = select_rows(hot, own_rows)
    for d in range(4):
        lateral_out[d] = messages[d * SLOTS:(d + 1) * SLOTS]
    lateral = [pltpu.make_async_remote_copy(
        src_ref=lateral_out.at[d], dst_ref=lateral_in.at[3 - d], send_sem=lsend_sem.at[d], recv_sem=lin_sem.at[3 - d],
        device_id=beside[d], device_id_type=pl.DeviceIdType.MESH) for d in range(4)]

    def arrived(d):
        return pltpu.make_async_remote_copy(
            src_ref=lateral_out.at[d], dst_ref=lateral_in.at[d], send_sem=lsend_sem.at[d], recv_sem=lin_sem.at[d],
            device_id=beside[d], device_id_type=pl.DeviceIdType.MESH)

    for d in range(4):
        @pl.when(jnp.logical_not(beside_later[d]))
        def _(d=d):
            lateral[d].start()

    for d in range(4):
        @pl.when(beside_later[d])
        def _(d=d):
            arrived(d).wait_recv()
            lateral[d].start()

    @pl.when(below_later)
    def _():
        go_up.wait_recv()
        go_down.start()

    @pl.when(above_later)
    def _():
        go_down.wait_recv()
        go_up.start()

    loads[VARS + 2].wait()

    for d in range(4):
        @pl.when(jnp.logical_not(beside_later[d]))
        def _(d=d):
            arrived(d).wait_recv()

    @pl.when(above_earlier)
    def _():
        go_down.wait_recv()

    @pl.when(below_earlier)
    def _():
        go_up.wait_recv()

    faces = jnp.concatenate([own_rows] + [lateral_in[d] for d in range(4)], axis=0)
    far = ghost_ref[...]
    face_id = lax.broadcasted_iota(jnp.int32, (4, SLOTS), 0)
    slot_id = lane((4, SLOTS))
    local = (near >= 0) & ((near >> 3) == rank)
    place = jnp.where(local, (face_id ^ 1) * SLOTS + (near & 7), face_id * SLOTS + slot_id)
    relative = far - rank * MSG + 2 * MSG
    block = sum((relative >= MSG * k).astype(jnp.int32) for k in range(1, 5))
    remote = 4 * SLOTS + SLOTS * (block - (block > 2).astype(jnp.int32)) + relative - MSG * block
    place = jnp.where(far >= 0, jnp.where(block == 2, -1, remote), place).astype(jnp.float32)
    columns = [diagonal(place[k:k + 1, :]) for k in range(4)]
    hot = one_hot(jnp.concatenate(columns, axis=0), 8 * SLOTS)
    chosen = select_rows(hot, faces)
    ghosts = [chosen[k * SLOTS:(k + 1) * SLOTS] for k in range(4)]
    ghosts.append(vertical_in[0])
    ghosts.append(vertical_in[1])

    total = [0.0] * VARS
    at = lane((SLOTS, CELLS))
    for axis in range(3):
        stride = EDGE ** (2 - axis)
        position = (at >> (3 * (2 - axis))) & 7
        low = [jnp.where(position == 0, spread_face(ghosts[2 * axis], v, axis), pltpu.roll(cells[v], stride, 1))
               for v in range(VARS)]
        high = [jnp.where(position == EDGE - 1, spread_face(ghosts[2 * axis + 1], v, axis),
                          pltpu.roll(cells[v], CELLS - stride, 1)) for v in range(VARS)]
        flux_low, speed_low = axis_flux(low, primitives(low), axis)
        flux_high, speed_high = axis_flux(high, primitives(high), axis)
        speed_here = jnp.abs(velocity[axis]) + sound
        lower = jnp.maximum(speed_low, speed_here)
        upper = jnp.maximum(speed_here, speed_high)
        for v in range(VARS):
            total[v] = total[v] + 0.5 * (
                (flux_high[v] - flux_low[v]) - (upper * (high[v] - cells[v]) - lower * (cells[v] - low[v])))
    for v in range(VARS):
        kept_out[v] = jnp.where(live, cells[v], 0.0)
        change_out[v] = jnp.where(live, total[v], 0.0)

    @pl.when(has_below)
    def _():
        go_down.wait_send()

    @pl.when(has_above)
    def _():
        go_up.wait_send()

    for copy in lateral:
        copy.wait_send()

    def finish(highest):
        top_out[...] = highest

    def of_hubs():
        return functools.reduce(jnp.maximum, [from_hubs[i] for i in range(nx)])

    def plane_top_of(rows):
        return jnp.max(from_plane[pl.ds(0, rows)], axis=0)

    def heard(number):
        settle(from_hubs, number, max_recv.at[1])
        overall[0] = of_hubs()

        @pl.when(is_early)
        def _():
            last = len(late_x) * ny * 2
            before = len(late_x) * n_late - last
            if before:
                settle(direct, before, max_recv.at[4])
                overall[0] = jnp.maximum(overall[0], jnp.max(direct[pl.ds(0, before)], axis=0))
            settle(direct, last, max_recv.at[5])
            overall[0] = jnp.maximum(overall[0], jnp.max(direct[pl.ds(before, last)], axis=0))

        return overall[0]

    for g in (0, 1):
        number = len(members[g]) * nx * targets - 1

        @pl.when(is_hub & (group == g))
        def _(g=g, number=number):
            @pl.when(jnp.logical_not(late_plane))
            def _():
                settle(from_plane, in_plane - 1, max_recv.at[0])
                value[1] = plane_top_of(in_plane)

            @pl.when(late_plane)
            def _():
                settle(from_plane, in_plane - n_late - 1, max_recv.at[0])
                value[2] = plane_top_of(in_plane - n_late)
                for px, py, pc in early_of[g]:
                    push(value.at[2], from_hubs.at[x], device(px, py, 0, pc), 2, 1)

                settle(from_late, n_late, max_recv.at[3])
                value[1] = jnp.maximum(value[2], jnp.max(from_late[...], axis=0))

            from_hubs[x] = value[1]

            def tell(px, py, pz, pc):
                push(value.at[1], from_hubs.at[x], device(px, py, pz, pc), 1, 1)

            def tell_z0(i, carry):
                py = i + members[g][0]
                for px in range(nx):
                    for pc in (HUB, 1 - HUB):
                        told = [ey for ex, ey, ec in early_of[g] if ex == px and ec == pc]
                        unless = []
                        if pc == HUB:
                            unless.append((px != x) | (py != y))
                        if told:
                            unless.append(jnp.logical_not(late_plane) | (py != told[0]))
                        if not unless:
                            tell(px, py, 0, pc)
                        else:
                            @pl.when(functools.reduce(jnp.logical_and, unless))
                            def _(px=px, pc=pc):
                                tell(px, py, 0, pc)
                return carry

            def tell_more(i, carry):
                py = i + members[g][0]
                for px in range(nx):
                    for pc in (HUB, 1 - HUB):
                        tell(px, py, 1, pc)
                    if nz > 2:
                        tell(px, py, 2, 1 - HUB)
                return carry

            lax.fori_loop(0, len(members[g]), tell_z0, 0)
            lax.fori_loop(0, len(members[g]), tell_more, 0)
            finish(heard(nx - 1))

            @pl.when(late_plane)
            def _():
                settle(from_plane, len(early_of[g]), max_send.at[2])
                settle(from_plane, number - len(early_of[g]), max_send.at[1])

            @pl.when(jnp.logical_not(late_plane))
            def _():
                settle(from_plane, number, max_send.at[1])

            settle(from_plane, 1, max_send.at[0])

    @pl.when(is_listener)
    def _():
        finish(heard(nx))

    if nz > 2:
        @pl.when(is_teller)
        def _():
            over_all = heard(nx)
            value[2] = over_all
            push(value.at[2], result.at[0], device(x, y, 2, HUB), 2, 2)
            for pz in range(3, nz):
                for pc in (HUB, 1 - HUB):
                    push(value.at[2], result.at[0], device(x, y, pz, pc), 2, 2)
            finish(over_all)
            settle(from_plane, 2 * nz - 5, max_send.at[2])

    @pl.when(is_other)
    def _():
        settle(result, 1, max_recv.at[2])
        finish(result[0])

    @pl.when(late)
    def _():
        settle(from_plane, 2 + len(early), max_send.at[0])

    @pl.when(jnp.logical_not(is_hub | late))
    def _():
        settle(from_plane, 2, max_send.at[0])


def apply_kernel(kept, change, top, updated, result, sems):
    step = COURANT / jnp.max(top[...], axis=1, keepdims=True)
    copies = []
    for v in range(VARS):
        result[v] = kept[v] - step * change[v]
        copies.append(pltpu.make_async_copy(result.at[v], updated.at[0, v], sems.at[v]))
        copies[-1].start()
    for copy in copies:
        copy.wait()


def per_device(sizes, state, patch_count, neighbour_table, send_table, ghost_table):
    nx, ny, nz, nc = sizes
    early, late_x, late_z = early_and_late(sizes)
    n_late = ny * late_z * 2
    any_space = pl.BlockSpec(memory_space=pl.ANY)
    vmem = pl.BlockSpec(memory_space=pltpu.VMEM)
    f32 = jnp.float32
    dma = pltpu.SemaphoreType.DMA
    block = pltpu.VMEM((VARS, SLOTS, CELLS), f32)
    kept, change, top = pl.pallas_call(
        functools.partial(kernel, sizes),
        out_shape=(block, block, pltpu.VMEM((1, LANES), f32)),
        in_specs=[any_space] * 4,
        out_specs=(vmem, vmem, vmem),
        scratch_shapes=[
            pltpu.VMEM((VARS, SLOTS, CELLS), f32),
            pltpu.VMEM((4, SLOTS), jnp.int32),
            pltpu.VMEM((MSG, 1, nx * ny), jnp.int32),
            pltpu.VMEM((4, SLOTS), jnp.int32),
            pltpu.VMEM((2, SLOTS, WIDE), f32),
            pltpu.VMEM((2, SLOTS, WIDE), f32),
            pltpu.VMEM((4, SLOTS, WIDE), f32),
            pltpu.VMEM((4, SLOTS, WIDE), f32),
            pltpu.VMEM((3, 1, LANES), f32),
            pltpu.VMEM((max(2 * ny * nz, 5 * nx * ny), 1, LANES), f32),
            pltpu.VMEM((n_late, 1, LANES), f32),
            pltpu.VMEM((nx, 1, LANES), f32),
            pltpu.VMEM((len(late_x) * n_late, 1, LANES), f32),
            pltpu.VMEM((1, 1, LANES), f32),
            pltpu.VMEM((1, 1, LANES), f32),
            dma((VARS,)), dma((3,)), dma, dma, dma((2,)), dma((4,)), dma((4,)), dma((3,)), dma((6,)),
        ],
        compiler_params=pltpu.CompilerParams(collective_id=0, has_side_effects=True),
        name="step",
    )(
        jnp.transpose(state, (0, 2, 1, 3)),
        jnp.transpose(neighbour_table, (0, 2, 1)),
        jnp.transpose(send_table, (2, 0, 1)),
        jnp.transpose(ghost_table, (0, 2, 1)),
    )
    updated = pl.pallas_call(
        apply_kernel,
        out_shape=jax.ShapeDtypeStruct((1, VARS, SLOTS, CELLS), f32),
        in_specs=[vmem] * 3,
        out_specs=any_space,
        scratch_shapes=[block, dma((VARS,))],
        name="apply",
    )(*[pltpu.with_memory_space_constraint(value, pltpu.VMEM) for value in (kept, change, top)])
    return jnp.transpose(updated, (0, 2, 1, 3))


def solution(mesh):
    nx = ny = round((mesh.shape["morton"]) ** 0.5)
    sizes = (nx, ny, mesh.shape["group"] // 2, 2)
    torus = Mesh(mesh.devices.reshape(sizes), AXES)
    return jax.shard_map(
        functools.partial(per_device, sizes),
        mesh=torus,
        in_specs=(
            P(GROUP, MORTON, None, None),
            P(MORTON),
            P(MORTON, None, None),
            P(MORTON, None, None),
            P(MORTON, None, None),
        ),
        out_specs=P(GROUP, MORTON, None, None),
        check_vma=False,
    )
```

```python
import functools

import jax
import jax.numpy as jnp
from jax import lax
from jax.experimental import pallas as pl
from jax.experimental.pallas import tpu as pltpu
from jax.sharding import Mesh
from jax.sharding import PartitionSpec as P

EDGE = 8
VARS = 5
CELLS = EDGE * EDGE * EDGE
FACE = EDGE * EDGE
SLOTS = 8
MSG = 5
LANES = 128
WIDE = 384
GAMMA = 1.4
COURANT = 0.8
AXES = ("morton_0", "morton_1", "group_0", "group_1")
MORTON = ("morton_0", "morton_1")
GROUP = ("group_0", "group_1")
OFFSETS = (-2, -1, 1, 2)
HUB = 1


def primitives(cells):
    density, mx, my, mz, energy = cells
    inverse = 1.0 / density
    velocity = (mx * inverse, my * inverse, mz * inverse)
    kinetic = mx * velocity[0] + my * velocity[1] + mz * velocity[2]
    pressure = (GAMMA - 1.0) * (energy - 0.5 * kinetic)
    sound = jnp.sqrt(GAMMA * pressure * inverse)
    return velocity, pressure, sound


def axis_flux(cells, prims, axis):
    velocity, pressure, sound = prims
    normal = velocity[axis]
    parts = [cells[1 + axis]]
    for comp in range(3):
        term = cells[1 + comp] * normal
        parts.append(term + pressure if comp == axis else term)
    parts.append((cells[4] + pressure) * normal)
    return parts, jnp.abs(normal) + sound


def lane(shape):
    return lax.broadcasted_iota(jnp.int32, shape, 1)


def pick_lanes(tile, index):
    return jnp.take_along_axis(tile, index, axis=1, mode="promise_in_bounds")


def tiles_of(wide):
    return [wide[:, q * LANES:(q + 1) * LANES] for q in range(wide.shape[1] // LANES)]


def pack_face(cells, face):
    axis, far = face // 2, face % 2
    if axis == 0:
        parts = [v[:, CELLS - FACE:] if far else v[:, :FACE] for v in cells]
        parts.append(jnp.zeros((SLOTS, FACE), jnp.float32))
        return jnp.concatenate(parts, axis=1)
    at = lane((SLOTS, LANES))
    place = at & (FACE - 1)
    if axis == 1:
        source = ((place >> 3) & 1) * FACE + far * (FACE - EDGE) + (place & 7)
    else:
        source = (place & 15) * EDGE + far * (EDGE - 1)
    packed = []
    for v in cells:
        tiles = tiles_of(v)
        out = pick_lanes(tiles[0], source)
        for q in range(1, 4):
            out = jnp.where((place >> 4) == q, pick_lanes(tiles[q], source), out)
        packed.append(out)
    packed.append(jnp.zeros((SLOTS, LANES), jnp.float32))
    pairs = [jnp.where(at < FACE, packed[2 * j], packed[2 * j + 1]) for j in range(3)]
    return jnp.concatenate(pairs, axis=1)


def spread_face(packed, var, axis):
    tile = tiles_of(packed)[var // 2]
    base = (var % 2) * FACE
    at = lane((SLOTS, LANES))
    if axis == 0:
        one = pick_lanes(tile, base + (at & (FACE - 1)))
        return jnp.concatenate([one] * 4, axis=1)
    out = []
    for q in range(4):
        if axis == 1:
            index = base + q * 16 + (at >> 6) * EDGE + (at & 7)
        else:
            index = base + q * 16 + (at >> 3)
        out.append(pick_lanes(tile, index))
    return jnp.concatenate(out, axis=1)


def diagonal(row):
    shape = (SLOTS, SLOTS)
    keep = lax.broadcasted_iota(jnp.int32, shape, 0) == lane(shape)
    return jnp.sum(jnp.where(keep, jnp.broadcast_to(row, shape), 0.0), axis=1, keepdims=True)


def one_hot(column, width):
    places = lane((column.shape[0], width)).astype(jnp.float32)
    return (column == places).astype(jnp.float32)


def select_rows(hot, table):
    return jnp.dot(hot, table, precision=lax.Precision.HIGHEST, preferred_element_type=jnp.float32)


def early_and_late(sizes):
    nx, ny, nz, nc = sizes
    late_x = [px for px in range(nx) if abs(px - nx // 2) <= nx // 4]
    early = [(0, 0, HUB)] + [(px, py, pc) for px, py in ((1, 0), (0, 1)) for pc in (HUB, 1 - HUB) if px not in late_x]
    return early, late_x, nz - nz // 2


def kernel(
    sizes,
    state, neighbour, send, ghost,
    kept_out, change_out, top_out,
    cells_ref, tables_ref, send_ref, halo_out, halo_in,
    value, from_plane, from_late, from_hubs, direct, result, overall,
    load_sem, table_sem, halo_sent, halo_arrived, max_sent, max_arrived, far_up, far_down,
):
    nx, ny, nz, nc = sizes
    x, y, z, c = [lax.axis_index(a) for a in AXES]
    rank = x * ny + y
    ranks = nx * ny
    in_plane = 2 * ny * nz
    slab = z * nc + c
    has_below, has_above = slab > 0, slab < nz * nc - 1
    mid = ny // 2

    members = [[0], list(range(1, ny))]
    early, late_x, late_z = early_and_late(sizes)
    n_late = ny * late_z * 2
    early_of = [[e for e in early if e[1] in members[g]] for g in (0, 1)]
    targets = 4 + (nz > 2)

    def device(px, py, pz, pc):
        return {"morton_0": px, "morton_1": py, "group_0": pz, "group_1": pc}

    def hub_of(px, group):
        return device(px, group * mid, 0, HUB)

    def at_rank(offset):
        j = lax.rem(rank + (offset + ranks), ranks)
        return device(lax.div(j, ny), lax.rem(j, ny), z, c)

    group = jnp.minimum(y, 1)

    late_plane = (x >= late_x[0]) & (x <= late_x[-1])
    late = late_plane & (z >= nz - late_z)
    is_early = functools.reduce(jnp.logical_or, [(x == px) & (y == py) & (c == pc) for px, py, pc in early]) & (z == 0)

    def key(px, py, pz, pc):
        hops = jnp.minimum(px, nx - px) + jnp.minimum(py, ny - py) + jnp.minimum(pz, nz - pz)
        far = lax.div(2 * px, nx) + lax.div(2 * py, ny) + lax.div(2 * pz, nz)
        number = ((pz * ny + py) * nx + px) * 2 + pc
        order = 14 * number + 443 * hops + 620 * far - 420 * pc
        return order * (2 * nx * ny * nz) + number

    my_key = key(x, y, z, c)

    def comes_later(p):
        return key(p["morton_0"], p["morton_1"], p["group_0"], p["group_1"]) > my_key

    is_hub = ((y == 0) | (y == mid)) & (z == 0) & (c == HUB)
    is_teller = (z == 2) & (c != HUB)
    is_listener = (z <= 1) & jnp.logical_not(is_hub)
    is_other = (z > 2) | ((z == 2) & (c == HUB))
    other = 1 - c
    below = device(x, y, lax.rem(z + (nz - 1) + c, nz), other)
    above = device(x, y, lax.rem(z + c, nz), other)

    loads = [pltpu.make_async_copy(state.at[0, v], cells_ref.at[v], load_sem) for v in range(VARS)] + [
        pltpu.make_async_copy(neighbour.at[0], tables_ref.at[0], table_sem.at[0]),
        pltpu.make_async_copy(ghost.at[0], tables_ref.at[1], table_sem.at[0]),
        pltpu.make_async_copy(send, send_ref, table_sem.at[1]),
    ]
    for load in loads:
        load.start()

    def settle(ref, number, sem):
        pltpu.make_async_copy(ref.at[pl.ds(0, number)], ref.at[pl.ds(0, number)], sem).wait()

    barrier = pltpu.get_barrier_semaphore()

    def greet(target):
        pl.semaphore_signal(barrier, inc=1, device_id=target, device_id_type=pl.DeviceIdType.MESH)

    beside = [at_rank(o) for o in OFFSETS]
    beside_later = [comes_later(p) for p in beside]
    below_later, above_later = has_below & comes_later(below), has_above & comes_later(above)
    below_earlier = has_below & jnp.logical_not(below_later)
    above_earlier = has_above & jnp.logical_not(above_later)
    partners = [(beside[d], beside_later[d]) for d in (1, 2)] + [(below, below_later), (above, above_later)]
    earlier = sum(jnp.logical_not(beside_later[d]).astype(jnp.int32) for d in (1, 2))
    earlier = earlier + below_earlier.astype(jnp.int32) + above_earlier.astype(jnp.int32)

    for target, later in partners:
        @pl.when(later)
        def _(target=target):
            greet(target)

    @pl.when(is_hub)
    def _():
        def plane(i, carry):
            py, pz, pc = lax.rem(lax.div(i, 2), ny), lax.div(i, 2 * ny), lax.rem(i, 2)

            @pl.when((py != y) | (pz != 0) | (pc != HUB))
            def _():
                greet(device(x, py, pz, pc))

            return carry

        lax.fori_loop(0, in_plane, plane, 0)
        for step in range(1, nx):
            greet(hub_of(lax.rem(x + step, nx), group))

    @pl.when(is_early)
    def _():
        def late_one(i, carry):
            px = late_x[0] + lax.rem(lax.div(i, 2), len(late_x))
            rest = lax.div(i, 2 * len(late_x))
            greet(device(px, lax.rem(rest, ny), nz - late_z + lax.div(rest, ny), lax.rem(i, 2)))
            return carry

        lax.fori_loop(0, len(late_x) * n_late, late_one, 0)

    @pl.when(is_listener | is_teller)
    def _():
        for px in range(nx):
            greet(hub_of(px, group))

    settle(tables_ref, 2, table_sem.at[0])
    near = tables_ref[0]
    settle(cells_ref, VARS, load_sem)
    in_row = diagonal(jnp.maximum(near[2:3, :], near[3:4, :]).astype(jnp.float32))
    live = jnp.broadcast_to(in_row, (SLOTS, CELLS)) >= 0.0
    cells = [cells_ref[v] for v in range(VARS)]
    prims = primitives(cells)
    velocity, pressure, sound = prims
    speed = jnp.abs(velocity[0]) + jnp.abs(velocity[1]) + jnp.abs(velocity[2]) + 3.0 * sound
    speed = jnp.where(live, speed, 0.0)
    top = jnp.max(functools.reduce(jnp.maximum, tiles_of(speed)), axis=0, keepdims=True)
    value[0] = top

    def push(source, target_ref, target, arrival):
        pltpu.make_async_remote_copy(
            src_ref=source, dst_ref=target_ref, send_sem=max_sent, recv_sem=max_arrived.at[arrival],
            device_id=target, device_id_type=pl.DeviceIdType.MESH).start()

    mine = (z * ny + y) * 2 + c

    @pl.when(is_hub)
    def _():
        from_plane[mine] = top
        told = jnp.where(group == 0, len(members[0]), len(members[1])) * nx * targets
        pl.semaphore_wait(barrier, told + earlier)
        push(value.at[0], from_plane.at[mine], hub_of(x, 1 - group), 0)

    @pl.when(late)
    def _():
        place = mine - 2 * ny * (nz - late_z)
        to_early = ((z - (nz - late_z)) * len(late_x) + x - late_x[0]) * (2 * ny) + y * 2 + c
        pl.semaphore_wait(barrier, 2 + len(early) + earlier)
        for px, py, pc in early:
            push(value.at[0], direct.at[to_early], device(px, py, 0, pc), 2 + (z == nz - 1).astype(jnp.int32))
        push(value.at[0], from_late.at[place], hub_of(x, 1), 2)
        push(value.at[0], from_late.at[place], hub_of(x, 0), 2)

    @pl.when(jnp.logical_not(is_hub | late))
    def _():
        pl.semaphore_wait(barrier, 2 + earlier)
        push(value.at[0], from_plane.at[mine], hub_of(x, 1), 0)
        push(value.at[0], from_plane.at[mine], hub_of(x, 0), 0)

    def to_partner(place, partner, at_theirs):
        return pltpu.make_async_remote_copy(
            src_ref=halo_out.at[place], dst_ref=halo_in.at[at_theirs], send_sem=halo_sent, recv_sem=halo_arrived.at[at_theirs],
            device_id=partner, device_id_type=pl.DeviceIdType.MESH)

    def arrived(place):
        pltpu.make_async_copy(halo_in.at[place], halo_in.at[place], halo_arrived.at[place]).wait()

    halo_out[4] = pack_face(cells, 4)
    halo_out[5] = pack_face(cells, 5)
    go_down, go_up = to_partner(4, below, 5), to_partner(5, above, 4)

    @pl.when(below_earlier)
    def _():
        go_down.start()

    @pl.when(above_earlier)
    def _():
        go_up.start()

    @pl.when(jnp.logical_not(has_below))
    def _():
        halo_in[4] = halo_out[4]

    @pl.when(jnp.logical_not(has_above))
    def _():
        halo_in[5] = halo_out[5]

    own = [pack_face(cells, face) for face in range(4)]
    own_rows = jnp.concatenate(own, axis=0)
    loads[-1].wait()
    rows = jnp.concatenate([send_ref[t] for t in range(MSG)] + [jnp.full((SLOTS - MSG, ranks), -1, jnp.int32)], axis=0)
    columns = []
    for offset in OFFSETS:
        j = lax.rem(rank + (offset + ranks), ranks)
        picked = jnp.where(lane((SLOTS, ranks)) == j, rows, 0).astype(jnp.float32)
        entry = jnp.sum(picked, axis=1, keepdims=True)
        entry_int = entry.astype(jnp.int32)
        row = jnp.where(entry_int >= 0, (entry_int & 3) * SLOTS + (entry_int >> 2), -1)
        columns.append(row.astype(jnp.float32))
    hot = one_hot(jnp.concatenate(columns, axis=0), 4 * SLOTS)
    messages = select_rows(hot, own_rows)
    for d in range(4):
        halo_out[d] = messages[d * SLOTS:(d + 1) * SLOTS]
    lateral = [to_partner(d, beside[d], 3 - d) for d in range(4)]

    for d in (1, 2):
        @pl.when(jnp.logical_not(beside_later[d]))
        def _(d=d):
            lateral[d].start()

    for d in (1, 2):
        @pl.when(beside_later[d])
        def _(d=d):
            arrived(d)
            lateral[d].start()

    pl.semaphore_signal(far_up, inc=1, device_id=beside[1], device_id_type=pl.DeviceIdType.MESH)
    pl.semaphore_signal(far_down, inc=1, device_id=beside[2], device_id_type=pl.DeviceIdType.MESH)

    @pl.when(below_later)
    def _():
        arrived(4)
        go_down.start()

    @pl.when(above_later)
    def _():
        arrived(5)
        go_up.start()

    pl.semaphore_wait(far_up, 1)
    lateral[3].start()
    pl.semaphore_wait(far_down, 1)
    lateral[0].start()


    for d in (1, 2):
        @pl.when(jnp.logical_not(beside_later[d]))
        def _(d=d):
            arrived(d)

    @pl.when(below_earlier)
    def _():
        arrived(4)

    @pl.when(above_earlier)
    def _():
        arrived(5)

    arrived(0)
    arrived(3)
    faces = jnp.concatenate([own_rows] + [halo_in[d] for d in range(4)], axis=0)
    far = tables_ref[1]
    face_id = lax.broadcasted_iota(jnp.int32, (4, SLOTS), 0)
    slot_id = lane((4, SLOTS))
    local = (near >= 0) & ((near >> 3) == rank)
    place = jnp.where(local, (face_id ^ 1) * SLOTS + (near & 7), face_id * SLOTS + slot_id)
    relative = far - rank * MSG + 2 * MSG
    block = sum((relative >= MSG * k).astype(jnp.int32) for k in range(1, 5))
    remote = 4 * SLOTS + SLOTS * (block - (block > 2).astype(jnp.int32)) + relative - MSG * block
    place = jnp.where(far >= 0, jnp.where(block == 2, -1, remote), place).astype(jnp.float32)
    columns = [diagonal(place[k:k + 1, :]) for k in range(4)]
    hot = one_hot(jnp.concatenate(columns, axis=0), 8 * SLOTS)
    chosen = select_rows(hot, faces)
    ghosts = [chosen[k * SLOTS:(k + 1) * SLOTS] for k in range(4)]
    ghosts.append(halo_in[4])
    ghosts.append(halo_in[5])

    total = [0.0] * VARS
    at = lane((SLOTS, CELLS))
    for axis in range(3):
        stride = EDGE ** (2 - axis)
        position = (at >> (3 * (2 - axis))) & 7
        low = [jnp.where(position == 0, spread_face(ghosts[2 * axis], v, axis), pltpu.roll(cells[v], stride, 1))
               for v in range(VARS)]
        high = [jnp.where(position == EDGE - 1, spread_face(ghosts[2 * axis + 1], v, axis),
                          pltpu.roll(cells[v], CELLS - stride, 1)) for v in range(VARS)]
        flux_low, speed_low = axis_flux(low, primitives(low), axis)
        flux_high, speed_high = axis_flux(high, primitives(high), axis)
        speed_here = jnp.abs(velocity[axis]) + sound
        lower = jnp.maximum(speed_low, speed_here)
        upper = jnp.maximum(speed_here, speed_high)
        for v in range(VARS):
            total[v] = total[v] + 0.5 * (
                (flux_high[v] - flux_low[v]) - (upper * (high[v] - cells[v]) - lower * (cells[v] - low[v])))
    for v in range(VARS):
        kept_out[v] = jnp.where(live, cells[v], 0.0)
        change_out[v] = jnp.where(live, total[v], 0.0)

    @pl.when(has_below & has_above)
    def _():
        settle(halo_out, 6, halo_sent)

    @pl.when(jnp.logical_not(has_below & has_above))
    def _():
        settle(halo_out, 5, halo_sent)

    def finish(highest):
        top_out[...] = highest

    def of_hubs():
        return functools.reduce(jnp.maximum, [from_hubs[i] for i in range(nx)])

    def plane_top_of(rows):
        return jnp.max(from_plane[pl.ds(0, rows)], axis=0)

    def heard(number):
        settle(from_hubs, number, max_arrived.at[1])
        overall[0] = of_hubs()

        @pl.when(is_early)
        def _():
            last = len(late_x) * ny * 2
            before = len(late_x) * n_late - last
            if before:
                settle(direct, before, max_arrived.at[2])
                overall[0] = jnp.maximum(overall[0], jnp.max(direct[pl.ds(0, before)], axis=0))
            settle(direct, last, max_arrived.at[3])
            overall[0] = jnp.maximum(overall[0], jnp.max(direct[pl.ds(before, last)], axis=0))

        return overall[0]

    for g in (0, 1):
        number = len(members[g]) * nx * targets - 1

        @pl.when(is_hub & (group == g))
        def _(g=g, number=number):
            @pl.when(jnp.logical_not(late_plane))
            def _():
                settle(from_plane, in_plane - 1, max_arrived.at[0])
                value[1] = plane_top_of(in_plane)

            @pl.when(late_plane)
            def _():
                settle(from_plane, in_plane - n_late - 1, max_arrived.at[0])
                value[2] = plane_top_of(in_plane - n_late)
                for px, py, pc in early_of[g]:
                    push(value.at[2], from_hubs.at[x], device(px, py, 0, pc), 1)

                settle(from_late, n_late, max_arrived.at[2])
                value[1] = jnp.maximum(value[2], jnp.max(from_late[...], axis=0))

            from_hubs[x] = value[1]

            def tell(px, py, pz, pc):
                push(value.at[1], from_hubs.at[x], device(px, py, pz, pc), 1)

            def tell_z0(i, carry):
                py = i + members[g][0]
                for px in range(nx):
                    for pc in (HUB, 1 - HUB):
                        told = [ey for ex, ey, ec in early_of[g] if ex == px and ec == pc]
                        unless = []
                        if pc == HUB:
                            unless.append((px != x) | (py != y))
                        if told:
                            unless.append(jnp.logical_not(late_plane) | (py != told[0]))
                        if not unless:
                            tell(px, py, 0, pc)
                        else:
                            @pl.when(functools.reduce(jnp.logical_and, unless))
                            def _(px=px, pc=pc):
                                tell(px, py, 0, pc)
                return carry

            def tell_more(i, carry):
                py = i + members[g][0]
                for px in range(nx):
                    for pc in (HUB, 1 - HUB):
                        tell(px, py, 1, pc)
                    if nz > 2:
                        tell(px, py, 2, 1 - HUB)
                return carry

            lax.fori_loop(0, len(members[g]), tell_z0, 0)
            lax.fori_loop(0, len(members[g]), tell_more, 0)
            finish(heard(nx - 1))
            settle(from_plane, number + 1, max_sent)

    @pl.when(is_listener)
    def _():
        finish(heard(nx))

    if nz > 2:
        @pl.when(is_teller)
        def _():
            over_all = heard(nx)
            value[2] = over_all
            push(value.at[2], result.at[0], device(x, y, 2, HUB), 1)
            for pz in range(3, nz):
                for pc in (HUB, 1 - HUB):
                    push(value.at[2], result.at[0], device(x, y, pz, pc), 1)
            finish(over_all)
            settle(from_plane, 2 + 2 * nz - 5, max_sent)

    @pl.when(is_other)
    def _():
        settle(result, 1, max_arrived.at[1])
        finish(result[0])

    @pl.when(late)
    def _():
        settle(from_plane, 2 + len(early), max_sent)

    @pl.when(jnp.logical_not(is_hub | late | (is_teller & (nz > 2))))
    def _():
        settle(from_plane, 2, max_sent)


def apply_kernel(kept, change, top, updated, result, sem):
    step = COURANT / jnp.max(top[...], axis=1, keepdims=True)
    for v in range(VARS):
        result[v] = kept[v] - step * change[v]
        pltpu.make_async_copy(result.at[v], updated.at[0, v], sem).start()
    pltpu.make_async_copy(result, updated.at[0], sem).wait()


def per_device(sizes, state, patch_count, neighbour_table, send_table, ghost_table):
    nx, ny, nz, nc = sizes
    early, late_x, late_z = early_and_late(sizes)
    n_late = ny * late_z * 2
    any_space = pl.BlockSpec(memory_space=pl.ANY)
    vmem = pl.BlockSpec(memory_space=pltpu.VMEM)
    f32 = jnp.float32
    dma = pltpu.SemaphoreType.DMA
    block = pltpu.VMEM((VARS, SLOTS, CELLS), f32)
    kept, change, top = pl.pallas_call(
        functools.partial(kernel, sizes),
        out_shape=(block, block, pltpu.VMEM((1, LANES), f32)),
        in_specs=[any_space] * 4,
        out_specs=(vmem, vmem, vmem),
        scratch_shapes=[
            pltpu.VMEM((VARS, SLOTS, CELLS), f32),
            pltpu.VMEM((2, 4, SLOTS), jnp.int32),
            pltpu.VMEM((MSG, 1, nx * ny), jnp.int32),
            pltpu.VMEM((6, SLOTS, WIDE), f32),
            pltpu.VMEM((6, SLOTS, WIDE), f32),
            pltpu.VMEM((3, 1, LANES), f32),
            pltpu.VMEM((max(2 * ny * nz, 5 * nx * ny), 1, LANES), f32),
            pltpu.VMEM((n_late, 1, LANES), f32),
            pltpu.VMEM((nx, 1, LANES), f32),
            pltpu.VMEM((len(late_x) * n_late, 1, LANES), f32),
            pltpu.VMEM((1, 1, LANES), f32),
            pltpu.VMEM((1, 1, LANES), f32),
            dma, dma((2,)), dma, dma((6,)), dma, dma((4,)), pltpu.SemaphoreType.REGULAR, pltpu.SemaphoreType.REGULAR,
        ],
        compiler_params=pltpu.CompilerParams(collective_id=0, has_side_effects=True),
        name="step",
    )(
        jnp.transpose(state, (0, 2, 1, 3)),
        jnp.transpose(neighbour_table, (0, 2, 1)),
        jnp.transpose(send_table, (2, 0, 1)),
        jnp.transpose(ghost_table, (0, 2, 1)),
    )
    updated = pl.pallas_call(
        apply_kernel,
        out_shape=jax.ShapeDtypeStruct((1, VARS, SLOTS, CELLS), f32),
        in_specs=[vmem] * 3,
        out_specs=any_space,
        scratch_shapes=[block, dma],
        name="apply",
    )(*[pltpu.with_memory_space_constraint(value, pltpu.VMEM) for value in (kept, change, top)])
    return jnp.transpose(updated, (0, 2, 1, 3))


def solution(mesh):
    nx = ny = round((mesh.shape["morton"]) ** 0.5)
    sizes = (nx, ny, mesh.shape["group"] // 2, 2)
    torus = Mesh(mesh.devices.reshape(sizes), AXES)
    return jax.shard_map(
        functools.partial(per_device, sizes),
        mesh=torus,
        in_specs=(
            P(GROUP, MORTON, None, None),
            P(MORTON),
            P(MORTON, None, None),
            P(MORTON, None, None),
            P(MORTON, None, None),
        ),
        out_specs=P(GROUP, MORTON, None, None),
        check_vma=False,
    )
```

```python
import functools

import jax
import jax.numpy as jnp
from jax import lax
from jax.experimental import pallas as pl
from jax.experimental.pallas import tpu as pltpu
from jax.sharding import Mesh
from jax.sharding import PartitionSpec as P

EDGE = 8
VARS = 5
CELLS = EDGE * EDGE * EDGE
FACE = EDGE * EDGE
SLOTS = 8
MSG = 5
LANES = 128
WIDE = 384
GAMMA = 1.4
COURANT = 0.8
AXES = ("morton_0", "morton_1", "group_0", "group_1")
MORTON = ("morton_0", "morton_1")
GROUP = ("group_0", "group_1")
OFFSETS = (-2, -1, 1, 2)
HUB = 1


def primitives(cells):
    density, mx, my, mz, energy = cells
    inverse = 1.0 / density
    velocity = (mx * inverse, my * inverse, mz * inverse)
    kinetic = mx * velocity[0] + my * velocity[1] + mz * velocity[2]
    pressure = (GAMMA - 1.0) * (energy - 0.5 * kinetic)
    sound = jnp.sqrt(GAMMA * pressure * inverse)
    return velocity, pressure, sound


def axis_flux(cells, prims, axis):
    velocity, pressure, sound = prims
    normal = velocity[axis]
    parts = [cells[1 + axis]]
    for comp in range(3):
        term = cells[1 + comp] * normal
        parts.append(term + pressure if comp == axis else term)
    parts.append((cells[4] + pressure) * normal)
    return parts, jnp.abs(normal) + sound


def lane(shape):
    return lax.broadcasted_iota(jnp.int32, shape, 1)


def pick_lanes(tile, index):
    return jnp.take_along_axis(tile, index, axis=1, mode="promise_in_bounds")


def tiles_of(wide):
    return [wide[:, q * LANES:(q + 1) * LANES] for q in range(wide.shape[1] // LANES)]


def pack_face(cells, face):
    axis, far = face // 2, face % 2
    if axis == 0:
        parts = [v[:, CELLS - FACE:] if far else v[:, :FACE] for v in cells]
        parts.append(jnp.zeros((SLOTS, FACE), jnp.float32))
        return jnp.concatenate(parts, axis=1)
    at = lane((SLOTS, LANES))
    place = at & (FACE - 1)
    if axis == 1:
        source = ((place >> 3) & 1) * FACE + far * (FACE - EDGE) + (place & 7)
    else:
        source = (place & 15) * EDGE + far * (EDGE - 1)
    packed = []
    for v in cells:
        tiles = tiles_of(v)
        out = pick_lanes(tiles[0], source)
        for q in range(1, 4):
            out = jnp.where((place >> 4) == q, pick_lanes(tiles[q], source), out)
        packed.append(out)
    packed.append(jnp.zeros((SLOTS, LANES), jnp.float32))
    pairs = [jnp.where(at < FACE, packed[2 * j], packed[2 * j + 1]) for j in range(3)]
    return jnp.concatenate(pairs, axis=1)


def spread_face(packed, var, axis):
    tile = tiles_of(packed)[var // 2]
    base = (var % 2) * FACE
    at = lane((SLOTS, LANES))
    if axis == 0:
        one = pick_lanes(tile, base + (at & (FACE - 1)))
        return jnp.concatenate([one] * 4, axis=1)
    out = []
    for q in range(4):
        if axis == 1:
            index = base + q * 16 + (at >> 6) * EDGE + (at & 7)
        else:
            index = base + q * 16 + (at >> 3)
        out.append(pick_lanes(tile, index))
    return jnp.concatenate(out, axis=1)


def diagonal(row):
    shape = (SLOTS, SLOTS)
    keep = lax.broadcasted_iota(jnp.int32, shape, 0) == lane(shape)
    return jnp.sum(jnp.where(keep, jnp.broadcast_to(row, shape), 0.0), axis=1, keepdims=True)


def one_hot(column, width):
    places = lane((column.shape[0], width)).astype(jnp.float32)
    return (column == places).astype(jnp.float32)


def select_rows(hot, table):
    return jnp.dot(hot, table, precision=lax.Precision.HIGHEST, preferred_element_type=jnp.float32)


def early_and_late(sizes):
    nx, ny, nz, nc = sizes
    late_x = [px for px in range(nx) if abs(px - nx // 2) <= nx // 4]
    early = [(0, 0, HUB)] + [(px, py, pc) for px, py in ((1, 0), (0, 1)) for pc in (HUB, 1 - HUB) if px not in late_x]
    return early, late_x, nz - nz // 2


def kernel(
    sizes,
    state, neighbour, send, ghost,
    kept_out, change_out, top_out,
    cells_ref, tables_ref, send_ref, halo_out, halo_in,
    value, from_plane, from_late, from_hubs, direct, result, overall,
    load_sem, table_sem, halo_sent, halo_arrived, max_sent, max_arrived, far,
):
    nx, ny, nz, nc = sizes
    x, y, z, c = [lax.axis_index(a) for a in AXES]
    rank = x * ny + y
    ranks = nx * ny
    in_plane = 2 * ny * nz
    slab = z * nc + c
    has_below, has_above = slab > 0, slab < nz * nc - 1
    mid = ny // 2

    members = [[0], list(range(1, ny))]
    early, late_x, late_z = early_and_late(sizes)
    n_late = ny * late_z * 2
    early_of = [[e for e in early if e[1] in members[g]] for g in (0, 1)]
    targets = 4 + (nz > 2)

    def device(px, py, pz, pc):
        return {"morton_0": px, "morton_1": py, "group_0": pz, "group_1": pc}

    def hub_of(px, group):
        return device(px, group * mid, 0, HUB)

    def at_rank(offset):
        j = lax.rem(rank + (offset + ranks), ranks)
        return device(lax.div(j, ny), lax.rem(j, ny), z, c)

    group = jnp.minimum(y, 1)

    late_plane = (x >= late_x[0]) & (x <= late_x[-1])
    late = late_plane & (z >= nz - late_z)
    is_early = functools.reduce(jnp.logical_or, [(x == px) & (y == py) & (c == pc) for px, py, pc in early]) & (z == 0)

    def key(px, py, pz, pc):
        hops = jnp.minimum(px, nx - px) + jnp.minimum(py, ny - py) + jnp.minimum(pz, nz - pz)
        far = lax.div(2 * px, nx) + lax.div(2 * py, ny) + lax.div(2 * pz, nz)
        number = ((pz * ny + py) * nx + px) * 2 + pc
        order = 14 * number + 443 * hops + 620 * far - 420 * pc
        return order * (2 * nx * ny * nz) + number

    my_key = key(x, y, z, c)

    def comes_later(p):
        return key(p["morton_0"], p["morton_1"], p["group_0"], p["group_1"]) > my_key

    is_hub = ((y == 0) | (y == mid)) & (z == 0) & (c == HUB)
    is_teller = (z == 2) & (c != HUB)
    is_listener = (z <= 1) & jnp.logical_not(is_hub)
    is_other = (z > 2) | ((z == 2) & (c == HUB))
    other = 1 - c
    below = device(x, y, lax.rem(z + (nz - 1) + c, nz), other)
    above = device(x, y, lax.rem(z + c, nz), other)

    loads = [pltpu.make_async_copy(state.at[0, v], cells_ref.at[v], load_sem) for v in range(VARS)] + [
        pltpu.make_async_copy(neighbour.at[0], tables_ref.at[0], table_sem.at[0]),
        pltpu.make_async_copy(ghost.at[0], tables_ref.at[1], table_sem.at[0]),
        pltpu.make_async_copy(send, send_ref, table_sem.at[1]),
    ]
    for load in loads:
        load.start()

    def settle(ref, number, sem):
        pltpu.make_async_copy(ref.at[pl.ds(0, number)], ref.at[pl.ds(0, number)], sem).wait()

    barrier = pltpu.get_barrier_semaphore()

    def greet(target):
        pl.semaphore_signal(barrier, inc=1, device_id=target, device_id_type=pl.DeviceIdType.MESH)

    beside = [at_rank(o) for o in OFFSETS]
    beside_later = [comes_later(p) for p in beside]
    below_later, above_later = has_below & comes_later(below), has_above & comes_later(above)
    below_earlier = has_below & jnp.logical_not(below_later)
    above_earlier = has_above & jnp.logical_not(above_later)
    partners = [(beside[d], beside_later[d]) for d in (1, 2)] + [(below, below_later), (above, above_later)]
    earlier = sum(jnp.logical_not(beside_later[d]).astype(jnp.int32) for d in (1, 2))
    earlier = earlier + below_earlier.astype(jnp.int32) + above_earlier.astype(jnp.int32)

    for target, later in partners:
        @pl.when(later)
        def _(target=target):
            greet(target)

    @pl.when(is_hub)
    def _():
        def plane(i, carry):
            py, pz, pc = lax.rem(lax.div(i, 2), ny), lax.div(i, 2 * ny), lax.rem(i, 2)

            @pl.when((py != y) | (pz != 0) | (pc != HUB))
            def _():
                greet(device(x, py, pz, pc))

            return carry

        lax.fori_loop(0, in_plane, plane, 0)
        for step in range(1, nx):
            greet(hub_of(lax.rem(x + step, nx), group))

    @pl.when(is_early)
    def _():
        def late_one(i, carry):
            px = late_x[0] + lax.rem(lax.div(i, 2), len(late_x))
            rest = lax.div(i, 2 * len(late_x))
            greet(device(px, lax.rem(rest, ny), nz - late_z + lax.div(rest, ny), lax.rem(i, 2)))
            return carry

        lax.fori_loop(0, len(late_x) * n_late, late_one, 0)

    @pl.when(is_listener | is_teller)
    def _():
        for px in range(nx):
            greet(hub_of(px, group))

    settle(tables_ref, 2, table_sem.at[0])
    near = tables_ref[0]
    settle(cells_ref, VARS, load_sem)
    in_row = diagonal(jnp.maximum(near[2:3, :], near[3:4, :]).astype(jnp.float32))
    live = jnp.broadcast_to(in_row, (SLOTS, CELLS)) >= 0.0
    cells = [cells_ref[v] for v in range(VARS)]
    prims = primitives(cells)
    velocity, pressure, sound = prims
    speed = jnp.abs(velocity[0]) + jnp.abs(velocity[1]) + jnp.abs(velocity[2]) + 3.0 * sound
    speed = jnp.where(live, speed, 0.0)
    top = jnp.max(functools.reduce(jnp.maximum, tiles_of(speed)), axis=0, keepdims=True)
    value[0] = top

    def push(source, target_ref, target, arrival):
        pltpu.make_async_remote_copy(
            src_ref=source, dst_ref=target_ref, send_sem=max_sent, recv_sem=max_arrived.at[arrival],
            device_id=target, device_id_type=pl.DeviceIdType.MESH).start()

    mine = (z * ny + y) * 2 + c

    @pl.when(is_hub)
    def _():
        from_plane[mine] = top
        told = jnp.where(group == 0, len(members[0]), len(members[1])) * nx * targets
        pl.semaphore_wait(barrier, told + earlier)
        push(value.at[0], from_plane.at[mine], hub_of(x, 1 - group), 0)

    @pl.when(late)
    def _():
        place = mine - 2 * ny * (nz - late_z)
        to_early = ((z - (nz - late_z)) * len(late_x) + x - late_x[0]) * (2 * ny) + y * 2 + c
        pl.semaphore_wait(barrier, 2 + len(early) + earlier)
        for px, py, pc in early:
            push(value.at[0], direct.at[to_early], device(px, py, 0, pc), 2 + (z == nz - 1).astype(jnp.int32))
        push(value.at[0], from_late.at[place], hub_of(x, 1), 2)
        push(value.at[0], from_late.at[place], hub_of(x, 0), 2)

    @pl.when(jnp.logical_not(is_hub | late))
    def _():
        pl.semaphore_wait(barrier, 2 + earlier)
        push(value.at[0], from_plane.at[mine], hub_of(x, 1), 0)
        push(value.at[0], from_plane.at[mine], hub_of(x, 0), 0)

    def to_partner(place, partner, at_theirs, later):
        which = 1 if later is None else later.astype(jnp.int32)
        return pltpu.make_async_remote_copy(
            src_ref=halo_out.at[place], dst_ref=halo_in.at[at_theirs], send_sem=halo_sent, recv_sem=halo_arrived.at[which],
            device_id=partner, device_id_type=pl.DeviceIdType.MESH)

    def arrived(number, most, which):
        for k in range(most + 1):
            if k:
                @pl.when(number == k)
                def _(k=k):
                    settle(halo_in, k, halo_arrived.at[which])

    halo_out[4] = pack_face(cells, 4)
    halo_out[5] = pack_face(cells, 5)
    go_down, go_up = to_partner(4, below, 5, below_later), to_partner(5, above, 4, above_later)

    @pl.when(below_earlier)
    def _():
        go_down.start()

    @pl.when(above_earlier)
    def _():
        go_up.start()

    @pl.when(jnp.logical_not(has_below))
    def _():
        halo_in[4] = halo_out[4]

    @pl.when(jnp.logical_not(has_above))
    def _():
        halo_in[5] = halo_out[5]

    own = [pack_face(cells, face) for face in range(4)]
    own_rows = jnp.concatenate(own, axis=0)
    loads[-1].wait()
    rows = jnp.concatenate([send_ref[t] for t in range(MSG)] + [jnp.full((SLOTS - MSG, ranks), -1, jnp.int32)], axis=0)
    columns = []
    for offset in OFFSETS:
        j = lax.rem(rank + (offset + ranks), ranks)
        picked = jnp.where(lane((SLOTS, ranks)) == j, rows, 0).astype(jnp.float32)
        entry = jnp.sum(picked, axis=1, keepdims=True)
        entry_int = entry.astype(jnp.int32)
        row = jnp.where(entry_int >= 0, (entry_int & 3) * SLOTS + (entry_int >> 2), -1)
        columns.append(row.astype(jnp.float32))
    hot = one_hot(jnp.concatenate(columns, axis=0), 4 * SLOTS)
    messages = select_rows(hot, own_rows)
    for d in range(4):
        halo_out[d] = messages[d * SLOTS:(d + 1) * SLOTS]
    lateral = [to_partner(d, beside[d], 3 - d, beside_later[d] if d in (1, 2) else None) for d in range(4)]

    for d in (1, 2):
        @pl.when(jnp.logical_not(beside_later[d]))
        def _(d=d):
            lateral[d].start()

    later = sum(flag.astype(jnp.int32) for _, flag in partners)
    arrived(later, 4, 0)
    for d in (1, 2):
        @pl.when(beside_later[d])
        def _(d=d):
            lateral[d].start()

    for d in (1, 2):
        pl.semaphore_signal(far, inc=1, device_id=beside[d], device_id_type=pl.DeviceIdType.MESH)

    @pl.when(below_later)
    def _():
        go_down.start()

    @pl.when(above_later)
    def _():
        go_up.start()

    pl.semaphore_wait(far, 2)
    lateral[3].start()
    lateral[0].start()


    arrived(earlier + 2, 6, 1)
    faces = jnp.concatenate([own_rows] + [halo_in[d] for d in range(4)], axis=0)
    sent_from = tables_ref[1]
    face_id = lax.broadcasted_iota(jnp.int32, (4, SLOTS), 0)
    slot_id = lane((4, SLOTS))
    local = (near >= 0) & ((near >> 3) == rank)
    place = jnp.where(local, (face_id ^ 1) * SLOTS + (near & 7), face_id * SLOTS + slot_id)
    relative = sent_from - rank * MSG + 2 * MSG
    block = sum((relative >= MSG * k).astype(jnp.int32) for k in range(1, 5))
    remote = 4 * SLOTS + SLOTS * (block - (block > 2).astype(jnp.int32)) + relative - MSG * block
    place = jnp.where(sent_from >= 0, jnp.where(block == 2, -1, remote), place).astype(jnp.float32)
    columns = [diagonal(place[k:k + 1, :]) for k in range(4)]
    hot = one_hot(jnp.concatenate(columns, axis=0), 8 * SLOTS)
    chosen = select_rows(hot, faces)
    ghosts = [chosen[k * SLOTS:(k + 1) * SLOTS] for k in range(4)]
    ghosts.append(halo_in[4])
    ghosts.append(halo_in[5])

    total = [0.0] * VARS
    at = lane((SLOTS, CELLS))
    for axis in range(3):
        stride = EDGE ** (2 - axis)
        position = (at >> (3 * (2 - axis))) & 7
        low = [jnp.where(position == 0, spread_face(ghosts[2 * axis], v, axis), pltpu.roll(cells[v], stride, 1))
               for v in range(VARS)]
        high = [jnp.where(position == EDGE - 1, spread_face(ghosts[2 * axis + 1], v, axis),
                          pltpu.roll(cells[v], CELLS - stride, 1)) for v in range(VARS)]
        flux_low, speed_low = axis_flux(low, primitives(low), axis)
        flux_high, speed_high = axis_flux(high, primitives(high), axis)
        speed_here = jnp.abs(velocity[axis]) + sound
        lower = jnp.maximum(speed_low, speed_here)
        upper = jnp.maximum(speed_here, speed_high)
        for v in range(VARS):
            total[v] = total[v] + 0.5 * (
                (flux_high[v] - flux_low[v]) - (upper * (high[v] - cells[v]) - lower * (cells[v] - low[v])))
    for v in range(VARS):
        kept_out[v] = jnp.where(live, cells[v], 0.0)
        change_out[v] = jnp.where(live, total[v], 0.0)

    @pl.when(has_below & has_above)
    def _():
        settle(halo_out, 6, halo_sent)

    @pl.when(jnp.logical_not(has_below & has_above))
    def _():
        settle(halo_out, 5, halo_sent)

    def finish(highest):
        top_out[...] = highest

    def of_hubs():
        return functools.reduce(jnp.maximum, [from_hubs[i] for i in range(nx)])

    def plane_top_of(rows):
        return jnp.max(from_plane[pl.ds(0, rows)], axis=0)

    def heard(number):
        settle(from_hubs, number, max_arrived.at[1])
        overall[0] = of_hubs()

        @pl.when(is_early)
        def _():
            last = len(late_x) * ny * 2
            before = len(late_x) * n_late - last
            if before:
                settle(direct, before, max_arrived.at[2])
                overall[0] = jnp.maximum(overall[0], jnp.max(direct[pl.ds(0, before)], axis=0))
            settle(direct, last, max_arrived.at[3])
            overall[0] = jnp.maximum(overall[0], jnp.max(direct[pl.ds(before, last)], axis=0))

        return overall[0]

    for g in (0, 1):
        number = len(members[g]) * nx * targets - 1

        @pl.when(is_hub & (group == g))
        def _(g=g, number=number):
            @pl.when(jnp.logical_not(late_plane))
            def _():
                settle(from_plane, in_plane - 1, max_arrived.at[0])
                value[1] = plane_top_of(in_plane)

            @pl.when(late_plane)
            def _():
                settle(from_plane, in_plane - n_late - 1, max_arrived.at[0])
                value[2] = plane_top_of(in_plane - n_late)
                for px, py, pc in early_of[g]:
                    push(value.at[2], from_hubs.at[x], device(px, py, 0, pc), 1)

                settle(from_late, n_late, max_arrived.at[2])
                value[1] = jnp.maximum(value[2], jnp.max(from_late[...], axis=0))

            from_hubs[x] = value[1]

            def tell(px, py, pz, pc):
                push(value.at[1], from_hubs.at[x], device(px, py, pz, pc), 1)

            def tell_z0(i, carry):
                py = i + members[g][0]
                for px in range(nx):
                    for pc in (HUB, 1 - HUB):
                        told = [ey for ex, ey, ec in early_of[g] if ex == px and ec == pc]
                        unless = []
                        if pc == HUB:
                            unless.append((px != x) | (py != y))
                        if told:
                            unless.append(jnp.logical_not(late_plane) | (py != told[0]))
                        if not unless:
                            tell(px, py, 0, pc)
                        else:
                            @pl.when(functools.reduce(jnp.logical_and, unless))
                            def _(px=px, pc=pc):
                                tell(px, py, 0, pc)
                return carry

            def tell_more(i, carry):
                py = i + members[g][0]
                for px in range(nx):
                    for pc in (HUB, 1 - HUB):
                        tell(px, py, 1, pc)
                    if nz > 2:
                        tell(px, py, 2, 1 - HUB)
                return carry

            lax.fori_loop(0, len(members[g]), tell_z0, 0)
            lax.fori_loop(0, len(members[g]), tell_more, 0)
            finish(heard(nx - 1))
            settle(from_plane, number + 1, max_sent)

    @pl.when(is_listener)
    def _():
        finish(heard(nx))

    if nz > 2:
        @pl.when(is_teller)
        def _():
            over_all = heard(nx)
            value[2] = over_all
            push(value.at[2], result.at[0], device(x, y, 2, HUB), 1)
            for pz in range(3, nz):
                for pc in (HUB, 1 - HUB):
                    push(value.at[2], result.at[0], device(x, y, pz, pc), 1)
            finish(over_all)
            settle(from_plane, 2 + 2 * nz - 5, max_sent)

    @pl.when(is_other)
    def _():
        settle(result, 1, max_arrived.at[1])
        finish(result[0])

    @pl.when(late)
    def _():
        settle(from_plane, 2 + len(early), max_sent)

    @pl.when(jnp.logical_not(is_hub | late | (is_teller & (nz > 2))))
    def _():
        settle(from_plane, 2, max_sent)


def apply_kernel(kept, change, top, updated, result, sem):
    step = COURANT / jnp.max(top[...], axis=1, keepdims=True)
    for v in range(VARS):
        result[v] = kept[v] - step * change[v]
        pltpu.make_async_copy(result.at[v], updated.at[0, v], sem).start()
    pltpu.make_async_copy(result, updated.at[0], sem).wait()


def per_device(sizes, state, patch_count, neighbour_table, send_table, ghost_table):
    nx, ny, nz, nc = sizes
    early, late_x, late_z = early_and_late(sizes)
    n_late = ny * late_z * 2
    any_space = pl.BlockSpec(memory_space=pl.ANY)
    vmem = pl.BlockSpec(memory_space=pltpu.VMEM)
    f32 = jnp.float32
    dma = pltpu.SemaphoreType.DMA
    block = pltpu.VMEM((VARS, SLOTS, CELLS), f32)
    kept, change, top = pl.pallas_call(
        functools.partial(kernel, sizes),
        out_shape=(block, block, pltpu.VMEM((1, LANES), f32)),
        in_specs=[any_space] * 4,
        out_specs=(vmem, vmem, vmem),
        scratch_shapes=[
            pltpu.VMEM((VARS, SLOTS, CELLS), f32),
            pltpu.VMEM((2, 4, SLOTS), jnp.int32),
            pltpu.VMEM((MSG, 1, nx * ny), jnp.int32),
            pltpu.VMEM((6, SLOTS, WIDE), f32),
            pltpu.VMEM((6, SLOTS, WIDE), f32),
            pltpu.VMEM((3, 1, LANES), f32),
            pltpu.VMEM((max(2 * ny * nz, 5 * nx * ny), 1, LANES), f32),
            pltpu.VMEM((n_late, 1, LANES), f32),
            pltpu.VMEM((nx, 1, LANES), f32),
            pltpu.VMEM((len(late_x) * n_late, 1, LANES), f32),
            pltpu.VMEM((1, 1, LANES), f32),
            pltpu.VMEM((1, 1, LANES), f32),
            dma, dma((2,)), dma, dma((2,)), dma, dma((4,)), pltpu.SemaphoreType.REGULAR,
        ],
        compiler_params=pltpu.CompilerParams(collective_id=0, has_side_effects=True),
        name="step",
    )(
        jnp.transpose(state, (0, 2, 1, 3)),
        jnp.transpose(neighbour_table, (0, 2, 1)),
        jnp.transpose(send_table, (2, 0, 1)),
        jnp.transpose(ghost_table, (0, 2, 1)),
    )
    updated = pl.pallas_call(
        apply_kernel,
        out_shape=jax.ShapeDtypeStruct((1, VARS, SLOTS, CELLS), f32),
        in_specs=[vmem] * 3,
        out_specs=any_space,
        scratch_shapes=[block, dma],
        name="apply",
    )(*[pltpu.with_memory_space_constraint(value, pltpu.VMEM) for value in (kept, change, top)])
    return jnp.transpose(updated, (0, 2, 1, 3))


def solution(mesh):
    nx = ny = round((mesh.shape["morton"]) ** 0.5)
    sizes = (nx, ny, mesh.shape["group"] // 2, 2)
    torus = Mesh(mesh.devices.reshape(sizes), AXES)
    return jax.shard_map(
        functools.partial(per_device, sizes),
        mesh=torus,
        in_specs=(
            P(GROUP, MORTON, None, None),
            P(MORTON),
            P(MORTON, None, None),
            P(MORTON, None, None),
            P(MORTON, None, None),
        ),
        out_specs=P(GROUP, MORTON, None, None),
        check_vma=False,
    )
```

```python
import functools

import jax
import jax.numpy as jnp
from jax import lax
from jax.experimental import pallas as pl
from jax.experimental.pallas import tpu as pltpu
from jax.sharding import Mesh
from jax.sharding import PartitionSpec as P

EDGE = 8
VARS = 5
CELLS = EDGE * EDGE * EDGE
FACE = EDGE * EDGE
SLOTS = 8
MSG = 5
LANES = 128
WIDE = 384
GAMMA = 1.4
COURANT = 0.8
AXES = ("morton_0", "morton_1", "group_0", "group_1")
MORTON = ("morton_0", "morton_1")
GROUP = ("group_0", "group_1")
OFFSETS = (-2, -1, 1, 2)
HUB = 1


def primitives(cells):
    density, mx, my, mz, energy = cells
    inverse = 1.0 / density
    velocity = (mx * inverse, my * inverse, mz * inverse)
    kinetic = mx * velocity[0] + my * velocity[1] + mz * velocity[2]
    pressure = (GAMMA - 1.0) * (energy - 0.5 * kinetic)
    sound = jnp.sqrt(GAMMA * pressure * inverse)
    return velocity, pressure, sound


def axis_flux(cells, prims, axis):
    velocity, pressure, sound = prims
    normal = velocity[axis]
    parts = [cells[1 + axis]]
    for comp in range(3):
        term = cells[1 + comp] * normal
        parts.append(term + pressure if comp == axis else term)
    parts.append((cells[4] + pressure) * normal)
    return parts, jnp.abs(normal) + sound


def lane(shape):
    return lax.broadcasted_iota(jnp.int32, shape, 1)


def pick_lanes(tile, index):
    return jnp.take_along_axis(tile, index, axis=1, mode="promise_in_bounds")


def tiles_of(wide):
    return [wide[:, q * LANES:(q + 1) * LANES] for q in range(wide.shape[1] // LANES)]


def pack_face(cells, face):
    axis, far = face // 2, face % 2
    if axis == 0:
        parts = [v[:, CELLS - FACE:] if far else v[:, :FACE] for v in cells]
        parts.append(jnp.zeros((SLOTS, FACE), jnp.float32))
        return jnp.concatenate(parts, axis=1)
    at = lane((SLOTS, LANES))
    place = at & (FACE - 1)
    if axis == 1:
        source = ((place >> 3) & 1) * FACE + far * (FACE - EDGE) + (place & 7)
    else:
        source = (place & 15) * EDGE + far * (EDGE - 1)
    packed = []
    for v in cells:
        tiles = tiles_of(v)
        out = pick_lanes(tiles[0], source)
        for q in range(1, 4):
            out = jnp.where((place >> 4) == q, pick_lanes(tiles[q], source), out)
        packed.append(out)
    packed.append(jnp.zeros((SLOTS, LANES), jnp.float32))
    pairs = [jnp.where(at < FACE, packed[2 * j], packed[2 * j + 1]) for j in range(3)]
    return jnp.concatenate(pairs, axis=1)


def spread_face(packed, var, axis):
    tile = tiles_of(packed)[var // 2]
    base = (var % 2) * FACE
    at = lane((SLOTS, LANES))
    if axis == 0:
        one = pick_lanes(tile, base + (at & (FACE - 1)))
        return jnp.concatenate([one] * 4, axis=1)
    out = []
    for q in range(4):
        if axis == 1:
            index = base + q * 16 + (at >> 6) * EDGE + (at & 7)
        else:
            index = base + q * 16 + (at >> 3)
        out.append(pick_lanes(tile, index))
    return jnp.concatenate(out, axis=1)


def diagonal(row):
    shape = (SLOTS, SLOTS)
    keep = lax.broadcasted_iota(jnp.int32, shape, 0) == lane(shape)
    return jnp.sum(jnp.where(keep, jnp.broadcast_to(row, shape), 0.0), axis=1, keepdims=True)


def one_hot(column, width):
    places = lane((column.shape[0], width)).astype(jnp.float32)
    return (column == places).astype(jnp.float32)


def select_rows(hot, table):
    return jnp.dot(hot, table, precision=lax.Precision.HIGHEST, preferred_element_type=jnp.float32)


def early_and_late(sizes):
    nx, ny, nz, nc = sizes
    late_x = [px for px in range(nx) if abs(px - nx // 2) <= nx // 4]
    early = [(0, 0, HUB)] + [(px, py, pc) for px, py in ((1, 0), (0, 1)) for pc in (HUB, 1 - HUB) if px not in late_x]
    return early, late_x, nz - nz // 2


def kernel(
    sizes,
    state, neighbour, send, ghost,
    kept_out, change_out, top_out,
    cells_ref, tables_ref, send_ref, halo_out, halo_in,
    value, from_plane, from_late, from_hubs, direct, result, overall,
    load_sem, table_sem, halo_sent, halo_arrived, max_sent, max_arrived, far,
):
    loads = [pltpu.make_async_copy(state.at[0, v], cells_ref.at[v], load_sem) for v in range(VARS)] + [
        pltpu.make_async_copy(neighbour.at[0], tables_ref.at[0], table_sem.at[0]),
        pltpu.make_async_copy(ghost.at[0], tables_ref.at[1], table_sem.at[0]),
        pltpu.make_async_copy(send, send_ref, table_sem.at[1]),
    ]
    for load in loads:
        load.start()

    nx, ny, nz, nc = sizes
    x, y, z, c = [lax.axis_index(a) for a in AXES]
    rank = x * ny + y
    ranks = nx * ny
    in_plane = 2 * ny * nz
    slab = z * nc + c
    has_below, has_above = slab > 0, slab < nz * nc - 1
    mid = ny // 2

    members = [[0], list(range(1, ny))]
    early, late_x, late_z = early_and_late(sizes)
    n_late = ny * late_z * 2
    early_of = [[e for e in early if e[1] in members[g]] for g in (0, 1)]
    targets = 4 + (nz > 2)

    def device(px, py, pz, pc):
        return {"morton_0": px, "morton_1": py, "group_0": pz, "group_1": pc}

    def hub_of(px, group):
        return device(px, group * mid, 0, HUB)

    def at_rank(offset):
        j = lax.rem(rank + (offset + ranks), ranks)
        return device(lax.div(j, ny), lax.rem(j, ny), z, c)

    group = jnp.minimum(y, 1)
    is_hub = ((y == 0) | (y == mid)) & (z == 0) & (c == HUB)

    barrier = pltpu.get_barrier_semaphore()

    def greet(target):
        pl.semaphore_signal(barrier, inc=1, device_id=target, device_id_type=pl.DeviceIdType.MESH)

    @pl.when(is_hub)
    def _():
        def plane(i, carry):
            py, pz, pc = lax.rem(lax.div(i, 2), ny), lax.div(i, 2 * ny), lax.rem(i, 2)

            @pl.when((py != y) | (pz != 0) | (pc != HUB))
            def _():
                greet(device(x, py, pz, pc))

            return carry

        lax.fori_loop(0, in_plane, plane, 0)
        for step in range(1, nx):
            greet(hub_of(lax.rem(x + step, nx), group))

    late_plane = (x >= late_x[0]) & (x <= late_x[-1])
    late = late_plane & (z >= nz - late_z)
    is_early = functools.reduce(jnp.logical_or, [(x == px) & (y == py) & (c == pc) for px, py, pc in early]) & (z == 0)

    def key(px, py, pz, pc):
        hops = jnp.minimum(px, nx - px) + jnp.minimum(py, ny - py) + jnp.minimum(pz, nz - pz)
        far = lax.div(2 * px, nx) + lax.div(2 * py, ny) + lax.div(2 * pz, nz)
        number = ((pz * ny + py) * nx + px) * 2 + pc
        order = 14 * number + 443 * hops + 620 * far - 420 * pc
        return order * (2 * nx * ny * nz) + number

    my_key = key(x, y, z, c)

    def comes_later(p):
        return key(p["morton_0"], p["morton_1"], p["group_0"], p["group_1"]) > my_key

    is_teller = (z == 2) & (c != HUB)
    is_listener = (z <= 1) & jnp.logical_not(is_hub)
    is_other = (z > 2) | ((z == 2) & (c == HUB))
    other = 1 - c
    below = device(x, y, lax.rem(z + (nz - 1) + c, nz), other)
    above = device(x, y, lax.rem(z + c, nz), other)

    def settle(ref, number, sem):
        pltpu.make_async_copy(ref.at[pl.ds(0, number)], ref.at[pl.ds(0, number)], sem).wait()

    beside = [at_rank(o) for o in OFFSETS]
    beside_later = [comes_later(p) for p in beside]
    below_later, above_later = has_below & comes_later(below), has_above & comes_later(above)
    below_earlier = has_below & jnp.logical_not(below_later)
    above_earlier = has_above & jnp.logical_not(above_later)
    partners = [(beside[d], beside_later[d]) for d in (1, 2)] + [(below, below_later), (above, above_later)]
    earlier = sum(jnp.logical_not(beside_later[d]).astype(jnp.int32) for d in (1, 2))
    earlier = earlier + below_earlier.astype(jnp.int32) + above_earlier.astype(jnp.int32)

    for target, later in partners:
        @pl.when(later)
        def _(target=target):
            greet(target)

    @pl.when(is_early)
    def _():
        def late_one(i, carry):
            px = late_x[0] + lax.rem(lax.div(i, 2), len(late_x))
            rest = lax.div(i, 2 * len(late_x))
            greet(device(px, lax.rem(rest, ny), nz - late_z + lax.div(rest, ny), lax.rem(i, 2)))
            return carry

        lax.fori_loop(0, len(late_x) * n_late, late_one, 0)

    @pl.when(is_listener | is_teller)
    def _():
        for px in range(nx):
            greet(hub_of(px, group))

    settle(tables_ref, 2, table_sem.at[0])
    near = tables_ref[0]
    settle(cells_ref, VARS, load_sem)
    in_row = diagonal(jnp.maximum(near[2:3, :], near[3:4, :]).astype(jnp.float32))
    live = jnp.broadcast_to(in_row, (SLOTS, CELLS)) >= 0.0
    cells = [cells_ref[v] for v in range(VARS)]
    prims = primitives(cells)
    velocity, pressure, sound = prims
    speed = jnp.abs(velocity[0]) + jnp.abs(velocity[1]) + jnp.abs(velocity[2]) + 3.0 * sound
    speed = jnp.where(live, speed, 0.0)
    top = jnp.max(functools.reduce(jnp.maximum, tiles_of(speed)), axis=0, keepdims=True)
    value[0] = top

    def push(source, target_ref, target, arrival):
        pltpu.make_async_remote_copy(
            src_ref=source, dst_ref=target_ref, send_sem=max_sent, recv_sem=max_arrived.at[arrival],
            device_id=target, device_id_type=pl.DeviceIdType.MESH).start()

    mine = (z * ny + y) * 2 + c

    @pl.when(late)
    def _():
        place = mine - 2 * ny * (nz - late_z)
        to_early = ((z - (nz - late_z)) * len(late_x) + x - late_x[0]) * (2 * ny) + y * 2 + c
        pl.semaphore_wait(barrier, 2 + len(early) + earlier)
        for px, py, pc in early:
            push(value.at[0], direct.at[to_early], device(px, py, 0, pc), 2 + (z == nz - 1).astype(jnp.int32))
        push(value.at[0], from_late.at[place], hub_of(x, 1), 2)
        push(value.at[0], from_late.at[place], hub_of(x, 0), 2)

    @pl.when(is_hub)
    def _():
        from_plane[mine] = top
        told = jnp.where(group == 0, len(members[0]), len(members[1])) * nx * targets
        pl.semaphore_wait(barrier, told + earlier)
        push(value.at[0], from_plane.at[mine], hub_of(x, 1 - group), 0)

    @pl.when(jnp.logical_not(is_hub | late))
    def _():
        pl.semaphore_wait(barrier, 2 + earlier)
        push(value.at[0], from_plane.at[mine], hub_of(x, 1), 0)
        push(value.at[0], from_plane.at[mine], hub_of(x, 0), 0)

    def to_partner(place, partner, at_theirs, later):
        which = 1 if later is None else later.astype(jnp.int32)
        return pltpu.make_async_remote_copy(
            src_ref=halo_out.at[place], dst_ref=halo_in.at[at_theirs], send_sem=halo_sent, recv_sem=halo_arrived.at[which],
            device_id=partner, device_id_type=pl.DeviceIdType.MESH)

    def arrived(number, most, which):
        for k in range(most + 1):
            if k:
                @pl.when(number == k)
                def _(k=k):
                    settle(halo_in, k, halo_arrived.at[which])

    halo_out[4] = pack_face(cells, 4)
    halo_out[5] = pack_face(cells, 5)
    go_down, go_up = to_partner(4, below, 5, below_later), to_partner(5, above, 4, above_later)

    @pl.when(below_earlier)
    def _():
        go_down.start()

    @pl.when(above_earlier)
    def _():
        go_up.start()

    @pl.when(jnp.logical_not(has_below))
    def _():
        halo_in[4] = halo_out[4]

    @pl.when(jnp.logical_not(has_above))
    def _():
        halo_in[5] = halo_out[5]

    own = [pack_face(cells, face) for face in range(4)]
    own_rows = jnp.concatenate(own, axis=0)
    loads[-1].wait()
    rows = jnp.concatenate([send_ref[t] for t in range(MSG)] + [jnp.full((SLOTS - MSG, ranks), -1, jnp.int32)], axis=0)
    columns = []
    for offset in OFFSETS:
        j = lax.rem(rank + (offset + ranks), ranks)
        picked = jnp.where(lane((SLOTS, ranks)) == j, rows, 0).astype(jnp.float32)
        entry = jnp.sum(picked, axis=1, keepdims=True)
        entry_int = entry.astype(jnp.int32)
        row = jnp.where(entry_int >= 0, (entry_int & 3) * SLOTS + (entry_int >> 2), -1)
        columns.append(row.astype(jnp.float32))
    hot = one_hot(jnp.concatenate(columns, axis=0), 4 * SLOTS)
    messages = select_rows(hot, own_rows)
    for d in range(4):
        halo_out[d] = messages[d * SLOTS:(d + 1) * SLOTS]
    lateral = [to_partner(d, beside[d], 3 - d, beside_later[d] if d in (1, 2) else None) for d in range(4)]

    for d in (1, 2):
        @pl.when(jnp.logical_not(beside_later[d]))
        def _(d=d):
            lateral[d].start()

    later = sum(flag.astype(jnp.int32) for _, flag in partners)
    arrived(later, 4, 0)
    for d in (1, 2):
        @pl.when(beside_later[d])
        def _(d=d):
            lateral[d].start()

    for d in (1, 2):
        pl.semaphore_signal(far, inc=1, device_id=beside[d], device_id_type=pl.DeviceIdType.MESH)

    @pl.when(below_later)
    def _():
        go_down.start()

    @pl.when(above_later)
    def _():
        go_up.start()

    pl.semaphore_wait(far, 2)
    lateral[3].start()
    lateral[0].start()


    arrived(earlier + 2, 6, 1)
    faces = jnp.concatenate([own_rows] + [halo_in[d] for d in range(4)], axis=0)
    sent_from = tables_ref[1]
    face_id = lax.broadcasted_iota(jnp.int32, (4, SLOTS), 0)
    slot_id = lane((4, SLOTS))
    local = (near >= 0) & ((near >> 3) == rank)
    place = jnp.where(local, (face_id ^ 1) * SLOTS + (near & 7), face_id * SLOTS + slot_id)
    relative = sent_from - rank * MSG + 2 * MSG
    block = sum((relative >= MSG * k).astype(jnp.int32) for k in range(1, 5))
    remote = 4 * SLOTS + SLOTS * (block - (block > 2).astype(jnp.int32)) + relative - MSG * block
    place = jnp.where(sent_from >= 0, jnp.where(block == 2, -1, remote), place).astype(jnp.float32)
    columns = [diagonal(place[k:k + 1, :]) for k in range(4)]
    hot = one_hot(jnp.concatenate(columns, axis=0), 8 * SLOTS)
    chosen = select_rows(hot, faces)
    ghosts = [chosen[k * SLOTS:(k + 1) * SLOTS] for k in range(4)]
    ghosts.append(halo_in[4])
    ghosts.append(halo_in[5])

    total = [0.0] * VARS
    at = lane((SLOTS, CELLS))
    for axis in range(3):
        stride = EDGE ** (2 - axis)
        position = (at >> (3 * (2 - axis))) & 7
        low = [jnp.where(position == 0, spread_face(ghosts[2 * axis], v, axis), pltpu.roll(cells[v], stride, 1))
               for v in range(VARS)]
        high = [jnp.where(position == EDGE - 1, spread_face(ghosts[2 * axis + 1], v, axis),
                          pltpu.roll(cells[v], CELLS - stride, 1)) for v in range(VARS)]
        flux_low, speed_low = axis_flux(low, primitives(low), axis)
        flux_high, speed_high = axis_flux(high, primitives(high), axis)
        speed_here = jnp.abs(velocity[axis]) + sound
        lower = jnp.maximum(speed_low, speed_here)
        upper = jnp.maximum(speed_here, speed_high)
        for v in range(VARS):
            total[v] = total[v] + 0.5 * (
                (flux_high[v] - flux_low[v]) - (upper * (high[v] - cells[v]) - lower * (cells[v] - low[v])))
    for v in range(VARS):
        kept_out[v] = jnp.where(live, cells[v], 0.0)
        change_out[v] = jnp.where(live, total[v], 0.0)

    @pl.when(has_below & has_above)
    def _():
        settle(halo_out, 6, halo_sent)

    @pl.when(jnp.logical_not(has_below & has_above))
    def _():
        settle(halo_out, 5, halo_sent)

    def finish(highest):
        top_out[...] = highest

    def of_hubs():
        return functools.reduce(jnp.maximum, [from_hubs[i] for i in range(nx)])

    def plane_top_of(rows):
        return jnp.max(from_plane[pl.ds(0, rows)], axis=0)

    def heard(number):
        settle(from_hubs, number, max_arrived.at[1])
        overall[0] = of_hubs()

        @pl.when(is_early)
        def _():
            last = len(late_x) * ny * 2
            before = len(late_x) * n_late - last
            if before:
                settle(direct, before, max_arrived.at[2])
                overall[0] = jnp.maximum(overall[0], jnp.max(direct[pl.ds(0, before)], axis=0))
            settle(direct, last, max_arrived.at[3])
            overall[0] = jnp.maximum(overall[0], jnp.max(direct[pl.ds(before, last)], axis=0))

        return overall[0]

    for g in (0, 1):
        number = len(members[g]) * nx * targets - 1

        @pl.when(is_hub & (group == g))
        def _(g=g, number=number):
            @pl.when(jnp.logical_not(late_plane))
            def _():
                settle(from_plane, in_plane - 1, max_arrived.at[0])
                value[1] = plane_top_of(in_plane)

            @pl.when(late_plane)
            def _():
                settle(from_plane, in_plane - n_late - 1, max_arrived.at[0])
                value[2] = plane_top_of(in_plane - n_late)
                for px, py, pc in early_of[g]:
                    push(value.at[2], from_hubs.at[x], device(px, py, 0, pc), 1)

                settle(from_late, n_late, max_arrived.at[2])
                value[1] = jnp.maximum(value[2], jnp.max(from_late[...], axis=0))

            from_hubs[x] = value[1]

            def tell(px, py, pz, pc):
                push(value.at[1], from_hubs.at[x], device(px, py, pz, pc), 1)

            def tell_z0(i, carry):
                py = i + members[g][0]
                for px in range(nx):
                    for pc in (HUB, 1 - HUB):
                        told = [ey for ex, ey, ec in early_of[g] if ex == px and ec == pc]
                        unless = []
                        if pc == HUB:
                            unless.append((px != x) | (py != y))
                        if told:
                            unless.append(jnp.logical_not(late_plane) | (py != told[0]))
                        if not unless:
                            tell(px, py, 0, pc)
                        else:
                            @pl.when(functools.reduce(jnp.logical_and, unless))
                            def _(px=px, pc=pc):
                                tell(px, py, 0, pc)
                return carry

            def tell_more(i, carry):
                py = i + members[g][0]
                for px in range(nx):
                    for pc in (HUB, 1 - HUB):
                        tell(px, py, 1, pc)
                    if nz > 2:
                        tell(px, py, 2, 1 - HUB)
                return carry

            lax.fori_loop(0, len(members[g]), tell_z0, 0)
            lax.fori_loop(0, len(members[g]), tell_more, 0)
            finish(heard(nx - 1))
            settle(from_plane, number + 1, max_sent)

    @pl.when(is_listener)
    def _():
        finish(heard(nx))

    if nz > 2:
        @pl.when(is_teller)
        def _():
            over_all = heard(nx)
            value[2] = over_all
            push(value.at[2], result.at[0], device(x, y, 2, HUB), 1)
            for pz in range(3, nz):
                for pc in (HUB, 1 - HUB):
                    push(value.at[2], result.at[0], device(x, y, pz, pc), 1)
            finish(over_all)
            settle(from_plane, 2 + 2 * nz - 5, max_sent)

    @pl.when(is_other)
    def _():
        settle(result, 1, max_arrived.at[1])
        finish(result[0])

    @pl.when(late)
    def _():
        settle(from_plane, 2 + len(early), max_sent)

    @pl.when(jnp.logical_not(is_hub | late | (is_teller & (nz > 2))))
    def _():
        settle(from_plane, 2, max_sent)


def apply_kernel(kept, change, top, updated, result, sem):
    step = COURANT / jnp.max(top[...], axis=1, keepdims=True)
    for v in range(VARS):
        result[v] = kept[v] - step * change[v]
        pltpu.make_async_copy(result.at[v], updated.at[0, v], sem).start()
    pltpu.make_async_copy(result, updated.at[0], sem).wait()


def per_device(sizes, state, patch_count, neighbour_table, send_table, ghost_table):
    nx, ny, nz, nc = sizes
    early, late_x, late_z = early_and_late(sizes)
    n_late = ny * late_z * 2
    any_space = pl.BlockSpec(memory_space=pl.ANY)
    vmem = pl.BlockSpec(memory_space=pltpu.VMEM)
    f32 = jnp.float32
    dma = pltpu.SemaphoreType.DMA
    block = pltpu.VMEM((VARS, SLOTS, CELLS), f32)
    kept, change, top = pl.pallas_call(
        functools.partial(kernel, sizes),
        out_shape=(block, block, pltpu.VMEM((1, LANES), f32)),
        in_specs=[any_space] * 4,
        out_specs=(vmem, vmem, vmem),
        scratch_shapes=[
            pltpu.VMEM((VARS, SLOTS, CELLS), f32),
            pltpu.VMEM((2, 4, SLOTS), jnp.int32),
            pltpu.VMEM((MSG, 1, nx * ny), jnp.int32),
            pltpu.VMEM((6, SLOTS, WIDE), f32),
            pltpu.VMEM((6, SLOTS, WIDE), f32),
            pltpu.VMEM((3, 1, LANES), f32),
            pltpu.VMEM((max(2 * ny * nz, 5 * nx * ny), 1, LANES), f32),
            pltpu.VMEM((n_late, 1, LANES), f32),
            pltpu.VMEM((nx, 1, LANES), f32),
            pltpu.VMEM((len(late_x) * n_late, 1, LANES), f32),
            pltpu.VMEM((1, 1, LANES), f32),
            pltpu.VMEM((1, 1, LANES), f32),
            dma, dma((2,)), dma, dma((2,)), dma, dma((4,)), pltpu.SemaphoreType.REGULAR,
        ],
        compiler_params=pltpu.CompilerParams(collective_id=0, has_side_effects=True),
        name="step",
    )(
        jnp.transpose(state, (0, 2, 1, 3)),
        jnp.transpose(neighbour_table, (0, 2, 1)),
        jnp.transpose(send_table, (2, 0, 1)),
        jnp.transpose(ghost_table, (0, 2, 1)),
    )
    updated = pl.pallas_call(
        apply_kernel,
        out_shape=jax.ShapeDtypeStruct((1, VARS, SLOTS, CELLS), f32),
        in_specs=[vmem] * 3,
        out_specs=any_space,
        scratch_shapes=[block, dma],
        name="apply",
    )(*[pltpu.with_memory_space_constraint(value, pltpu.VMEM) for value in (kept, change, top)])
    return jnp.transpose(updated, (0, 2, 1, 3))


def solution(mesh):
    nx = ny = round((mesh.shape["morton"]) ** 0.5)
    sizes = (nx, ny, mesh.shape["group"] // 2, 2)
    torus = Mesh(mesh.devices.reshape(sizes), AXES)
    return jax.shard_map(
        functools.partial(per_device, sizes),
        mesh=torus,
        in_specs=(
            P(GROUP, MORTON, None, None),
            P(MORTON),
            P(MORTON, None, None),
            P(MORTON, None, None),
            P(MORTON, None, None),
        ),
        out_specs=P(GROUP, MORTON, None, None),
        check_vma=False,
    )
```

```python
import functools

import jax
import jax.numpy as jnp
from jax import lax
from jax.experimental import pallas as pl
from jax.experimental.pallas import tpu as pltpu
from jax.sharding import Mesh
from jax.sharding import PartitionSpec as P

EDGE = 8
VARS = 5
CELLS = EDGE * EDGE * EDGE
FACE = EDGE * EDGE
SLOTS = 8
MSG = 5
LANES = 128
WIDE = 384
GAMMA = 1.4
COURANT = 0.8
AXES = ("morton_0", "morton_1", "group_0", "group_1")
MORTON = ("morton_0", "morton_1")
GROUP = ("group_0", "group_1")
OFFSETS = (-2, -1, 1, 2)
HUB = 1


def primitives(cells):
    density, mx, my, mz, energy = cells
    inverse = 1.0 / density
    velocity = (mx * inverse, my * inverse, mz * inverse)
    kinetic = mx * velocity[0] + my * velocity[1] + mz * velocity[2]
    pressure = (GAMMA - 1.0) * (energy - 0.5 * kinetic)
    sound = jnp.sqrt(GAMMA * pressure * inverse)
    return velocity, pressure, sound


def axis_flux(cells, prims, axis):
    velocity, pressure, sound = prims
    normal = velocity[axis]
    parts = [cells[1 + axis]]
    for comp in range(3):
        term = cells[1 + comp] * normal
        parts.append(term + pressure if comp == axis else term)
    parts.append((cells[4] + pressure) * normal)
    return parts, jnp.abs(normal) + sound


def lane(shape):
    return lax.broadcasted_iota(jnp.int32, shape, 1)


def pick_lanes(tile, index):
    return jnp.take_along_axis(tile, index, axis=1, mode="promise_in_bounds")


def tiles_of(wide):
    return [wide[:, q * LANES:(q + 1) * LANES] for q in range(wide.shape[1] // LANES)]


def pack_face(cells, face):
    axis, far = face // 2, face % 2
    if axis == 0:
        parts = [v[:, CELLS - FACE:] if far else v[:, :FACE] for v in cells]
        parts.append(jnp.zeros((SLOTS, FACE), jnp.float32))
        return jnp.concatenate(parts, axis=1)
    at = lane((SLOTS, LANES))
    place = at & (FACE - 1)
    if axis == 1:
        source = ((place >> 3) & 1) * FACE + far * (FACE - EDGE) + (place & 7)
    else:
        source = (place & 15) * EDGE + far * (EDGE - 1)
    packed = []
    for v in cells:
        tiles = tiles_of(v)
        out = pick_lanes(tiles[0], source)
        for q in range(1, 4):
            out = jnp.where((place >> 4) == q, pick_lanes(tiles[q], source), out)
        packed.append(out)
    packed.append(jnp.zeros((SLOTS, LANES), jnp.float32))
    pairs = [jnp.where(at < FACE, packed[2 * j], packed[2 * j + 1]) for j in range(3)]
    return jnp.concatenate(pairs, axis=1)


def spread_face(packed, var, axis):
    tile = tiles_of(packed)[var // 2]
    base = (var % 2) * FACE
    at = lane((SLOTS, LANES))
    if axis == 0:
        one = pick_lanes(tile, base + (at & (FACE - 1)))
        return jnp.concatenate([one] * 4, axis=1)
    out = []
    for q in range(4):
        if axis == 1:
            index = base + q * 16 + (at >> 6) * EDGE + (at & 7)
        else:
            index = base + q * 16 + (at >> 3)
        out.append(pick_lanes(tile, index))
    return jnp.concatenate(out, axis=1)


def diagonal(row):
    shape = (SLOTS, SLOTS)
    keep = lax.broadcasted_iota(jnp.int32, shape, 0) == lane(shape)
    return jnp.sum(jnp.where(keep, jnp.broadcast_to(row, shape), 0.0), axis=1, keepdims=True)


def one_hot(column, width):
    places = lane((column.shape[0], width)).astype(jnp.float32)
    return (column == places).astype(jnp.float32)


def select_rows(hot, table):
    return jnp.dot(hot, table, precision=lax.Precision.HIGHEST, preferred_element_type=jnp.float32)


def early_and_late(sizes):
    nx, ny, nz, nc = sizes
    late_x = [px for px in range(nx) if abs(px - nx // 2) <= nx // 4]
    early = [(0, 0, HUB)] + [(px, py, pc) for px, py in ((1, 0), (0, 1)) for pc in (HUB, 1 - HUB) if px not in late_x]
    return early, late_x, nz - nz // 2


def kernel(
    sizes,
    state, neighbour, send, ghost,
    kept_out, change_out, top_out,
    cells_ref, tables_ref, send_ref, halo_out, halo_in,
    value, from_plane, from_late, from_hubs, direct, result, overall,
    load_sem, table_sem, halo_sent, halo_arrived, max_sent, max_arrived, far,
):
    loads = [
        pltpu.make_async_copy(neighbour.at[0], tables_ref.at[0], table_sem.at[0]),
        pltpu.make_async_copy(ghost.at[0], tables_ref.at[1], table_sem.at[0]),
    ] + [pltpu.make_async_copy(state.at[0, v], cells_ref.at[v], load_sem) for v in range(VARS)] + [
        pltpu.make_async_copy(send, send_ref, table_sem.at[1]),
    ]
    for load in loads:
        load.start()

    nx, ny, nz, nc = sizes
    x, y, z, c = [lax.axis_index(a) for a in AXES]
    rank = x * ny + y
    ranks = nx * ny
    in_plane = 2 * ny * nz
    slab = z * nc + c
    has_below, has_above = slab > 0, slab < nz * nc - 1
    mid = ny // 2

    members = [[0], list(range(1, ny))]
    early, late_x, late_z = early_and_late(sizes)
    n_late = ny * late_z * 2
    early_of = [[e for e in early if e[1] in members[g]] for g in (0, 1)]
    targets = 4 + (nz > 2)

    def device(px, py, pz, pc):
        return {"morton_0": px, "morton_1": py, "group_0": pz, "group_1": pc}

    def hub_of(px, group):
        return device(px, group * mid, 0, HUB)

    def at_rank(offset):
        j = lax.rem(rank + (offset + ranks), ranks)
        return device(lax.div(j, ny), lax.rem(j, ny), z, c)

    group = jnp.minimum(y, 1)
    is_hub = ((y == 0) | (y == mid)) & (z == 0) & (c == HUB)

    barrier = pltpu.get_barrier_semaphore()

    def greet(target):
        pl.semaphore_signal(barrier, inc=1, device_id=target, device_id_type=pl.DeviceIdType.MESH)

    @pl.when(is_hub)
    def _():
        def plane(i, carry):
            py, pz, pc = lax.rem(lax.div(i, 2), ny), lax.div(i, 2 * ny), lax.rem(i, 2)

            @pl.when((py != y) | (pz != 0) | (pc != HUB))
            def _():
                greet(device(x, py, pz, pc))

            return carry

        lax.fori_loop(0, in_plane, plane, 0)
        for step in range(1, nx):
            greet(hub_of(lax.rem(x + step, nx), group))

    late_plane = (x >= late_x[0]) & (x <= late_x[-1])
    late = late_plane & (z >= nz - late_z)
    is_early = functools.reduce(jnp.logical_or, [(x == px) & (y == py) & (c == pc) for px, py, pc in early]) & (z == 0)

    def key(px, py, pz, pc):
        hops = jnp.minimum(px, nx - px) + jnp.minimum(py, ny - py) + jnp.minimum(pz, nz - pz)
        far = lax.div(2 * px, nx) + lax.div(2 * py, ny) + lax.div(2 * pz, nz)
        number = ((pz * ny + py) * nx + px) * 2 + pc
        order = 14 * number + 443 * hops + 620 * far - 420 * pc
        return order * (2 * nx * ny * nz) + number

    my_key = key(x, y, z, c)

    def comes_later(p):
        return key(p["morton_0"], p["morton_1"], p["group_0"], p["group_1"]) > my_key

    is_teller = (z == 2) & (c != HUB)
    is_listener = (z <= 1) & jnp.logical_not(is_hub)
    is_other = (z > 2) | ((z == 2) & (c == HUB))
    other = 1 - c
    below = device(x, y, lax.rem(z + (nz - 1) + c, nz), other)
    above = device(x, y, lax.rem(z + c, nz), other)

    def settle(ref, number, sem):
        pltpu.make_async_copy(ref.at[pl.ds(0, number)], ref.at[pl.ds(0, number)], sem).wait()

    beside = [at_rank(o) for o in OFFSETS]
    beside_later = [comes_later(p) for p in beside]
    below_later, above_later = has_below & comes_later(below), has_above & comes_later(above)
    below_earlier = has_below & jnp.logical_not(below_later)
    above_earlier = has_above & jnp.logical_not(above_later)
    partners = [(beside[d], beside_later[d]) for d in (1, 2)] + [(below, below_later), (above, above_later)]
    earlier = sum(jnp.logical_not(beside_later[d]).astype(jnp.int32) for d in (1, 2))
    earlier = earlier + below_earlier.astype(jnp.int32) + above_earlier.astype(jnp.int32)

    for target, later in partners:
        @pl.when(later)
        def _(target=target):
            greet(target)

    @pl.when(is_early)
    def _():
        def late_one(i, carry):
            px = late_x[0] + lax.rem(lax.div(i, 2), len(late_x))
            rest = lax.div(i, 2 * len(late_x))
            greet(device(px, lax.rem(rest, ny), nz - late_z + lax.div(rest, ny), lax.rem(i, 2)))
            return carry

        lax.fori_loop(0, len(late_x) * n_late, late_one, 0)

    @pl.when(is_listener | is_teller)
    def _():
        for px in range(nx):
            greet(hub_of(px, group))

    settle(tables_ref, 2, table_sem.at[0])
    near = tables_ref[0]
    in_row = diagonal(jnp.maximum(near[2:3, :], near[3:4, :]).astype(jnp.float32))
    live = jnp.broadcast_to(in_row, (SLOTS, CELLS)) >= 0.0
    settle(cells_ref, VARS, load_sem)
    cells = [cells_ref[v] for v in range(VARS)]
    prims = primitives(cells)
    velocity, pressure, sound = prims
    speed = jnp.abs(velocity[0]) + jnp.abs(velocity[1]) + jnp.abs(velocity[2]) + 3.0 * sound
    speed = jnp.where(live, speed, 0.0)
    top = jnp.max(functools.reduce(jnp.maximum, tiles_of(speed)), axis=0, keepdims=True)
    value[0] = top

    def push(source, target_ref, target, arrival):
        pltpu.make_async_remote_copy(
            src_ref=source, dst_ref=target_ref, send_sem=max_sent, recv_sem=max_arrived.at[arrival],
            device_id=target, device_id_type=pl.DeviceIdType.MESH).start()

    mine = (z * ny + y) * 2 + c

    @pl.when(late)
    def _():
        place = mine - 2 * ny * (nz - late_z)
        to_early = ((z - (nz - late_z)) * len(late_x) + x - late_x[0]) * (2 * ny) + y * 2 + c
        pl.semaphore_wait(barrier, 2 + len(early) + earlier)
        for px, py, pc in early:
            push(value.at[0], direct.at[to_early], device(px, py, 0, pc), 2 + (z == nz - 1).astype(jnp.int32))
        push(value.at[0], from_late.at[place], hub_of(x, 1), 2)
        push(value.at[0], from_late.at[place], hub_of(x, 0), 2)

    @pl.when(is_hub)
    def _():
        from_plane[mine] = top
        told = jnp.where(group == 0, len(members[0]), len(members[1])) * nx * targets
        pl.semaphore_wait(barrier, told + earlier)
        push(value.at[0], from_plane.at[mine], hub_of(x, 1 - group), 0)

    @pl.when(jnp.logical_not(is_hub | late))
    def _():
        pl.semaphore_wait(barrier, 2 + earlier)
        push(value.at[0], from_plane.at[mine], hub_of(x, 1), 0)
        push(value.at[0], from_plane.at[mine], hub_of(x, 0), 0)

    def to_partner(place, partner, at_theirs, later):
        which = 1 if later is None else later.astype(jnp.int32)
        return pltpu.make_async_remote_copy(
            src_ref=halo_out.at[place], dst_ref=halo_in.at[at_theirs], send_sem=halo_sent, recv_sem=halo_arrived.at[which],
            device_id=partner, device_id_type=pl.DeviceIdType.MESH)

    def arrived(number, most, which):
        for k in range(most + 1):
            if k:
                @pl.when(number == k)
                def _(k=k):
                    settle(halo_in, k, halo_arrived.at[which])

    halo_out[4] = pack_face(cells, 4)
    halo_out[5] = pack_face(cells, 5)
    go_down, go_up = to_partner(4, below, 5, below_later), to_partner(5, above, 4, above_later)

    @pl.when(below_earlier)
    def _():
        go_down.start()

    @pl.when(above_earlier)
    def _():
        go_up.start()

    @pl.when(jnp.logical_not(has_below))
    def _():
        halo_in[4] = halo_out[4]

    @pl.when(jnp.logical_not(has_above))
    def _():
        halo_in[5] = halo_out[5]

    own = [pack_face(cells, face) for face in range(4)]
    own_rows = jnp.concatenate(own, axis=0)
    loads[-1].wait()
    rows = jnp.concatenate([send_ref[t] for t in range(MSG)] + [jnp.full((SLOTS - MSG, ranks), -1, jnp.int32)], axis=0)
    columns = []
    for offset in OFFSETS:
        j = lax.rem(rank + (offset + ranks), ranks)
        picked = jnp.where(lane((SLOTS, ranks)) == j, rows, 0).astype(jnp.float32)
        entry = jnp.sum(picked, axis=1, keepdims=True)
        entry_int = entry.astype(jnp.int32)
        row = jnp.where(entry_int >= 0, (entry_int & 3) * SLOTS + (entry_int >> 2), -1)
        columns.append(row.astype(jnp.float32))
    hot = one_hot(jnp.concatenate(columns, axis=0), 4 * SLOTS)
    messages = select_rows(hot, own_rows)
    for d in range(4):
        halo_out[d] = messages[d * SLOTS:(d + 1) * SLOTS]
    lateral = [to_partner(d, beside[d], 3 - d, beside_later[d] if d in (1, 2) else None) for d in range(4)]

    for d in (1, 2):
        @pl.when(jnp.logical_not(beside_later[d]))
        def _(d=d):
            lateral[d].start()

    later = sum(flag.astype(jnp.int32) for _, flag in partners)
    arrived(later, 4, 0)
    for d in (1, 2):
        @pl.when(beside_later[d])
        def _(d=d):
            lateral[d].start()

    for d in (1, 2):
        pl.semaphore_signal(far, inc=1, device_id=beside[d], device_id_type=pl.DeviceIdType.MESH)

    @pl.when(below_later)
    def _():
        go_down.start()

    @pl.when(above_later)
    def _():
        go_up.start()

    pl.semaphore_wait(far, 2)
    lateral[3].start()
    lateral[0].start()


    arrived(earlier + 2, 6, 1)
    faces = jnp.concatenate([own_rows] + [halo_in[d] for d in range(4)], axis=0)
    sent_from = tables_ref[1]
    face_id = lax.broadcasted_iota(jnp.int32, (4, SLOTS), 0)
    slot_id = lane((4, SLOTS))
    local = (near >= 0) & ((near >> 3) == rank)
    place = jnp.where(local, (face_id ^ 1) * SLOTS + (near & 7), face_id * SLOTS + slot_id)
    relative = sent_from - rank * MSG + 2 * MSG
    block = sum((relative >= MSG * k).astype(jnp.int32) for k in range(1, 5))
    remote = 4 * SLOTS + SLOTS * (block - (block > 2).astype(jnp.int32)) + relative - MSG * block
    place = jnp.where(sent_from >= 0, jnp.where(block == 2, -1, remote), place).astype(jnp.float32)
    columns = [diagonal(place[k:k + 1, :]) for k in range(4)]
    hot = one_hot(jnp.concatenate(columns, axis=0), 8 * SLOTS)
    chosen = select_rows(hot, faces)
    ghosts = [chosen[k * SLOTS:(k + 1) * SLOTS] for k in range(4)]
    ghosts.append(halo_in[4])
    ghosts.append(halo_in[5])

    total = [0.0] * VARS
    at = lane((SLOTS, CELLS))
    for axis in range(3):
        stride = EDGE ** (2 - axis)
        position = (at >> (3 * (2 - axis))) & 7
        low = [jnp.where(position == 0, spread_face(ghosts[2 * axis], v, axis), pltpu.roll(cells[v], stride, 1))
               for v in range(VARS)]
        high = [jnp.where(position == EDGE - 1, spread_face(ghosts[2 * axis + 1], v, axis),
                          pltpu.roll(cells[v], CELLS - stride, 1)) for v in range(VARS)]
        flux_low, speed_low = axis_flux(low, primitives(low), axis)
        flux_high, speed_high = axis_flux(high, primitives(high), axis)
        speed_here = jnp.abs(velocity[axis]) + sound
        lower = jnp.maximum(speed_low, speed_here)
        upper = jnp.maximum(speed_here, speed_high)
        for v in range(VARS):
            total[v] = total[v] + 0.5 * (
                (flux_high[v] - flux_low[v]) - (upper * (high[v] - cells[v]) - lower * (cells[v] - low[v])))
    for v in range(VARS):
        kept_out[v] = jnp.where(live, cells[v], 0.0)
        change_out[v] = jnp.where(live, total[v], 0.0)

    @pl.when(has_below & has_above)
    def _():
        settle(halo_out, 6, halo_sent)

    @pl.when(jnp.logical_not(has_below & has_above))
    def _():
        settle(halo_out, 5, halo_sent)

    def finish(highest):
        top_out[...] = highest

    def of_hubs():
        return functools.reduce(jnp.maximum, [from_hubs[i] for i in range(nx)])

    def plane_top_of(rows):
        return jnp.max(from_plane[pl.ds(0, rows)], axis=0)

    def heard(number):
        settle(from_hubs, number, max_arrived.at[1])
        overall[0] = of_hubs()

        @pl.when(is_early)
        def _():
            last = len(late_x) * ny * 2
            before = len(late_x) * n_late - last
            if before:
                settle(direct, before, max_arrived.at[2])
                overall[0] = jnp.maximum(overall[0], jnp.max(direct[pl.ds(0, before)], axis=0))
            settle(direct, last, max_arrived.at[3])
            overall[0] = jnp.maximum(overall[0], jnp.max(direct[pl.ds(before, last)], axis=0))

        return overall[0]

    for g in (0, 1):
        number = len(members[g]) * nx * targets - 1

        @pl.when(is_hub & (group == g))
        def _(g=g, number=number):
            @pl.when(jnp.logical_not(late_plane))
            def _():
                settle(from_plane, in_plane - 1, max_arrived.at[0])
                value[1] = plane_top_of(in_plane)

            @pl.when(late_plane)
            def _():
                settle(from_plane, in_plane - n_late - 1, max_arrived.at[0])
                value[2] = plane_top_of(in_plane - n_late)
                for px, py, pc in early_of[g]:
                    push(value.at[2], from_hubs.at[x], device(px, py, 0, pc), 1)

                settle(from_late, n_late, max_arrived.at[2])
                value[1] = jnp.maximum(value[2], jnp.max(from_late[...], axis=0))

            from_hubs[x] = value[1]

            def tell(px, py, pz, pc):
                push(value.at[1], from_hubs.at[x], device(px, py, pz, pc), 1)

            def tell_z0(i, carry):
                py = i + members[g][0]
                for px in range(nx):
                    for pc in (HUB, 1 - HUB):
                        told = [ey for ex, ey, ec in early_of[g] if ex == px and ec == pc]
                        unless = []
                        if pc == HUB:
                            unless.append((px != x) | (py != y))
                        if told:
                            unless.append(jnp.logical_not(late_plane) | (py != told[0]))
                        if not unless:
                            tell(px, py, 0, pc)
                        else:
                            @pl.when(functools.reduce(jnp.logical_and, unless))
                            def _(px=px, pc=pc):
                                tell(px, py, 0, pc)
                return carry

            def tell_more(i, carry):
                py = i + members[g][0]
                for px in range(nx):
                    for pc in (HUB, 1 - HUB):
                        tell(px, py, 1, pc)
                    if nz > 2:
                        tell(px, py, 2, 1 - HUB)
                return carry

            lax.fori_loop(0, len(members[g]), tell_z0, 0)
            lax.fori_loop(0, len(members[g]), tell_more, 0)
            finish(heard(nx - 1))
            settle(from_plane, number + 1, max_sent)

    @pl.when(is_listener)
    def _():
        finish(heard(nx))

    if nz > 2:
        @pl.when(is_teller)
        def _():
            over_all = heard(nx)
            value[2] = over_all
            push(value.at[2], result.at[0], device(x, y, 2, HUB), 1)
            for pz in range(3, nz):
                for pc in (HUB, 1 - HUB):
                    push(value.at[2], result.at[0], device(x, y, pz, pc), 1)
            finish(over_all)
            settle(from_plane, 2 + 2 * nz - 5, max_sent)

    @pl.when(is_other)
    def _():
        settle(result, 1, max_arrived.at[1])
        finish(result[0])

    @pl.when(late)
    def _():
        settle(from_plane, 2 + len(early), max_sent)

    @pl.when(jnp.logical_not(is_hub | late | (is_teller & (nz > 2))))
    def _():
        settle(from_plane, 2, max_sent)


def apply_kernel(kept, change, top, updated, result, sem):
    step = COURANT / jnp.max(top[...], axis=1, keepdims=True)
    for v in range(VARS):
        result[v] = kept[v] - step * change[v]
        pltpu.make_async_copy(result.at[v], updated.at[0, v], sem).start()
    pltpu.make_async_copy(result, updated.at[0], sem).wait()


def per_device(sizes, state, patch_count, neighbour_table, send_table, ghost_table):
    nx, ny, nz, nc = sizes
    early, late_x, late_z = early_and_late(sizes)
    n_late = ny * late_z * 2
    any_space = pl.BlockSpec(memory_space=pl.ANY)
    vmem = pl.BlockSpec(memory_space=pltpu.VMEM)
    f32 = jnp.float32
    dma = pltpu.SemaphoreType.DMA
    block = pltpu.VMEM((VARS, SLOTS, CELLS), f32)
    kept, change, top = pl.pallas_call(
        functools.partial(kernel, sizes),
        out_shape=(block, block, pltpu.VMEM((1, LANES), f32)),
        in_specs=[any_space] * 4,
        out_specs=(vmem, vmem, vmem),
        scratch_shapes=[
            pltpu.VMEM((VARS, SLOTS, CELLS), f32),
            pltpu.VMEM((2, 4, SLOTS), jnp.int32),
            pltpu.VMEM((MSG, 1, nx * ny), jnp.int32),
            pltpu.VMEM((6, SLOTS, WIDE), f32),
            pltpu.VMEM((6, SLOTS, WIDE), f32),
            pltpu.VMEM((3, 1, LANES), f32),
            pltpu.VMEM((max(2 * ny * nz, 5 * nx * ny), 1, LANES), f32),
            pltpu.VMEM((n_late, 1, LANES), f32),
            pltpu.VMEM((nx, 1, LANES), f32),
            pltpu.VMEM((len(late_x) * n_late, 1, LANES), f32),
            pltpu.VMEM((1, 1, LANES), f32),
            pltpu.VMEM((1, 1, LANES), f32),
            dma, dma((2,)), dma, dma((2,)), dma, dma((4,)), pltpu.SemaphoreType.REGULAR,
        ],
        compiler_params=pltpu.CompilerParams(collective_id=0, has_side_effects=True),
        name="step",
    )(
        jnp.transpose(state, (0, 2, 1, 3)),
        jnp.transpose(neighbour_table, (0, 2, 1)),
        jnp.transpose(send_table, (2, 0, 1)),
        jnp.transpose(ghost_table, (0, 2, 1)),
    )
    updated = pl.pallas_call(
        apply_kernel,
        out_shape=jax.ShapeDtypeStruct((1, VARS, SLOTS, CELLS), f32),
        in_specs=[vmem] * 3,
        out_specs=any_space,
        scratch_shapes=[block, dma],
        name="apply",
    )(*[pltpu.with_memory_space_constraint(value, pltpu.VMEM) for value in (kept, change, top)])
    return jnp.transpose(updated, (0, 2, 1, 3))


def solution(mesh):
    nx = ny = round((mesh.shape["morton"]) ** 0.5)
    sizes = (nx, ny, mesh.shape["group"] // 2, 2)
    torus = Mesh(mesh.devices.reshape(sizes), AXES)
    return jax.shard_map(
        functools.partial(per_device, sizes),
        mesh=torus,
        in_specs=(
            P(GROUP, MORTON, None, None),
            P(MORTON),
            P(MORTON, None, None),
            P(MORTON, None, None),
            P(MORTON, None, None),
        ),
        out_specs=P(GROUP, MORTON, None, None),
        check_vma=False,
    )
```

```python
import functools

import jax
import jax.numpy as jnp
from jax import lax
from jax.experimental import pallas as pl
from jax.experimental.pallas import tpu as pltpu
from jax.sharding import Mesh
from jax.sharding import PartitionSpec as P

EDGE = 8
VARS = 5
CELLS = EDGE * EDGE * EDGE
FACE = EDGE * EDGE
SLOTS = 8
MSG = 5
LANES = 128
WIDE = 384
GAMMA = 1.4
COURANT = 0.8
AXES = ("morton_0", "morton_1", "group_0", "group_1")
MORTON = ("morton_0", "morton_1")
GROUP = ("group_0", "group_1")
OFFSETS = (-2, -1, 1, 2)
HUB = 1


def primitives(cells):
    density, mx, my, mz, energy = cells
    inverse = 1.0 / density
    velocity = (mx * inverse, my * inverse, mz * inverse)
    kinetic = mx * velocity[0] + my * velocity[1] + mz * velocity[2]
    pressure = (GAMMA - 1.0) * (energy - 0.5 * kinetic)
    sound = jnp.sqrt(GAMMA * pressure * inverse)
    return velocity, pressure, sound


def axis_flux(cells, prims, axis):
    velocity, pressure, sound = prims
    normal = velocity[axis]
    parts = [cells[1 + axis]]
    for comp in range(3):
        term = cells[1 + comp] * normal
        parts.append(term + pressure if comp == axis else term)
    parts.append((cells[4] + pressure) * normal)
    return parts, jnp.abs(normal) + sound


def lane(shape):
    return lax.broadcasted_iota(jnp.int32, shape, 1)


def pick_lanes(tile, index):
    return jnp.take_along_axis(tile, index, axis=1, mode="promise_in_bounds")


def tiles_of(wide):
    return [wide[:, q * LANES:(q + 1) * LANES] for q in range(wide.shape[1] // LANES)]


def pack_face(cells, face):
    axis, far = face // 2, face % 2
    if axis == 0:
        parts = [v[:, CELLS - FACE:] if far else v[:, :FACE] for v in cells]
        parts.append(jnp.zeros((SLOTS, FACE), jnp.float32))
        return jnp.concatenate(parts, axis=1)
    at = lane((SLOTS, LANES))
    place = at & (FACE - 1)
    if axis == 1:
        source = ((place >> 3) & 1) * FACE + far * (FACE - EDGE) + (place & 7)
    else:
        source = (place & 15) * EDGE + far * (EDGE - 1)
    packed = []
    for v in cells:
        tiles = tiles_of(v)
        out = pick_lanes(tiles[0], source)
        for q in range(1, 4):
            out = jnp.where((place >> 4) == q, pick_lanes(tiles[q], source), out)
        packed.append(out)
    packed.append(jnp.zeros((SLOTS, LANES), jnp.float32))
    pairs = [jnp.where(at < FACE, packed[2 * j], packed[2 * j + 1]) for j in range(3)]
    return jnp.concatenate(pairs, axis=1)


def spread_face(packed, var, axis):
    tile = tiles_of(packed)[var // 2]
    base = (var % 2) * FACE
    at = lane((SLOTS, LANES))
    if axis == 0:
        one = pick_lanes(tile, base + (at & (FACE - 1)))
        return jnp.concatenate([one] * 4, axis=1)
    out = []
    for q in range(4):
        if axis == 1:
            index = base + q * 16 + (at >> 6) * EDGE + (at & 7)
        else:
            index = base + q * 16 + (at >> 3)
        out.append(pick_lanes(tile, index))
    return jnp.concatenate(out, axis=1)


def diagonal(row):
    shape = (SLOTS, SLOTS)
    keep = lax.broadcasted_iota(jnp.int32, shape, 0) == lane(shape)
    return jnp.sum(jnp.where(keep, jnp.broadcast_to(row, shape), 0.0), axis=1, keepdims=True)


def one_hot(column, width):
    places = lane((column.shape[0], width)).astype(jnp.float32)
    return (column == places).astype(jnp.float32)


def select_rows(hot, table):
    return jnp.dot(hot, table, precision=lax.Precision.HIGHEST, preferred_element_type=jnp.float32)


def early_and_late(sizes):
    nx, ny, nz, nc = sizes
    late_x = [px for px in range(nx) if abs(px - nx // 2) <= nx // 4]
    early = [(0, 0, HUB)] + [(px, py, pc) for px, py in ((1, 0), (0, 1)) for pc in (HUB, 1 - HUB) if px not in late_x]
    return early, late_x, nz - nz // 2


def kernel(
    sizes,
    state, neighbour, send, ghost,
    kept_out, change_out, top_out,
    cells_ref, tables_ref, send_ref, halo_out, halo_in,
    value, from_plane, from_late, from_hubs, direct, result, overall,
    load_sem, table_sem, halo_sent, halo_arrived, max_sent, max_arrived, far,
):
    loads = [
        pltpu.make_async_copy(neighbour.at[0], tables_ref.at[0], table_sem.at[0]),
        pltpu.make_async_copy(ghost.at[0], tables_ref.at[1], table_sem.at[0]),
    ] + [pltpu.make_async_copy(state.at[0, v], cells_ref.at[v], load_sem) for v in range(VARS)] + [
        pltpu.make_async_copy(send, send_ref, table_sem.at[1]),
    ]
    for load in loads:
        load.start()

    nx, ny, nz, nc = sizes
    x, y, z, c = [lax.axis_index(a) for a in AXES]
    rank = x * ny + y
    ranks = nx * ny
    in_plane = 2 * ny * nz
    slab = z * nc + c
    has_below, has_above = slab > 0, slab < nz * nc - 1
    mid = ny // 2

    members = [[0], list(range(1, ny))]
    early, late_x, late_z = early_and_late(sizes)
    n_late = ny * late_z * 2
    early_of = [[e for e in early if e[1] in members[g]] for g in (0, 1)]
    targets = 4 + (nz > 2)

    def device(px, py, pz, pc):
        return {"morton_0": px, "morton_1": py, "group_0": pz, "group_1": pc}

    def hub_of(px, group):
        return device(px, group * mid, 0, HUB)

    def at_rank(offset):
        j = lax.rem(rank + (offset + ranks), ranks)
        return device(lax.div(j, ny), lax.rem(j, ny), z, c)

    group = jnp.minimum(y, 1)
    is_hub = ((y == 0) | (y == mid)) & (z == 0) & (c == HUB)

    barrier = pltpu.get_barrier_semaphore()

    def greet(target):
        pl.semaphore_signal(barrier, inc=1, device_id=target, device_id_type=pl.DeviceIdType.MESH)

    @pl.when(is_hub)
    def _():
        def plane(i, carry):
            py, pz, pc = lax.rem(lax.div(i, 2), ny), lax.div(i, 2 * ny), lax.rem(i, 2)

            @pl.when((py != y) | (pz != 0) | (pc != HUB))
            def _():
                greet(device(x, py, pz, pc))

            return carry

        lax.fori_loop(0, in_plane, plane, 0)
        for step in range(1, nx):
            greet(hub_of(lax.rem(x + step, nx), group))

    late_plane = (x >= late_x[0]) & (x <= late_x[-1])
    late = late_plane & (z >= nz - late_z)
    is_early = functools.reduce(jnp.logical_or, [(x == px) & (y == py) & (c == pc) for px, py, pc in early]) & (z == 0)

    def key(px, py, pz, pc):
        hops = jnp.minimum(px, nx - px) + jnp.minimum(py, ny - py) + jnp.minimum(pz, nz - pz)
        far = lax.div(2 * px, nx) + lax.div(2 * py, ny) + lax.div(2 * pz, nz)
        number = ((pz * ny + py) * nx + px) * 2 + pc
        order = 14 * number + 443 * hops + 620 * far - 420 * pc
        return order * (2 * nx * ny * nz) + number

    my_key = key(x, y, z, c)

    def comes_later(p):
        return key(p["morton_0"], p["morton_1"], p["group_0"], p["group_1"]) > my_key

    is_teller = (z == 2) & (c != HUB)
    is_listener = (z <= 1) & jnp.logical_not(is_hub)
    is_other = (z > 2) | ((z == 2) & (c == HUB))
    other = 1 - c
    below = device(x, y, lax.rem(z + (nz - 1) + c, nz), other)
    above = device(x, y, lax.rem(z + c, nz), other)

    def settle(ref, number, sem):
        pltpu.make_async_copy(ref.at[pl.ds(0, number)], ref.at[pl.ds(0, number)], sem).wait()

    beside = [at_rank(o) for o in OFFSETS]
    beside_later = [comes_later(p) for p in beside]
    below_later, above_later = has_below & comes_later(below), has_above & comes_later(above)
    below_earlier = has_below & jnp.logical_not(below_later)
    above_earlier = has_above & jnp.logical_not(above_later)
    partners = [(beside[d], beside_later[d]) for d in (1, 2)] + [(below, below_later), (above, above_later)]
    earlier = sum(jnp.logical_not(beside_later[d]).astype(jnp.int32) for d in (1, 2))
    earlier = earlier + below_earlier.astype(jnp.int32) + above_earlier.astype(jnp.int32)

    for target, later in partners:
        @pl.when(later)
        def _(target=target):
            greet(target)

    @pl.when(is_early)
    def _():
        def late_one(i, carry):
            px = late_x[0] + lax.rem(lax.div(i, 2), len(late_x))
            rest = lax.div(i, 2 * len(late_x))
            greet(device(px, lax.rem(rest, ny), nz - late_z + lax.div(rest, ny), lax.rem(i, 2)))
            return carry

        lax.fori_loop(0, len(late_x) * n_late, late_one, 0)

    @pl.when(is_listener | is_teller)
    def _():
        for px in range(nx):
            greet(hub_of(px, group))

    settle(tables_ref, 2, table_sem.at[0])
    near = tables_ref[0]
    in_row = diagonal(jnp.maximum(near[2:3, :], near[3:4, :]).astype(jnp.float32))
    live = jnp.broadcast_to(in_row, (SLOTS, CELLS)) >= 0.0
    settle(cells_ref, VARS, load_sem)
    cells = [cells_ref[v] for v in range(VARS)]
    prims = primitives(cells)
    velocity, pressure, sound = prims
    speed = jnp.abs(velocity[0]) + jnp.abs(velocity[1]) + jnp.abs(velocity[2]) + 3.0 * sound
    speed = jnp.where(live, speed, 0.0)
    top = jnp.max(functools.reduce(jnp.maximum, tiles_of(speed)), axis=0, keepdims=True)
    value[0] = top

    def push(source, target_ref, target, arrival):
        pltpu.make_async_remote_copy(
            src_ref=source, dst_ref=target_ref, send_sem=max_sent, recv_sem=max_arrived.at[arrival],
            device_id=target, device_id_type=pl.DeviceIdType.MESH).start()

    mine = (z * ny + y) * 2 + c

    @pl.when(late)
    def _():
        place = mine - 2 * ny * (nz - late_z)
        turned = lax.rem(x + (len(late_x) - nx // 2 - 1), len(late_x))
        to_early = ((z - (nz - late_z)) * len(late_x) + turned) * (2 * ny) + y * 2 + c
        pl.semaphore_wait(barrier, 2 + len(early) + earlier)
        for px, py, pc in early:
            push(value.at[0], direct.at[to_early], device(px, py, 0, pc), 2 + ((z == nz - 1) & (x == nx // 2)).astype(jnp.int32))
        push(value.at[0], from_late.at[place], hub_of(x, 1), 2)
        push(value.at[0], from_late.at[place], hub_of(x, 0), 2)

    @pl.when(is_hub)
    def _():
        from_plane[mine] = top
        told = jnp.where(group == 0, len(members[0]), len(members[1])) * nx * targets
        pl.semaphore_wait(barrier, told + earlier)
        push(value.at[0], from_plane.at[mine], hub_of(x, 1 - group), 0)

    @pl.when(jnp.logical_not(is_hub | late))
    def _():
        pl.semaphore_wait(barrier, 2 + earlier)
        push(value.at[0], from_plane.at[mine], hub_of(x, 1), 0)
        push(value.at[0], from_plane.at[mine], hub_of(x, 0), 0)

    def to_partner(place, partner, at_theirs, later):
        which = 1 if later is None else later.astype(jnp.int32)
        return pltpu.make_async_remote_copy(
            src_ref=halo_out.at[place], dst_ref=halo_in.at[at_theirs], send_sem=halo_sent, recv_sem=halo_arrived.at[which],
            device_id=partner, device_id_type=pl.DeviceIdType.MESH)

    def arrived(number, most, which):
        for k in range(most + 1):
            if k:
                @pl.when(number == k)
                def _(k=k):
                    settle(halo_in, k, halo_arrived.at[which])

    halo_out[4] = pack_face(cells, 4)
    halo_out[5] = pack_face(cells, 5)
    go_down, go_up = to_partner(4, below, 5, below_later), to_partner(5, above, 4, above_later)

    @pl.when(below_earlier)
    def _():
        go_down.start()

    @pl.when(above_earlier)
    def _():
        go_up.start()

    @pl.when(jnp.logical_not(has_below))
    def _():
        halo_in[4] = halo_out[4]

    @pl.when(jnp.logical_not(has_above))
    def _():
        halo_in[5] = halo_out[5]

    own = [pack_face(cells, face) for face in range(4)]
    own_rows = jnp.concatenate(own, axis=0)
    loads[-1].wait()
    rows = jnp.concatenate([send_ref[t] for t in range(MSG)] + [jnp.full((SLOTS - MSG, ranks), -1, jnp.int32)], axis=0)
    columns = []
    for offset in OFFSETS:
        j = lax.rem(rank + (offset + ranks), ranks)
        picked = jnp.where(lane((SLOTS, ranks)) == j, rows, 0).astype(jnp.float32)
        entry = jnp.sum(picked, axis=1, keepdims=True)
        entry_int = entry.astype(jnp.int32)
        row = jnp.where(entry_int >= 0, (entry_int & 3) * SLOTS + (entry_int >> 2), -1)
        columns.append(row.astype(jnp.float32))
    hot = one_hot(jnp.concatenate(columns, axis=0), 4 * SLOTS)
    messages = select_rows(hot, own_rows)
    for d in range(4):
        halo_out[d] = messages[d * SLOTS:(d + 1) * SLOTS]
    lateral = [to_partner(d, beside[d], 3 - d, beside_later[d] if d in (1, 2) else None) for d in range(4)]

    for d in (1, 2):
        @pl.when(jnp.logical_not(beside_later[d]))
        def _(d=d):
            lateral[d].start()

    later = sum(flag.astype(jnp.int32) for _, flag in partners)
    arrived(later, 4, 0)
    for d in (1, 2):
        @pl.when(beside_later[d])
        def _(d=d):
            lateral[d].start()

    for d in (1, 2):
        pl.semaphore_signal(far, inc=1, device_id=beside[d], device_id_type=pl.DeviceIdType.MESH)

    @pl.when(below_later)
    def _():
        go_down.start()

    @pl.when(above_later)
    def _():
        go_up.start()

    pl.semaphore_wait(far, 2)
    lateral[3].start()
    lateral[0].start()


    arrived(earlier + 2, 6, 1)
    faces = jnp.concatenate([own_rows] + [halo_in[d] for d in range(4)], axis=0)
    sent_from = tables_ref[1]
    face_id = lax.broadcasted_iota(jnp.int32, (4, SLOTS), 0)
    slot_id = lane((4, SLOTS))
    local = (near >= 0) & ((near >> 3) == rank)
    place = jnp.where(local, (face_id ^ 1) * SLOTS + (near & 7), face_id * SLOTS + slot_id)
    relative = sent_from - rank * MSG + 2 * MSG
    block = sum((relative >= MSG * k).astype(jnp.int32) for k in range(1, 5))
    remote = 4 * SLOTS + SLOTS * (block - (block > 2).astype(jnp.int32)) + relative - MSG * block
    place = jnp.where(sent_from >= 0, jnp.where(block == 2, -1, remote), place).astype(jnp.float32)
    columns = [diagonal(place[k:k + 1, :]) for k in range(4)]
    hot = one_hot(jnp.concatenate(columns, axis=0), 8 * SLOTS)
    chosen = select_rows(hot, faces)
    ghosts = [chosen[k * SLOTS:(k + 1) * SLOTS] for k in range(4)]
    ghosts.append(halo_in[4])
    ghosts.append(halo_in[5])

    total = [0.0] * VARS
    at = lane((SLOTS, CELLS))
    for axis in range(3):
        stride = EDGE ** (2 - axis)
        position = (at >> (3 * (2 - axis))) & 7
        low = [jnp.where(position == 0, spread_face(ghosts[2 * axis], v, axis), pltpu.roll(cells[v], stride, 1))
               for v in range(VARS)]
        high = [jnp.where(position == EDGE - 1, spread_face(ghosts[2 * axis + 1], v, axis),
                          pltpu.roll(cells[v], CELLS - stride, 1)) for v in range(VARS)]
        flux_low, speed_low = axis_flux(low, primitives(low), axis)
        flux_high, speed_high = axis_flux(high, primitives(high), axis)
        speed_here = jnp.abs(velocity[axis]) + sound
        lower = jnp.maximum(speed_low, speed_here)
        upper = jnp.maximum(speed_here, speed_high)
        for v in range(VARS):
            total[v] = total[v] + 0.5 * (
                (flux_high[v] - flux_low[v]) - (upper * (high[v] - cells[v]) - lower * (cells[v] - low[v])))
    for v in range(VARS):
        kept_out[v] = jnp.where(live, cells[v], 0.0)
        change_out[v] = jnp.where(live, total[v], 0.0)

    @pl.when(has_below & has_above)
    def _():
        settle(halo_out, 6, halo_sent)

    @pl.when(jnp.logical_not(has_below & has_above))
    def _():
        settle(halo_out, 5, halo_sent)

    def finish(highest):
        top_out[...] = highest

    def of_hubs():
        return functools.reduce(jnp.maximum, [from_hubs[i] for i in range(nx)])

    def plane_top_of(rows):
        return jnp.max(from_plane[pl.ds(0, rows)], axis=0)

    def heard(number):
        settle(from_hubs, number, max_arrived.at[1])
        overall[0] = of_hubs()

        @pl.when(is_early)
        def _():
            last = ny * 2
            before = len(late_x) * n_late - last
            if before:
                settle(direct, before, max_arrived.at[2])
                overall[0] = jnp.maximum(overall[0], jnp.max(direct[pl.ds(0, before)], axis=0))
            settle(direct, last, max_arrived.at[3])
            overall[0] = jnp.maximum(overall[0], jnp.max(direct[pl.ds(before, last)], axis=0))

        return overall[0]

    for g in (0, 1):
        number = len(members[g]) * nx * targets - 1

        @pl.when(is_hub & (group == g))
        def _(g=g, number=number):
            @pl.when(jnp.logical_not(late_plane))
            def _():
                settle(from_plane, in_plane - 1, max_arrived.at[0])
                value[1] = plane_top_of(in_plane)

            @pl.when(late_plane)
            def _():
                settle(from_plane, in_plane - n_late - 1, max_arrived.at[0])
                value[2] = plane_top_of(in_plane - n_late)
                for px, py, pc in early_of[g]:
                    push(value.at[2], from_hubs.at[x], device(px, py, 0, pc), 1)

                settle(from_late, n_late, max_arrived.at[2])
                value[1] = jnp.maximum(value[2], jnp.max(from_late[...], axis=0))

            from_hubs[x] = value[1]

            def tell(px, py, pz, pc):
                push(value.at[1], from_hubs.at[x], device(px, py, pz, pc), 1)

            def tell_z0(i, carry):
                py = i + members[g][0]
                for px in range(nx):
                    for pc in (HUB, 1 - HUB):
                        told = [ey for ex, ey, ec in early_of[g] if ex == px and ec == pc]
                        unless = []
                        if pc == HUB:
                            unless.append((px != x) | (py != y))
                        if told:
                            unless.append(jnp.logical_not(late_plane) | (py != told[0]))
                        if not unless:
                            tell(px, py, 0, pc)
                        else:
                            @pl.when(functools.reduce(jnp.logical_and, unless))
                            def _(px=px, pc=pc):
                                tell(px, py, 0, pc)
                return carry

            def tell_more(i, carry):
                py = i + members[g][0]
                for px in range(nx):
                    for pc in (HUB, 1 - HUB):
                        tell(px, py, 1, pc)
                    if nz > 2:
                        tell(px, py, 2, 1 - HUB)
                return carry

            lax.fori_loop(0, len(members[g]), tell_z0, 0)
            lax.fori_loop(0, len(members[g]), tell_more, 0)
            finish(heard(nx - 1))
            settle(from_plane, number + 1, max_sent)

    @pl.when(is_listener)
    def _():
        finish(heard(nx))

    if nz > 2:
        @pl.when(is_teller)
        def _():
            over_all = heard(nx)
            value[2] = over_all
            push(value.at[2], result.at[0], device(x, y, 2, HUB), 1)
            for pz in range(3, nz):
                for pc in (HUB, 1 - HUB):
                    push(value.at[2], result.at[0], device(x, y, pz, pc), 1)
            finish(over_all)
            settle(from_plane, 2 + 2 * nz - 5, max_sent)

    @pl.when(is_other)
    def _():
        settle(result, 1, max_arrived.at[1])
        finish(result[0])

    @pl.when(late)
    def _():
        settle(from_plane, 2 + len(early), max_sent)

    @pl.when(jnp.logical_not(is_hub | late | (is_teller & (nz > 2))))
    def _():
        settle(from_plane, 2, max_sent)


def apply_kernel(kept, change, top, updated, result, sem):
    step = COURANT / jnp.max(top[...], axis=1, keepdims=True)
    for v in range(VARS):
        result[v] = kept[v] - step * change[v]
        pltpu.make_async_copy(result.at[v], updated.at[0, v], sem).start()
    pltpu.make_async_copy(result, updated.at[0], sem).wait()


def per_device(sizes, state, patch_count, neighbour_table, send_table, ghost_table):
    nx, ny, nz, nc = sizes
    early, late_x, late_z = early_and_late(sizes)
    n_late = ny * late_z * 2
    any_space = pl.BlockSpec(memory_space=pl.ANY)
    vmem = pl.BlockSpec(memory_space=pltpu.VMEM)
    f32 = jnp.float32
    dma = pltpu.SemaphoreType.DMA
    block = pltpu.VMEM((VARS, SLOTS, CELLS), f32)
    kept, change, top = pl.pallas_call(
        functools.partial(kernel, sizes),
        out_shape=(block, block, pltpu.VMEM((1, LANES), f32)),
        in_specs=[any_space] * 4,
        out_specs=(vmem, vmem, vmem),
        scratch_shapes=[
            pltpu.VMEM((VARS, SLOTS, CELLS), f32),
            pltpu.VMEM((2, 4, SLOTS), jnp.int32),
            pltpu.VMEM((MSG, 1, nx * ny), jnp.int32),
            pltpu.VMEM((6, SLOTS, WIDE), f32),
            pltpu.VMEM((6, SLOTS, WIDE), f32),
            pltpu.VMEM((3, 1, LANES), f32),
            pltpu.VMEM((max(2 * ny * nz, 5 * nx * ny), 1, LANES), f32),
            pltpu.VMEM((n_late, 1, LANES), f32),
            pltpu.VMEM((nx, 1, LANES), f32),
            pltpu.VMEM((len(late_x) * n_late, 1, LANES), f32),
            pltpu.VMEM((1, 1, LANES), f32),
            pltpu.VMEM((1, 1, LANES), f32),
            dma, dma((2,)), dma, dma((2,)), dma, dma((4,)), pltpu.SemaphoreType.REGULAR,
        ],
        compiler_params=pltpu.CompilerParams(collective_id=0, has_side_effects=True),
        name="step",
    )(
        jnp.transpose(state, (0, 2, 1, 3)),
        jnp.transpose(neighbour_table, (0, 2, 1)),
        jnp.transpose(send_table, (2, 0, 1)),
        jnp.transpose(ghost_table, (0, 2, 1)),
    )
    updated = pl.pallas_call(
        apply_kernel,
        out_shape=jax.ShapeDtypeStruct((1, VARS, SLOTS, CELLS), f32),
        in_specs=[vmem] * 3,
        out_specs=any_space,
        scratch_shapes=[block, dma],
        name="apply",
    )(*[pltpu.with_memory_space_constraint(value, pltpu.VMEM) for value in (kept, change, top)])
    return jnp.transpose(updated, (0, 2, 1, 3))


def solution(mesh):
    nx = ny = round((mesh.shape["morton"]) ** 0.5)
    sizes = (nx, ny, mesh.shape["group"] // 2, 2)
    torus = Mesh(mesh.devices.reshape(sizes), AXES)
    return jax.shard_map(
        functools.partial(per_device, sizes),
        mesh=torus,
        in_specs=(
            P(GROUP, MORTON, None, None),
            P(MORTON),
            P(MORTON, None, None),
            P(MORTON, None, None),
            P(MORTON, None, None),
        ),
        out_specs=P(GROUP, MORTON, None, None),
        check_vma=False,
    )
```
